32 devices in a mesh: tm: 4 (over z), map: 8 (over y, x, core).
Axes of the slice: x: 2, y: 2, z: 4, core: 2. Of those that a mesh axis runs over, the one named last changes fastest.
Arguments:
- points: float32 [3, 32768, 128], P(None, ('tm', 'map')), may hold values from -6 to 6
- poses: float32 [6, 1024], P(None, ('tm', 'map')), may hold values from -1.5 to 1.5
- normal_angles: float32 [2, 8192], P(None, ('tm', 'map')), may hold values from -3.140625 to 3.140625
- voxel_ids: int32 [32768], P(('tm', 'map')), may hold values from -1 to 8191, as said below
- scan_ids: int32 [32768], P(('tm', 'map')), may hold values from 0 to 255
Outputs:
- hessian: float32 [36, 1024], P(None, ('tm', 'map'))
- gradient: float32 [6, 1024], P(None, ('tm', 'map'))
- plane_cost: float32 [8192], P(('tm', 'map'))
The draws below stay inside these ranges and needn't reach their ends.
Inputs may be any that keep to these rules, and one draw needn't show every extreme that they name: `voxel_ids`: -1 marks an empty slot. Otherwise the block at position s among the 1024 blocks of its device has its voxel among those of owner o = s // 32, that is, in [o * 256, (o + 1) * 256), where owners are devices in tm+map order. In every draw some owner gets a live block in every slot from every device.
All inputs are finite; a program needn't handle non-finite values.
Results may differ from the reference program's by a relative error of at most 0.0003.
Values sent between devices are 32-bit elements; how exact they have to be, the bound alone decides.
A program may use at most 128 MiB of HBM per device.

```python
import jax
import jax.numpy as jnp
from jax import lax

PTS = 128
CAP = 32
VOX_DEV = 256
BLK_DEV = 1024
BLOCKS = 32768
VOXELS = 8192
SCAN_ROW = 256
SCANS = 1024
N_MAP = 8
DEVICES = 32


def draw_voxel_ids(key, part):
    keys = jax.random.split(jax.random.fold_in(key, 71), 5)
    slot = jnp.arange(BLOCKS, dtype=jnp.int32)
    owner_of = slot % BLK_DEV // CAP
    hottest = jax.random.randint(keys[0], (), 0, DEVICES)
    level = jax.random.randint(keys[1], (DEVICES,), 3, 10)
    level = jnp.where(jnp.arange(DEVICES, dtype=jnp.int32) == hottest, 10, level)
    coin = jax.random.randint(keys[2], (BLOCKS,), 0, 10)
    first = jax.random.randint(keys[3], (BLOCKS,), 0, VOX_DEV)
    second = jax.random.randint(keys[4], (BLOCKS,), 0, VOX_DEV)
    picked = jnp.minimum(first, second)
    return jnp.where(coin < level[owner_of], owner_of * VOX_DEV + picked, -1).astype(jnp.int32)


def with_ends(result, stream_key, smallest, high):
    longest = result.shape.index(max(result.shape))
    spots = []
    for shift in (0, 1):
        where = [jax.random.randint(jax.random.fold_in(stream_key, axis), (), 0, length) for axis, length in enumerate(result.shape)]
        where[longest] = (where[longest] + shift) % result.shape[longest]
        spots.append(tuple(where))
    return result.at[spots[0]].set(smallest).at[spots[1]].set(high)


def block_scale(rng, extent, shards, smallest, top_value):
    def one(axis_at, parts):
        heights = jax.random.uniform(jax.random.fold_in(jax.random.fold_in(rng, 6), axis_at), (parts,), jnp.float32, smallest / len(shards), top_value / len(shards))
        return jnp.repeat(jnp.exp(heights), extent[axis_at] // parts).reshape((-1,) + (1,) * (len(extent) - axis_at - 1))

    factor_of = one(*shards[0])
    for cut in shards[1:]:
        factor_of = factor_of * one(*cut)
    return factor_of


def normal_values(stream_key, extent, spread, reach, shards=(), held_as=jnp.bfloat16):
    drawn = jax.random.normal(stream_key, extent, jnp.float32) * spread
    if len(shards) > 0:
        drawn = block_scale(stream_key, extent, shards, -0.22, 0.18) * drawn
    return jnp.clip(drawn, min=-reach, max=reach).astype(held_as)


def setup_inputs(seed: int = 0) -> dict:
    splits = jax.random.split(jax.random.key(seed), 6)
    return {
        "points": normal_values(splits[0], (3, BLOCKS, PTS), 1.0, 6.0, ((1, 32),), jnp.float32),
        "poses": jnp.clip(jax.random.uniform(splits[1], (6, SCANS), jnp.float32, -1.5, 1.5) * block_scale(splits[1], (6, SCANS), ((1, 32),), -0.4, 0.0), -1.5, 1.5),
        "normal_angles": jnp.clip(jax.random.uniform(splits[2], (2, VOXELS), jnp.float32, -3.140625, 3.140625), -3.140625, 3.140625),
        "voxel_ids": draw_voxel_ids(jax.random.fold_in(splits[5], 71), 0),
        "scan_ids": with_ends(jax.random.randint(splits[4], (BLOCKS,), 0, SCAN_ROW), jax.random.fold_in(splits[4], 1), 0, SCAN_ROW - 1).astype(jnp.int32),
    }


def rigid(angles):
    cos_x, sin_x = jnp.cos(angles[0]), jnp.sin(angles[0])
    cos_y, sin_y = jnp.cos(angles[1]), jnp.sin(angles[1])
    cos_z, sin_z = jnp.cos(angles[2]), jnp.sin(angles[2])
    return jnp.stack([
        cos_z * cos_y, cos_z * sin_y * sin_x - sin_z * cos_x, cos_z * sin_y * cos_x + sin_z * sin_x,
        sin_z * cos_y, sin_z * sin_y * sin_x + cos_z * cos_x, sin_z * sin_y * cos_x - cos_z * sin_x,
        -sin_y, cos_y * sin_x, cos_y * cos_x,
        angles[3], angles[4], angles[5]])


def transform(points, per_block):
    rows_out = []
    for axis_out in range(3):
        acc = per_block[9 + axis_out][:, None]
        for axis_in in range(3):
            acc = acc + per_block[3 * axis_out + axis_in][:, None] * points[axis_in]
        rows_out.append(acc)
    return jnp.stack(rows_out)


def moments_of(world_pts):
    first = jnp.sum(world_pts, axis=2)
    pairs = [(0, 0), (1, 1), (2, 2), (0, 1), (0, 2), (1, 2)]
    second = jnp.stack([jnp.sum(world_pts[i] * world_pts[j], axis=1) for i, j in pairs])
    return jnp.concatenate([first, second], axis=0)


def unit_normal(normal_angles):
    theta, phi = normal_angles[0], normal_angles[1]
    return jnp.stack([jnp.sin(theta) * jnp.cos(phi), jnp.sin(theta) * jnp.sin(phi), jnp.cos(theta)])


def block_terms(world_pts, normal, offset):
    cross = jnp.stack([
        world_pts[1] * normal[2][:, None] - world_pts[2] * normal[1][:, None],
        world_pts[2] * normal[0][:, None] - world_pts[0] * normal[2][:, None],
        world_pts[0] * normal[1][:, None] - world_pts[1] * normal[0][:, None]])
    normal_b = jnp.broadcast_to(normal[:, :, None], world_pts.shape)
    jacobian = jnp.concatenate([cross, normal_b], axis=0)
    resid = jnp.sum(world_pts * normal[:, :, None], axis=0) - offset[:, None]
    outer = jnp.einsum('ibp,jbp->ijb', jacobian, jacobian, precision=lax.Precision.HIGHEST)
    grad_b = jnp.einsum('ibp,bp->ib', jacobian, resid, precision=lax.Precision.HIGHEST)
    return jnp.concatenate([outer.reshape(36, -1), grad_b], axis=0)


def reference(points, poses, normal_angles, voxel_ids, scan_ids):
    pose_table = rigid(poses)
    block_index = jnp.arange(BLOCKS, dtype=jnp.int32)
    global_scan = (block_index // BLK_DEV // N_MAP) * SCAN_ROW + scan_ids
    is_live = voxel_ids >= 0

    def span_world(index):
        start = (index * BLK_DEV).astype(jnp.int32)
        pts = lax.dynamic_slice_in_dim(points, start, BLK_DEV, 1)
        scans = lax.dynamic_slice_in_dim(global_scan, start, BLK_DEV, 0)
        return transform(pts, pose_table[:, scans])

    def span_moments(index):
        start = (index * BLK_DEV).astype(jnp.int32)
        live_c = lax.dynamic_slice_in_dim(is_live, start, BLK_DEV, 0)
        return jnp.where(live_c[None, :], moments_of(span_world(index)), 0.0)

    moments = lax.map(span_moments, jnp.arange(DEVICES, dtype=jnp.int32))
    moments = jnp.transpose(moments, (0, 2, 1)).reshape(BLOCKS, 9)
    segment = jnp.where(is_live, voxel_ids, VOXELS)
    voxel_sums = jax.ops.segment_sum(moments, segment, num_segments=VOXELS + 1)[:VOXELS].T
    counts = jax.ops.segment_sum(is_live.astype(jnp.float32), segment, num_segments=VOXELS + 1)[:VOXELS] * PTS
    floor_count = jnp.maximum(counts, 1.0)
    normal = unit_normal(normal_angles)
    offset = jnp.sum(normal * voxel_sums[:3], axis=0) / floor_count
    quadric = (normal[0] ** 2 * voxel_sums[3] + normal[1] ** 2 * voxel_sums[4] + normal[2] ** 2 * voxel_sums[5]
               + 2.0 * (normal[0] * normal[1] * voxel_sums[6] + normal[0] * normal[2] * voxel_sums[7]
                        + normal[1] * normal[2] * voxel_sums[8]))
    plane_cost = quadric / floor_count - offset ** 2
    safe_ids = jnp.where(is_live, voxel_ids, 0)
    block_normal = jnp.where(is_live[None, :], normal[:, safe_ids], 0.0)
    block_offset = jnp.where(is_live, offset[safe_ids], 0.0)

    def span_terms(index):
        start = (index * BLK_DEV).astype(jnp.int32)
        norm_c = lax.dynamic_slice_in_dim(block_normal, start, BLK_DEV, 1)
        off_c = lax.dynamic_slice_in_dim(block_offset, start, BLK_DEV, 0)
        return block_terms(span_world(index), norm_c, off_c)

    terms = lax.map(span_terms, jnp.arange(DEVICES, dtype=jnp.int32))
    terms = jnp.transpose(terms, (0, 2, 1)).reshape(BLOCKS, 42)
    per_scan = jax.ops.segment_sum(terms, global_scan, num_segments=SCANS).T
    per_scan = per_scan * (SCANS / (BLOCKS * PTS))
    return per_scan[:36], per_scan[36:], plane_cost
```

```python
import functools

import jax
import jax.numpy as jnp
from jax import lax
from jax.experimental import pallas as pl
from jax.experimental.pallas import tpu as pltpu
from jax.sharding import PartitionSpec as P

LANES = 128
MESH = pl.DeviceIdType.MESH
PAIRS = [(0, 0), (1, 1), (2, 2), (0, 1), (0, 2), (1, 2)]
PAIR_ROW = {}
for _k, (_i, _j) in enumerate(PAIRS):
    PAIR_ROW[(_i, _j)] = _k
    PAIR_ROW[(_j, _i)] = _k


ROWS = [("h", i, j) for i in range(6) for j in range(i, 6)] + [("g", i) for i in range(6)]


def parts_of(x):
    high = x.astype(jnp.bfloat16)
    rest = x - high.astype(jnp.float32)
    mid = rest.astype(jnp.bfloat16)
    low = (rest - mid.astype(jnp.float32)).astype(jnp.bfloat16)
    return jnp.concatenate([high, mid, low], axis=0)


def joined(y):
    rows = y.shape[0] // 3
    return y[:rows] + y[rows : 2 * rows] + y[2 * rows :]


def group_turn(pieces, out_group, group, lanes_per):
    total = None
    for a, piece in enumerate(pieces):
        shift = lax.rem((a - out_group) * lanes_per + LANES, LANES)
        if isinstance(out_group, int):
            shift = ((a - out_group) * lanes_per) % LANES
        moved = piece if isinstance(shift, int) and shift == 0 else pltpu.roll(piece, shift, 1)
        total = moved if total is None else jnp.where(group == a, moved, total)
    return total


def loop(count, body):
    if count <= 8:
        for i in range(count):
            body(i)
    else:
        def step(i, carry):
            body(i)
            return carry

        lax.fori_loop(0, count, step, 0)


def kernel(
    sizes,
    points,
    poses,
    angles,
    voxel_ids,
    scan_ids,
    packed,
    pts,
    pose_pad,
    table,
    sent,
    world,
    vox_row,
    send1,
    recv1,
    moved,
    send2,
    recv2,
    back,
    terms,
    send3,
    recv3,
    pts_sem,
    sends,
    recvs,
):
    n_tm, n_map, slots, npoints, scale = sizes
    devices = n_tm * n_map
    blocks = pts.shape[1]
    chunks = blocks // LANES
    per = LANES // slots
    own_scans = poses.shape[1]
    spread = LANES // own_scans
    scans = own_scans * n_map
    wide = scans // LANES
    voxels = angles.shape[1]
    tm = lax.axis_index("tm")
    mp = lax.axis_index("map")
    me = tm * n_map + mp

    def place(q):
        return (q // n_map, lax.rem(q, n_map))

    def chunk_copy(r):
        rows = pl.ds(r * LANES, LANES)
        return pltpu.make_async_copy(points.at[:, rows, :], pts.at[:, rows, :], pts_sem.at[r])

    loop(chunks, lambda r: chunk_copy(r).start())
    barrier = pltpu.get_barrier_semaphore()

    def greet(i, carry):
        pl.semaphore_signal(
            barrier, inc=1, device_id=place(lax.rem(me + i, devices)), device_id_type=MESH
        )
        return carry

    lax.fori_loop(1, devices, greet, 0)

    lane = lax.broadcasted_iota(jnp.int32, (8, LANES), 1)

    pose_pad[...] = jnp.zeros_like(pose_pad)
    for g in range(spread):
        pose_pad[0:6, g * own_scans : (g + 1) * own_scans] = poses[...]
    pose = pose_pad[...]
    cos, sin = jnp.cos(pose), jnp.sin(pose)
    cx, cy, cz = cos[0:1], cos[1:2], cos[2:3]
    sx, sy, sz = sin[0:1], sin[1:2], sin[2:3]
    rows = [
        cz * cy,
        cz * sy * sx - sz * cx,
        cz * sy * cx + sz * sx,
        sz * cy,
        sz * sy * sx + cz * cx,
        sz * sy * cx - cz * sx,
        -sy,
        cy * sx,
        cy * cx,
        pose[3:4],
        pose[4:5],
        pose[5:6],
    ]
    sent[...] = jnp.zeros_like(sent)

    def sent_row(k):
        return 8 * (k // 6) + k % 6

    for k, row in enumerate(rows):
        sent[pl.ds(sent_row(11 + k), chunks, stride=32), :] = jnp.broadcast_to(
            row, (chunks, LANES)
        )
    ids = voxel_ids[...]
    row_of = lax.broadcasted_iota(jnp.int32, ids.shape, 0)
    lane_of = lax.broadcasted_iota(jnp.int32, ids.shape, 1)
    owner_of = row_of * per + lane_of // slots
    local_ids = jnp.where(ids >= 0, ids - owner_of * voxels, -1).astype(jnp.float32)
    sent[pl.ds(sent_row(9), chunks, stride=32), :] = local_ids
    sent[pl.ds(sent_row(10), chunks, stride=32), :] = scan_ids[...].astype(jnp.float32)

    theta, phi = angles[0:1, :], angles[1:2, :]
    sin_theta = jnp.sin(theta)
    normal = [sin_theta * jnp.cos(phi), sin_theta * jnp.sin(phi), jnp.cos(theta)]

    def raw_moments(r):
        chunk_copy(r).wait()
        at = pl.ds(r * LANES, LANES)
        xyz = [pts[i, at, :].T for i in range(3)]
        sums = [jnp.sum(x, axis=0, keepdims=True) for x in xyz]
        sums += [jnp.sum(xyz[i] * xyz[j], axis=0, keepdims=True) for i, j in PAIRS]
        for k, row in enumerate(sums):
            sent[pl.ds(r * 32 + sent_row(k), 1), :] = row

    group = lane // slots

    def pack(r):
        raw_moments(r)
        pieces = [sent[pl.ds(pl.multiple_of(r * 32 + 8 * c, 8), 8), :] for c in range(4)]
        for g in range(per):
            send1[r * per + g] = group_turn(pieces, g, group, slots)[0:6]

    loop(chunks, pack)
    pl.semaphore_wait(barrier, devices - 1)

    def map_copy(i, source, dest, s):
        peer = lax.rem(mp + i, n_map)
        return pltpu.make_async_remote_copy(
            src_ref=source(peer),
            dst_ref=dest.at[mp],
            send_sem=sends.at[s],
            recv_sem=recvs.at[s],
            device_id=(tm, peer),
            device_id_type=MESH,
        )

    def wait_bytes(ref, sem):
        pltpu.make_async_copy(ref, ref, sem).wait()

    scan_iota = lax.broadcasted_iota(jnp.int32, (scans, LANES), 0)

    def scan_hot(r):
        return jnp.where(scan_ids[pl.ds(r, 1), :] == scan_iota, 1.0, 0.0).astype(jnp.bfloat16)

    def every(ref, k, stride):
        return ref[pl.ds(k, chunks, stride=stride), :]

    def transformed(source):
        first = [every(source, sent_row(k), 32) for k in range(3)]
        second = [every(source, sent_row(3 + k), 32) for k in range(6)]
        pose_at = [every(table, sent_row(11 + k) - 8, 24) for k in range(12)]
        rot = [pose_at[3 * i : 3 * i + 3] for i in range(3)]
        shift = pose_at[9:]
        turned = [sum(rot[i][j] * first[j] for j in range(3)) for i in range(3)]
        half_turned = [
            [sum(rot[i][k] * second[PAIR_ROW[(k, j)]] for k in range(3)) for j in range(3)]
            for i in range(3)
        ]
        m1 = [turned[i] + npoints * shift[i] for i in range(3)]
        m2 = [
            sum(half_turned[i][k] * rot[j][k] for k in range(3))
            + turned[i] * shift[j]
            + shift[i] * m1[j]
            for i, j in PAIRS
        ]
        return m1, m2

    upper = tm // (n_tm // 2)

    def all_copy(i, source, dest, s):
        step = lax.rem(i, devices) // n_map
        tm_peer = (1 - upper) * (n_tm - 1 - step) + upper * step
        peer = tm_peer * n_map + lax.rem(mp + i, n_map)
        return pltpu.make_async_remote_copy(
            src_ref=source(peer),
            dst_ref=dest.at[me],
            send_sem=sends.at[s],
            recv_sem=recvs.at[s],
            device_id=place(peer),
            device_id_type=MESH,
        ), peer

    def send_all(source, dest, s):
        def start_with(i, carry):
            copy, peer = all_copy(i, source, dest, s)

            @pl.when(peer != me)
            def _():
                copy.start()

            return carry

        lax.fori_loop(0, devices, start_with, 0, unroll=4)

    send_all(lambda peer: send1.at[peer], recv1, 1)
    recv1[me] = send1[me]
    wait_bytes(recv1.at[pl.ds(0, devices - 1)], recvs.at[1])

    vox_iota = lax.broadcasted_iota(jnp.int32, (voxels, LANES), 0).astype(jnp.float32)
    zero2 = jnp.zeros((2, LANES), jnp.float32)

    def unpack(r):
        pieces = [jnp.concatenate([recv1[r * per + g], zero2], axis=0) for g in range(per)]
        for c in range(4):
            moved[pl.ds(pl.multiple_of(r * 32 + 8 * c, 8), 8), :] = group_turn(
                pieces, c, group, slots
            )

    loop(chunks, unpack)

    def vox_hot(r):
        row = moved[pl.ds(r * 32 + sent_row(9), 1), :]
        return jnp.where(row == vox_iota, 1.0, 0.0).astype(jnp.bfloat16)

    float_iota = scan_iota.astype(jnp.float32)

    def group_parts(t):
        return parts_of(
            jnp.concatenate(
                [
                    moved[pl.ds(pl.multiple_of((t * wide + h) * 32 + 8, 8), 24), :]
                    for h in range(wide)
                ],
                axis=1,
            )
        )

    def look_up(t):
        table_parts = group_parts(t)
        for h in range(wide):
            r = t * wide + h
            row = moved[pl.ds(r * 32 + sent_row(10), 1), :]
            hot = jnp.where(row == float_iota, 1.0, 0.0).astype(jnp.bfloat16)
            found = jnp.dot(table_parts, hot, preferred_element_type=jnp.float32)
            table[pl.ds(pl.multiple_of(r * 24, 8), 24), :] = joined(found)

    loop(n_tm, look_up)
    m1, m2 = transformed(moved)
    world[...] = jnp.ones_like(world)
    for k, value in enumerate(m1 + m2):
        world[pl.ds(k, chunks, stride=16), :] = value

    contract_last = (((1,), (1,)), ((), ()))
    def add_voxels(r, acc):
        values = world[pl.ds(pl.multiple_of(r * 16, 16), 16), :]
        return acc + lax.dot_general(
            parts_of(values), vox_hot(r), contract_last, preferred_element_type=jnp.float32
        )

    def summed(body, rows, columns):
        acc = jnp.zeros((rows, columns), jnp.float32)
        if chunks <= 8:
            for r in range(chunks):
                acc = body(r, acc)
            return acc
        return lax.fori_loop(0, chunks, body, acc)

    sums = joined(summed(add_voxels, 48, voxels))
    s1 = [sums[k : k + 1] for k in range(3)]
    s2 = [sums[3 + k : 4 + k] for k in range(6)]
    floor_count = jnp.maximum(sums[9:10] * npoints, 1.0)
    offset = sum(normal[i] * s1[i] for i in range(3)) / floor_count
    quadric = sum(normal[i] ** 2 * s2[i] for i in range(3)) + 2.0 * sum(
        normal[PAIRS[k][0]] * normal[PAIRS[k][1]] * s2[k] for k in range(3, 6)
    )
    cost = quadric / floor_count - offset**2
    for h in range(voxels // LANES):
        packed[8 + h : 9 + h, :] = cost[:, h * LANES : (h + 1) * LANES]
    vox_row[...] = jnp.zeros_like(vox_row)
    for k, row in enumerate(normal + [offset]):
        vox_row[k : k + 1, :] = row
    reply_parts = parts_of(vox_row[...])

    def reply(r):
        found = jnp.dot(reply_parts, vox_hot(r), preferred_element_type=jnp.float32)
        value = joined(found)
        rolled = [value] + [pltpu.roll(value, slots * a, 1) for a in range(1, per)]
        for g in range(per):
            total = jnp.zeros_like(value)
            for c in range(4):
                total = jnp.where(corner & (group == c), rolled[(c - g) % per], total)
            send2[r * per + g] = jnp.sum(total, axis=0, keepdims=True)

    corner = lax.broadcasted_iota(jnp.int32, (8, LANES), 0) == group
    loop(chunks, reply)
    send_all(lambda peer: send2.at[peer], recv2, 2)
    recv2[me] = send2[me]

    own_parts = group_parts(tm)

    def look_up_own(r):
        found = jnp.dot(own_parts, scan_hot(r), preferred_element_type=jnp.float32)
        table[pl.ds(pl.multiple_of(r * 24, 8), 24), :] = joined(found)

    loop(chunks, look_up_own)
    m1, m2 = transformed(sent)
    wait_bytes(recv2.at[pl.ds(0, devices - 1)], recvs.at[2])

    back[...] = recv2[...].reshape(devices, LANES)
    pieces = [back[pl.ds(g, chunks, stride=per), :] for g in range(per)]
    wide_group = lane_of // slots
    n = [group_turn(pieces, c, wide_group, slots) for c in range(3)]
    d = group_turn(pieces, 3, wide_group, slots)

    def skew(v):
        return [n[2] * v[1] - n[1] * v[2], n[0] * v[2] - n[2] * v[0], n[1] * v[0] - n[0] * v[1]]

    full = [[m2[PAIR_ROW[(i, j)]] for j in range(3)] for i in range(3)]
    columns = [skew([full[k][j] for k in range(3)]) for j in range(3)]
    left = [[columns[j][i] for j in range(3)] for i in range(3)]
    corner_block = [skew(left[i]) for i in range(3)]
    skew_first = skew(m1)
    found = {}
    for i in range(3):
        for j in range(3):
            if j >= i:
                found[("h", i, j)] = corner_block[i][j]
                found[("h", 3 + i, 3 + j)] = npoints * n[i] * n[j]
            found[("h", i, 3 + j)] = skew_first[i] * n[j]
    rest = n[0] * m1[0] + n[1] * m1[1] + n[2] * m1[2] - npoints * d
    for i in range(3):
        found[("g", i)] = sum(left[i][j] * n[j] for j in range(3)) - d * skew_first[i]
        found[("g", 3 + i)] = n[i] * rest
    for name, value in found.items():
        k = ROWS.index(name)
        terms[pl.ds(k, chunks, stride=32), :] = value
    for k in range(len(found), 32):
        terms[pl.ds(k, chunks, stride=32), :] = jnp.zeros_like(d)

    def add_scans(r, acc):
        values = parts_of(terms[pl.ds(pl.multiple_of(r * 32, 32), 32), :])
        return acc + lax.dot_general(
            values, scan_hot(r), contract_last, preferred_element_type=jnp.float32
        )

    per_scan = joined(summed(add_scans, 96, scans)) * scale
    scan_group = lane // own_scans
    for h in range(wide):
        pieces = [
            per_scan[8 * c : 8 * c + 8, h * LANES : (h + 1) * LANES] for c in range(4)
        ]
        for b in range(spread):
            send3[h * spread + b] = group_turn(pieces, b, scan_group, own_scans)
    for i in range(1, n_map):
        map_copy(i, lambda peer: send3.at[peer], recv3, 0).start()
    recv3[mp] = send3[mp]
    wait_bytes(recv3.at[pl.ds(0, n_map - 1)], recvs.at[0])
    total = recv3[0]
    for m in range(1, n_map):
        total = total + recv3[m]
    packed[0:8, :] = total

    wait_bytes(send1.at[pl.ds(0, devices - 1)], sends.at[1])
    wait_bytes(recv2.at[pl.ds(0, devices - 1)], sends.at[2])
    wait_bytes(send3.at[pl.ds(0, n_map - 1)], sends.at[0])


def finish(packed, hess_out, grad_out, cost_out, lines):
    own_scans = grad_out.shape[1]
    total = packed[0:8, :]
    lined = [total] + [pltpu.roll(total, LANES - own_scans * c, 1) for c in range(1, 4)]

    def row_at(name):
        k = ROWS.index(name)
        return lined[k // 8][k % 8 : k % 8 + 1]

    lines[...] = jnp.zeros_like(lines)
    for i in range(6):
        for j in range(6):
            lines[6 * i + j : 6 * i + j + 1, :] = row_at(("h", min(i, j), max(i, j)))
        grad_out[i : i + 1, :] = row_at(("g", i))[:, 0:own_scans]
    hess_out[...] = lines[...].T[0:own_scans, 0:36]
    for h in range(cost_out.shape[1] // LANES):
        cost_out[:, h * LANES : (h + 1) * LANES] = packed[8 + h : 9 + h, :]


def local(points, poses, normal_angles, voxel_ids, scan_ids):
    blocks, npoints = points.shape[1:]
    n_tm, n_map = lax.axis_size("tm"), lax.axis_size("map")
    devices = n_tm * n_map
    slots = blocks // devices
    chunks = blocks // LANES
    vox_count = normal_angles.shape[1]
    own_scans = poses.shape[1]
    assert LANES % slots == 0 and own_scans * 4 == LANES and n_map % 4 == 0
    assert npoints == LANES and slots * 4 == LANES
    scale = own_scans * devices / (blocks * devices * npoints)
    f32 = jnp.float32
    vmem = pl.BlockSpec(memory_space=pltpu.VMEM)
    extra = -(-(vox_count // LANES) // 8) * 8
    packed = pl.pallas_call(
        functools.partial(kernel, (n_tm, n_map, slots, float(npoints), scale)),
        out_shape=pltpu.VMEM((8 + extra, LANES), f32),
        in_specs=[pl.BlockSpec(memory_space=pl.ANY)] + [vmem] * 4,
        out_specs=vmem,
        scratch_shapes=[
            pltpu.VMEM(points.shape, f32),
            pltpu.VMEM((8, LANES), f32),
            pltpu.VMEM((chunks * 24, LANES), f32),
            pltpu.VMEM((chunks * 32, LANES), f32),
            pltpu.VMEM((chunks * 16, LANES), f32),
            pltpu.VMEM((8, vox_count), f32),
            pltpu.VMEM((devices, 6, LANES), f32),
            pltpu.VMEM((devices, 6, LANES), f32),
            pltpu.VMEM((chunks * 32, LANES), f32),
            pltpu.VMEM((devices, 1, LANES), f32),
            pltpu.VMEM((devices, 1, LANES), f32),
            pltpu.VMEM((devices, LANES), f32),
            pltpu.VMEM((chunks * 32, LANES), f32),
            pltpu.VMEM((n_map, 8, LANES), f32),
            pltpu.VMEM((n_map, 8, LANES), f32),
            pltpu.SemaphoreType.DMA((chunks,)),
            pltpu.SemaphoreType.DMA((3,)),
            pltpu.SemaphoreType.DMA((3,)),
        ],
        compiler_params=pltpu.CompilerParams(collective_id=0, has_side_effects=True),
    )(
        points,
        poses,
        normal_angles,
        voxel_ids.reshape(chunks, LANES),
        scan_ids.reshape(chunks, LANES),
    )
    hess, grad, cost = pl.pallas_call(
        finish,
        out_shape=(
            jax.ShapeDtypeStruct((own_scans, 36), f32),
            jax.ShapeDtypeStruct((6, own_scans), f32),
            jax.ShapeDtypeStruct((1, vox_count), f32),
        ),
        in_specs=[vmem],
        out_specs=(vmem, vmem, vmem),
        scratch_shapes=[pltpu.VMEM((LANES, LANES), f32)],
    )(pltpu.with_memory_space_constraint(packed, pltpu.VMEM))
    return hess.T, grad, cost.reshape(vox_count)


def solution(mesh):
    return jax.shard_map(
        local,
        mesh=mesh,
        in_specs=(
            P(None, ("tm", "map"), None),
            P(None, ("tm", "map")),
            P(None, ("tm", "map")),
            P(("tm", "map")),
            P(("tm", "map")),
        ),
        out_specs=(P(None, ("tm", "map")), P(None, ("tm", "map")), P(("tm", "map"))),
        check_vma=False,
    )
```

```python
import functools

import jax
import jax.numpy as jnp
from jax import lax
from jax.experimental import pallas as pl
from jax.experimental.pallas import tpu as pltpu
from jax.sharding import PartitionSpec as P

LANES = 128
MESH = pl.DeviceIdType.MESH
PAIRS = [(0, 0), (1, 1), (2, 2), (0, 1), (0, 2), (1, 2)]
PAIR_ROW = {}
for _k, (_i, _j) in enumerate(PAIRS):
    PAIR_ROW[(_i, _j)] = _k
    PAIR_ROW[(_j, _i)] = _k

ROWS = [("h", i, j) for i in range(6) for j in range(i, 6)] + [("g", i) for i in range(6)]

TILE = 16
VOX_ROW, SCAN_ROW, POSE_ROW = 9, 10, 12
CONTRACT_LAST = (((1,), (1,)), ((), ()))


def split(x):
    high = x.astype(jnp.bfloat16).astype(jnp.float32)
    rest = x - high
    mid = rest.astype(jnp.bfloat16).astype(jnp.float32)
    return jnp.concatenate([high, mid, rest - mid], axis=0).astype(jnp.bfloat16)


def joined(y):
    rows = y.shape[0] // 3
    return y[:rows] + y[rows : 2 * rows] + y[2 * rows :]


def group_turn(pieces, out_group, group, lanes_per):
    total = None
    for a, piece in enumerate(pieces):
        shift = ((a - out_group) * lanes_per) % LANES
        moved = piece if shift == 0 else pltpu.roll(piece, shift, 1)
        total = moved if total is None else jnp.where(group == a, moved, total)
    return total


def loop(count, body):
    if count <= 8:
        for i in range(count):
            body(i)
    else:
        def step(i, carry):
            body(i)
            return carry

        lax.fori_loop(0, count, step, 0)


def summed(count, body, rows, columns):
    acc = jnp.zeros((rows, columns), jnp.float32)
    if count <= 8:
        for i in range(count):
            acc = acc + body(i)
        return acc
    return lax.fori_loop(0, count, lambda i, total: total + body(i), acc)


def aligned(start, size, unit=8):
    if not isinstance(start, int):
        start = pl.multiple_of(start, unit)
    return pl.ds(start, size)


def kernel(
    sizes,
    points,
    poses,
    angles,
    voxel_ids,
    scan_ids,
    hess_out,
    grad_out,
    cost_out,
    pts,
    pose_in,
    angle_in,
    vox_in,
    scan_in,
    pose_pad,
    sent,
    send1,
    recv1,
    send_n,
    recv_n,
    scan_hot,
    vox_hot,
    table,
    world,
    send_a,
    recv_a,
    total_a,
    normals,
    quads,
    send_q,
    recv_q,
    terms,
    late,
    send_h,
    recv_h,
    send_g,
    recv_g,
    lines,
    pts_sem,
    in_sem,
    sends,
    recvs,
):
    n_tm, n_map, slots, npoints, scale = sizes
    blocks = pts.shape[1]
    chunks = blocks // LANES
    per = LANES // slots
    own_scans = pose_in.shape[1]
    spread = LANES // own_scans
    scans = own_scans * n_map
    wide = scans // LANES
    voxels = angle_in.shape[1]
    halves = voxels // LANES
    parts = n_tm // per
    arrived = n_map * parts
    pairs = arrived // 2
    message = parts * TILE
    a_rows = 2 * n_tm
    tm = lax.axis_index("tm")
    mp = lax.axis_index("map")
    f32, bf16 = jnp.float32, jnp.bfloat16

    small = [
        pltpu.make_async_copy(src, dst, in_sem.at[i])
        for i, (src, dst) in enumerate(
            [(poses, pose_in), (angles, angle_in), (voxel_ids, vox_in), (scan_ids, scan_in)]
        )
    ]
    loads = pts_sem.shape[0]
    span = blocks // loads

    def points_copy(r):
        rows = pl.ds(r * span, span)
        return pltpu.make_async_copy(points.at[:, rows, :], pts.at[:, rows, :], pts_sem.at[r])

    for copy in small:
        copy.start()
    loop(loads, lambda r: points_copy(r).start())
    barrier = pltpu.get_barrier_semaphore()
    plane = [(tm, lax.rem(mp + i, n_map)) for i in range(1, n_map)]
    column = [(lax.rem(tm + i, n_tm), mp) for i in range(1, n_tm)]
    for peer in column + plane:
        pl.semaphore_signal(barrier, inc=1, device_id=peer, device_id_type=MESH)

    def send(source, dest, peer, s):
        pltpu.make_async_remote_copy(
            src_ref=source,
            dst_ref=dest,
            send_sem=sends.at[0],
            recv_sem=recvs.at[s],
            device_id=peer,
            device_id_type=MESH,
        ).start()

    def wait_rows(rows, sem):
        ref = pts.at[0, pl.ds(0, rows), :]
        pltpu.make_async_copy(ref, ref, sem).wait()

    def every(ref, k, stride, count=arrived):
        return ref[pl.ds(k, count, stride=stride), :]

    lane = lax.broadcasted_iota(jnp.int32, (8, LANES), 1)
    group = lane // slots
    chunk_of = lax.broadcasted_iota(jnp.int32, (arrived, LANES), 0)
    turn_of = (
        lax.broadcasted_iota(jnp.int32, (arrived, LANES), 1) // slots + per * lax.rem(chunk_of, parts)
    )
    own_turn = [turn_of == t for t in range(n_tm)]
    for t in range(n_tm):
        world[pl.ds(3 * n_tm + t, arrived, stride=4 * n_tm), :] = jnp.where(own_turn[t], 1.0, 0.0)
    sent[...] = jnp.zeros_like(sent)
    quads[...] = jnp.zeros_like(quads)
    late[...] = jnp.zeros_like(late)
    pose_pad[...] = jnp.zeros_like(pose_pad)
    lines[...] = jnp.zeros_like(lines)

    for copy in small:
        copy.wait()
    for g in range(spread):
        pose_pad[0:6, g * own_scans : (g + 1) * own_scans] = pose_in[...]
    pose = pose_pad[...]
    cos, sin = jnp.cos(pose), jnp.sin(pose)
    cx, cy, cz = cos[0:1], cos[1:2], cos[2:3]
    sx, sy, sz = sin[0:1], sin[1:2], sin[2:3]
    pose_rows = [
        [cz * cy, cz * sy * sx - sz * cx, cz * sy * cx + sz * sx],
        [sz * cy, sz * sy * sx + cz * cx, sz * sy * cx - cz * sx],
        [-sy, cy * sx, cy * cx],
        [pose[3:4], pose[4:5], pose[5:6]],
    ]
    scan_group = lane[0:1] // own_scans
    pose_lines = []
    for q in range(3):
        line = pose_rows[0][q]
        for g in range(1, 4):
            line = jnp.where(scan_group == g, pose_rows[g][q], line)
        pose_lines.append(line)

    ids = vox_in[...]
    row_of = lax.broadcasted_iota(jnp.int32, ids.shape, 0)
    lane_of = lax.broadcasted_iota(jnp.int32, ids.shape, 1)
    owner_of = row_of * per + lane_of // slots
    local_ids = jnp.where(ids >= 0, ids - owner_of * voxels, -1).astype(f32)
    sent[pl.ds(VOX_ROW, chunks, stride=TILE), :] = local_ids
    sent[pl.ds(SCAN_ROW, chunks, stride=TILE), :] = scan_in[...].astype(f32)

    theta, phi = angle_in[0:1, :], angle_in[1:2, :]
    sin_theta = jnp.sin(theta)
    own_normal = [sin_theta * jnp.cos(phi), sin_theta * jnp.sin(phi), jnp.cos(theta)]
    for c in range(3):
        for h in range(halves):
            k = c * halves + h
            send_n[k : k + 1, :] = own_normal[c][:, h * LANES : (h + 1) * LANES]

    def raw_moments(r):
        at = aligned(r * LANES, LANES, LANES)
        xyz = [pts[i, at, :].T for i in range(3)]
        sums = [jnp.sum(x, axis=0, keepdims=True) for x in xyz]
        sums += [jnp.sum(xyz[i] * xyz[j], axis=0, keepdims=True) for i, j in PAIRS]
        for k, row in enumerate(sums):
            sent[pl.ds(r * TILE + k, 1), :] = row

    def load_step(r):
        points_copy(r).wait()
        for i in range(span // LANES):
            raw_moments(r * (span // LANES) + i)

    loop(loads, load_step)
    row_chunks = n_map // per

    def pack(peer_row):
        for g in range(per):
            peer = peer_row * per + g
            for u in range(parts):
                for half in range(2):
                    pieces = [
                        sent[
                            aligned(
                                ((u * per + a) * row_chunks + peer_row) * TILE + 8 * half, 8
                            ),
                            :,
                        ]
                        for a in range(per)
                    ]
                    at = aligned(peer * message + u * TILE + 8 * half, 8)
                    send1[at, :] = group_turn(pieces, g, group, slots)
            for q in range(3):
                send1[pl.ds(peer * message + POSE_ROW + q, 1), :] = pose_lines[q]

    loop(row_chunks, pack)

    pl.semaphore_wait(barrier, n_map - 1 + n_tm - 1)
    mine = aligned(mp * message, message)
    for peer in plane:
        send(send1.at[aligned(peer[1] * message, message), :], recv1.at[mine, :], peer, 0)
    n_size = send_n.shape[0]
    n_mine = aligned(tm * n_size, n_size)
    for peer in column:
        send(send_n, recv_n.at[n_mine, :], peer, 1)
    recv1[mine, :] = send1[mine, :]
    recv_n[n_mine, :] = send_n[...]
    wait_rows((n_map - 1) * message, recvs.at[0])

    def pair_row(p, k):
        return jnp.concatenate(
            [recv1[pl.ds((2 * p + i) * TILE + k, 1), :] for i in range(2)], axis=1
        )

    scan_iota = lax.broadcasted_iota(jnp.int32, (scans, 2 * LANES), 0).astype(f32)
    vox_iota = lax.broadcasted_iota(jnp.int32, (voxels, 2 * LANES), 0).astype(f32)

    def mark(p):
        scan_hot[p] = jnp.where(pair_row(p, SCAN_ROW) == scan_iota, 1.0, 0.0).astype(bf16)
        vox_hot[p] = jnp.where(pair_row(p, VOX_ROW) == vox_iota, 1.0, 0.0).astype(bf16)

    top = lax.broadcasted_iota(jnp.int32, (8, LANES), 0) < 4
    columns = []
    for h in range(wide):
        tiles = [recv1[(h * spread + a) * message + 8 : (h * spread + a) * message + 16, :] for a in range(spread)]
        turned = [group_turn(tiles, g, group, own_scans) for g in range(4)]
        low = jnp.where(top, pltpu.roll(turned[1], 4, 0), turned[0])
        high = jnp.where(top, pltpu.roll(turned[3], 4, 0), turned[2])
        columns.append(jnp.concatenate([low, high], axis=0))
    pose_table = split(jnp.concatenate(columns, axis=1))
    table_row = {}
    for q in range(3):
        table_row[(1, q)], table_row[(0, q)] = q, 4 + q
        table_row[(3, q)], table_row[(2, q)] = 8 + q, 12 + q

    def look_up(p):
        mark(p)
        found = joined(jnp.dot(pose_table, scan_hot[p], preferred_element_type=f32))
        for i in range(2):
            table[aligned((2 * p + i) * TILE, TILE), :] = found[:, i * LANES : (i + 1) * LANES]

    loop(pairs, look_up)
    rot = [[every(table, table_row[(i, j)], TILE) for j in range(3)] for i in range(3)]
    shift = [every(table, table_row[(3, j)], TILE) for j in range(3)]
    first = [every(recv1, k, TILE) for k in range(3)]
    turned_first = [sum(rot[i][j] * first[j] for j in range(3)) for i in range(3)]
    m1 = [turned_first[i] + npoints * shift[i] for i in range(3)]
    for c in range(3):
        for t in range(n_tm):
            world[pl.ds(c * n_tm + t, arrived, stride=4 * n_tm), :] = jnp.where(
                own_turn[t], m1[c], 0.0
            )

    def pair_tile(ref, p, rows):
        return jnp.concatenate(
            [ref[aligned((2 * p + i) * rows, rows), :] for i in range(2)], axis=1
        )

    def add_voxels(p):
        return lax.dot_general(
            split(pair_tile(world, p, 4 * n_tm)), vox_hot[p], CONTRACT_LAST,
            preferred_element_type=f32,
        )

    sums = joined(summed(pairs, add_voxels, 12 * n_tm, voxels))
    wait_rows((n_tm - 1) * n_size, recvs.at[1])
    normal = [
        jnp.concatenate(
            [every(recv_n, c * halves + h, n_size, n_tm) for h in range(halves)], axis=1
        )
        for c in range(3)
    ]
    along = sum(normal[c] * sums[c * n_tm : (c + 1) * n_tm] for c in range(3))
    count = sums[3 * n_tm : 4 * n_tm]
    for h in range(halves):
        at = slice(h * LANES, (h + 1) * LANES)
        send_a[h * a_rows : h * a_rows + n_tm, :] = along[:, at]
        send_a[h * a_rows + n_tm : (h + 1) * a_rows, :] = count[:, at]

    a_size = halves * a_rows
    a_mine = aligned(tm * a_size, a_size)
    for peer in column:
        send(send_a, recv_a.at[a_mine, :], peer, 2)
    recv_a[a_mine, :] = send_a[...]

    normal_table = split(jnp.concatenate(normal + [jnp.zeros_like(count)], axis=0))

    def find_normals(p):
        found = joined(jnp.dot(normal_table, vox_hot[p], preferred_element_type=f32))
        for i in range(2):
            normals[aligned((2 * p + i) * 4 * n_tm, 4 * n_tm), :] = found[
                :, i * LANES : (i + 1) * LANES
            ]

    loop(pairs, find_normals)
    n = []
    for c in range(3):
        value = every(normals, c * n_tm, 4 * n_tm)
        for t in range(1, n_tm):
            value = jnp.where(own_turn[t], every(normals, c * n_tm + t, 4 * n_tm), value)
        n.append(value)
    second = [every(recv1, 3 + k, TILE) for k in range(6)]
    half_turned = [
        [sum(rot[i][k] * second[PAIR_ROW[(k, j)]] for k in range(3)) for j in range(3)]
        for i in range(3)
    ]
    m2 = [
        sum(half_turned[i][k] * rot[j][k] for k in range(3))
        + turned_first[i] * shift[j]
        + shift[i] * m1[j]
        for i, j in PAIRS
    ]
    quad = sum(n[i] ** 2 * m2[i] for i in range(3)) + 2.0 * sum(
        n[PAIRS[k][0]] * n[PAIRS[k][1]] * m2[k] for k in range(3, 6)
    )
    for t in range(n_tm):
        quads[pl.ds(t, arrived, stride=8), :] = jnp.where(own_turn[t], quad, 0.0)

    def add_quads(p):
        return lax.dot_general(
            split(pair_tile(quads, p, 8)), vox_hot[p], CONTRACT_LAST, preferred_element_type=f32
        )

    quad_sums = joined(summed(pairs, add_quads, 24, voxels))
    for t in range(n_tm):
        for h in range(halves):
            send_q[t, h : h + 1, :] = quad_sums[t : t + 1, h * LANES : (h + 1) * LANES]
    for peer in column:
        send(send_q.at[peer[0]], recv_q.at[tm], peer, 3)
    recv_q[tm] = send_q[tm]

    def skew(v):
        return [n[2] * v[1] - n[1] * v[2], n[0] * v[2] - n[2] * v[0], n[1] * v[0] - n[0] * v[1]]

    full = [[m2[PAIR_ROW[(i, j)]] for j in range(3)] for i in range(3)]
    skewed = [skew([full[k][j] for k in range(3)]) for j in range(3)]
    left = [[skewed[j][i] for j in range(3)] for i in range(3)]
    corner_block = [skew(left[i]) for i in range(3)]
    skew_first = skew(m1)
    found = {}
    for i in range(3):
        for j in range(3):
            if j >= i:
                found[("h", i, j)] = corner_block[i][j]
                found[("h", 3 + i, 3 + j)] = npoints * n[i] * n[j]
            found[("h", i, 3 + j)] = skew_first[i] * n[j]
    rest = n[0] * m1[0] + n[1] * m1[1] + n[2] * m1[2]
    for i in range(3):
        found[("g", i)] = sum(left[i][j] * n[j] for j in range(3))
        found[("g", 3 + i)] = n[i] * rest
        late[pl.ds(i, arrived, stride=8), :] = skew_first[i]
        late[pl.ds(3 + i, arrived, stride=8), :] = npoints * n[i]
    for name, value in found.items():
        terms[pl.ds(ROWS.index(name), arrived, stride=32), :] = value
    for k in range(len(found), 32):
        terms[pl.ds(k, arrived, stride=32), :] = jnp.zeros_like(rest)

    def add_scans(p):
        return lax.dot_general(
            split(pair_tile(terms, p, 32)), scan_hot[p], CONTRACT_LAST, preferred_element_type=f32
        )

    per_scan = joined(summed(pairs, add_scans, 96, scans)) * scale
    own_group = lane // own_scans
    for h in range(wide):
        pieces = [per_scan[8 * c : 8 * c + 8, h * LANES : (h + 1) * LANES] for c in range(4)]
        for b in range(spread):
            at = (h * spread + b) * 8
            send_h[at : at + 8, :] = group_turn(pieces, b, own_group, own_scans)
    eight = aligned(mp * 8, 8)
    for peer in plane:
        send(send_h.at[aligned(peer[1] * 8, 8), :], recv_h.at[eight, :], peer, 4)
    recv_h[eight, :] = send_h[eight, :]

    wait_rows((n_tm - 1) * a_size, recvs.at[2])
    offsets = []
    for h in range(halves):
        total = recv_a[h * a_rows : (h + 1) * a_rows, :]
        for t in range(1, n_tm):
            total = total + recv_a[t * a_size + h * a_rows : t * a_size + (h + 1) * a_rows, :]
        floor = jnp.maximum(total[n_tm:] * npoints, 1.0)
        offset = total[:n_tm] / floor
        total_a[h * a_rows : h * a_rows + n_tm, :] = offset
        total_a[h * a_rows + n_tm : (h + 1) * a_rows, :] = floor
        offsets.append(offset)
    offset = jnp.concatenate(offsets, axis=1)
    if n_tm % 8:
        offset = jnp.concatenate([offset, jnp.zeros((8 - n_tm % 8, voxels), f32)], axis=0)
    offset_table = split(offset)
    d_rows = offset.shape[0]
    turn_row = lax.broadcasted_iota(jnp.int32, (d_rows, 2 * LANES), 0)
    turn_lane = lax.rem(lax.broadcasted_iota(jnp.int32, (d_rows, 2 * LANES), 1), LANES) // slots

    def add_late(p):
        value = joined(jnp.dot(offset_table, vox_hot[p], preferred_element_type=f32))
        turn = turn_lane
        if parts > 1:
            in_pair = lax.broadcasted_iota(jnp.int32, (d_rows, 2 * LANES), 1) // LANES
            turn = turn_lane + per * lax.rem(2 * p + in_pair, parts)
        d = jnp.sum(jnp.where(turn_row == turn, value, 0.0), axis=0, keepdims=True)
        return lax.dot_general(
            split(pair_tile(late, p, 8) * d), scan_hot[p], CONTRACT_LAST,
            preferred_element_type=f32,
        )

    moved = joined(summed(pairs, add_late, 24, scans)) * scale
    for h in range(wide):
        send_g[h * 8 : h * 8 + 8, :] = moved[:, h * LANES : (h + 1) * LANES]
    for peer in plane:
        source = send_g.at[aligned(peer[1] // spread * 8, 8), :]
        send(source, recv_g.at[eight, :], peer, 5)
    recv_g[eight, :] = send_g[aligned(mp // spread * 8, 8), :]

    wait_rows((n_map - 1) * 8, recvs.at[4])
    total = recv_h[0:8, :]
    for m in range(1, n_map):
        total = total + recv_h[m * 8 : m * 8 + 8, :]
    lined = [total] + [pltpu.roll(total, LANES - own_scans * c, 1) for c in range(1, 4)]

    def row_at(name):
        k = ROWS.index(name)
        return lined[k // 8][k % 8 : k % 8 + 1]

    for i in range(6):
        for j in range(6):
            lines[6 * i + j : 6 * i + j + 1, :] = row_at(("h", min(i, j), max(i, j)))
    hess_out[...] = lines[...].T[0:own_scans, 0:36]
    gradient = jnp.concatenate([row_at(("g", i)) for i in range(6)], axis=0)

    pltpu.make_async_copy(
        recv_q.at[pl.ds(0, n_tm - 1)], recv_q.at[pl.ds(0, n_tm - 1)], recvs.at[3]
    ).wait()
    quad_total = recv_q[0]
    for t in range(1, n_tm):
        quad_total = quad_total + recv_q[t]
    own_offset = total_a[pl.ds(tm, halves, stride=a_rows), :]
    own_floor = total_a[pl.ds(n_tm + tm, halves, stride=a_rows), :]
    cost = quad_total / own_floor - own_offset**2
    for h in range(halves):
        cost_out[:, h * LANES : (h + 1) * LANES] = cost[h : h + 1]

    wait_rows((n_map - 1) * 8, recvs.at[5])
    change = recv_g[0:8, :]
    for m in range(1, n_map):
        change = change + recv_g[m * 8 : m * 8 + 8, :]
    change = pltpu.roll(change, LANES - own_scans * lax.rem(mp, spread), 1)
    grad_out[...] = (gradient - change[0:6])[:, 0:own_scans]

    rows_sent = (n_map - 1) * (message + 16) + (n_tm - 1) * (n_size + a_size + halves)
    wait_rows(rows_sent, sends.at[0])


def finish(hess_in, grad_in, cost_in, hess_out, grad_out, cost_out, sems):
    copies = [
        pltpu.make_async_copy(src, dst, sems.at[i])
        for i, (src, dst) in enumerate(
            [(hess_in, hess_out), (grad_in, grad_out), (cost_in, cost_out)]
        )
    ]
    for copy in copies:
        copy.start()
    for copy in copies:
        copy.wait()


def local(points, poses, normal_angles, voxel_ids, scan_ids):
    blocks, npoints = points.shape[1:]
    n_tm, n_map = lax.axis_size("tm"), lax.axis_size("map")
    devices = n_tm * n_map
    slots = blocks // devices
    chunks = blocks // LANES
    vox_count = normal_angles.shape[1]
    own_scans = poses.shape[1]
    assert npoints == LANES and slots * 4 == LANES and own_scans * 4 == LANES
    assert n_map % 4 == 0 and n_tm % 4 == 0 and vox_count % LANES == 0
    scale = own_scans * devices / (blocks * devices * npoints)
    f32, bf16 = jnp.float32, jnp.bfloat16
    scans = own_scans * n_map
    halves = vox_count // LANES
    arrived = n_map * n_tm // 4
    n_rows = -(-3 * halves // 8) * 8
    a_rows = 2 * n_tm * halves
    hbm = pl.BlockSpec(memory_space=pl.ANY)
    vmem = pl.BlockSpec(memory_space=pltpu.VMEM)
    shapes = [(own_scans, 36), (6, own_scans), (1, vox_count)]
    results = pl.pallas_call(
        functools.partial(kernel, (n_tm, n_map, slots, float(npoints), scale)),
        out_shape=tuple(pltpu.VMEM(shape, f32) for shape in shapes),
        in_specs=[hbm] * 5,
        out_specs=(vmem,) * 3,
        scratch_shapes=[
            pltpu.VMEM(points.shape, f32),
            pltpu.VMEM(poses.shape, f32),
            pltpu.VMEM(normal_angles.shape, f32),
            pltpu.VMEM((chunks, LANES), jnp.int32),
            pltpu.VMEM((chunks, LANES), jnp.int32),
            pltpu.VMEM((8, LANES), f32),
            pltpu.VMEM((chunks * TILE, LANES), f32),
            pltpu.VMEM((arrived * TILE, LANES), f32),
            pltpu.VMEM((arrived * TILE, LANES), f32),
            pltpu.VMEM((n_rows, LANES), f32),
            pltpu.VMEM((n_tm * n_rows, LANES), f32),
            pltpu.VMEM((arrived // 2, scans, 2 * LANES), bf16),
            pltpu.VMEM((arrived // 2, vox_count, 2 * LANES), bf16),
            pltpu.VMEM((arrived * TILE, LANES), f32),
            pltpu.VMEM((arrived * 4 * n_tm, LANES), f32),
            pltpu.VMEM((a_rows, LANES), f32),
            pltpu.VMEM((n_tm * a_rows, LANES), f32),
            pltpu.VMEM((a_rows, LANES), f32),
            pltpu.VMEM((arrived * 4 * n_tm, LANES), f32),
            pltpu.VMEM((arrived * 8, LANES), f32),
            pltpu.VMEM((n_tm, halves, LANES), f32),
            pltpu.VMEM((n_tm, halves, LANES), f32),
            pltpu.VMEM((arrived * 32, LANES), f32),
            pltpu.VMEM((arrived * 8, LANES), f32),
            pltpu.VMEM((n_map * 8, LANES), f32),
            pltpu.VMEM((n_map * 8, LANES), f32),
            pltpu.VMEM((scans // LANES * 8, LANES), f32),
            pltpu.VMEM((n_map * 8, LANES), f32),
            pltpu.VMEM((LANES, LANES), f32),
            pltpu.SemaphoreType.DMA((4,)),
            pltpu.SemaphoreType.DMA((4,)),
            pltpu.SemaphoreType.DMA((1,)),
            pltpu.SemaphoreType.DMA((6,)),
        ],
        compiler_params=pltpu.CompilerParams(collective_id=0, has_side_effects=True),
    )(
        points,
        poses,
        normal_angles,
        voxel_ids.reshape(chunks, LANES),
        scan_ids.reshape(chunks, LANES),
    )
    hess, grad, cost = pl.pallas_call(
        finish,
        out_shape=tuple(jax.ShapeDtypeStruct(shape, f32) for shape in shapes),
        in_specs=[vmem] * 3,
        out_specs=(hbm,) * 3,
        scratch_shapes=[pltpu.SemaphoreType.DMA((3,))],
    )(*[pltpu.with_memory_space_constraint(x, pltpu.VMEM) for x in results])
    return hess.T, grad, cost.reshape(vox_count)


def solution(mesh):
    return jax.shard_map(
        local,
        mesh=mesh,
        in_specs=(
            P(None, ("tm", "map"), None),
            P(None, ("tm", "map")),
            P(None, ("tm", "map")),
            P(("tm", "map")),
            P(("tm", "map")),
        ),
        out_specs=(P(None, ("tm", "map")), P(None, ("tm", "map")), P(("tm", "map"))),
        check_vma=False,
    )
```

```python
import functools

import jax
import jax.numpy as jnp
from jax import lax
from jax.experimental import pallas as pl
from jax.experimental.pallas import tpu as pltpu
from jax.sharding import PartitionSpec as P

LANES = 128
MESH = pl.DeviceIdType.MESH
PAIRS = [(0, 0), (1, 1), (2, 2), (0, 1), (0, 2), (1, 2)]
PAIR_ROW = {}
for _k, (_i, _j) in enumerate(PAIRS):
    PAIR_ROW[(_i, _j)] = _k
    PAIR_ROW[(_j, _i)] = _k

ROWS = [("h", i, j) for i in range(6) for j in range(i, 6)] + [("g", i) for i in range(6)]

TILE = 16
VOX_ROW, SCAN_ROW, POSE_ROW = 9, 10, 12
SHARE = 2
CONTRACT_LAST = (((1,), (1,)), ((), ()))


def split(x):
    high = x.astype(jnp.bfloat16).astype(jnp.float32)
    rest = x - high
    mid = rest.astype(jnp.bfloat16).astype(jnp.float32)
    return jnp.concatenate([high, mid, rest - mid], axis=0).astype(jnp.bfloat16)


def joined(y):
    rows = y.shape[0] // 3
    return y[:rows] + y[rows : 2 * rows] + y[2 * rows :]


def group_turn(pieces, out_group, group, lanes_per):
    total = None
    for a, piece in enumerate(pieces):
        shift = ((a - out_group) * lanes_per) % LANES
        moved = piece if shift == 0 else pltpu.roll(piece, shift, 1)
        total = moved if total is None else jnp.where(group == a, moved, total)
    return total


def loop(count, body):
    if count <= 8:
        for i in range(count):
            body(i)
    else:
        def step(i, carry):
            body(i)
            return carry

        lax.fori_loop(0, count, step, 0)


def summed(count, body, rows, columns):
    acc = jnp.zeros((rows, columns), jnp.float32)
    if count <= 8:
        for i in range(count):
            acc = acc + body(i)
        return acc
    return lax.fori_loop(0, count, lambda i, total: total + body(i), acc)


def aligned(start, size, unit=8):
    if not isinstance(start, int):
        start = pl.multiple_of(start, unit)
    return pl.ds(start, size)


def kernel(
    sizes,
    points,
    poses,
    angles,
    voxel_ids,
    scan_ids,
    hess_out,
    grad_out,
    cost_out,
    pts,
    pose_in,
    angle_in,
    vox_in,
    scan_in,
    pose_pad,
    sent,
    send1,
    recv1,
    pair_n,
    recv_n,
    scan_hot,
    vox_hot,
    table,
    world,
    send_a,
    recv_a,
    total_a,
    normals,
    quads,
    send_q,
    recv_q,
    send_c,
    recv_c,
    terms,
    late,
    send_h,
    recv_h,
    send_g,
    recv_g,
    lines,
    pts_sem,
    in_sem,
    sends,
    recvs,
):
    n_tm, n_map, slots, npoints, scale = sizes
    reducers = n_map // SHARE
    blocks = pts.shape[1]
    chunks = blocks // LANES
    per = LANES // slots
    own_scans = pose_in.shape[1]
    spread = LANES // own_scans
    scans = own_scans * n_map
    wide = scans // LANES
    voxels = angle_in.shape[1]
    halves = voxels // LANES
    parts = n_tm // per
    step = SHARE * parts
    arrived = n_map * step
    couples = n_map // 2 * parts
    message = step * TILE
    n_size = pair_n.shape[0] // SHARE
    a_rows = 2 * n_tm
    a_size = SHARE * halves * a_rows
    tm = lax.axis_index("tm")
    mp = lax.axis_index("map")
    rd = mp // SHARE
    part = lax.rem(mp, SHARE)
    reduces = part == SHARE - 1
    f32, bf16 = jnp.float32, jnp.bfloat16

    small = [
        pltpu.make_async_copy(src, dst, in_sem.at[i])
        for i, (src, dst) in enumerate(
            [(poses, pose_in), (angles, angle_in), (voxel_ids, vox_in), (scan_ids, scan_in)]
        )
    ]
    loads = pts_sem.shape[0]
    span = blocks // loads

    def points_copy(r):
        rows = pl.ds(r * span, span)
        return pltpu.make_async_copy(points.at[:, rows, :], pts.at[:, rows, :], pts_sem.at[r])

    for copy in small:
        copy.start()
    loop(loads, lambda r: points_copy(r).start())
    barrier = pltpu.get_barrier_semaphore()
    near = (tm, rd * SHARE + SHARE - 1)
    first_of = (tm, rd * SHARE)
    plane = [(tm, lax.rem(mp + i, n_map)) for i in range(1, n_map)]
    column = [(lax.rem(tm + i, n_tm), mp) for i in range(1, n_tm)]
    others = [lax.rem(rd + i, reducers) for i in range(1, reducers)]

    def greet(peer):
        pl.semaphore_signal(barrier, inc=1, device_id=peer, device_id_type=MESH)

    @pl.when(reduces)
    def _():
        for peer in column + plane:
            greet(peer)

    @pl.when(jnp.logical_not(reduces))
    def _():
        for other in others:
            greet((tm, other * SHARE + SHARE - 1))
        greet(near)

    def send(source, dest, peer, s):
        pltpu.make_async_remote_copy(
            src_ref=source,
            dst_ref=dest,
            send_sem=sends.at[0],
            recv_sem=recvs.at[s],
            device_id=peer,
            device_id_type=MESH,
        ).start()

    def wait_rows(rows, sem):
        ref = pts.at[0, pl.ds(0, rows), :]
        pltpu.make_async_copy(ref, ref, sem).wait()

    def every(ref, k, stride, count=arrived):
        return ref[pl.ds(k, count, stride=stride), :]

    lane = lax.broadcasted_iota(jnp.int32, (8, LANES), 1)
    group = lane // slots
    chunk_of = lax.broadcasted_iota(jnp.int32, (arrived, LANES), 0)
    turn_of = (
        lax.broadcasted_iota(jnp.int32, (arrived, LANES), 1) // slots + per * lax.rem(chunk_of, parts)
    )
    own_turn = [turn_of == t for t in range(n_tm)]
    sent[...] = jnp.zeros_like(sent)

    for copy in small:
        copy.wait()
    pose_pad[...] = jnp.zeros_like(pose_pad)
    for g in range(spread):
        pose_pad[0:6, g * own_scans : (g + 1) * own_scans] = pose_in[...]
    pose = pose_pad[...]
    cos, sin = jnp.cos(pose), jnp.sin(pose)
    cx, cy, cz = cos[0:1], cos[1:2], cos[2:3]
    sx, sy, sz = sin[0:1], sin[1:2], sin[2:3]
    pose_rows = [
        [cz * cy, cz * sy * sx - sz * cx, cz * sy * cx + sz * sx],
        [sz * cy, sz * sy * sx + cz * cx, sz * sy * cx - cz * sx],
        [-sy, cy * sx, cy * cx],
        [pose[3:4], pose[4:5], pose[5:6]],
    ]
    scan_group = lane[0:1] // own_scans
    pose_lines = []
    for q in range(3):
        line = pose_rows[0][q]
        for g in range(1, 4):
            line = jnp.where(scan_group == g, pose_rows[g][q], line)
        pose_lines.append(line)

    ids = vox_in[...]
    row_of = lax.broadcasted_iota(jnp.int32, ids.shape, 0)
    lane_of = lax.broadcasted_iota(jnp.int32, ids.shape, 1)
    owner_of = row_of * per + lane_of // slots
    local_ids = jnp.where(ids >= 0, ids - owner_of * voxels, -1).astype(f32)
    sent[pl.ds(VOX_ROW, chunks, stride=TILE), :] = local_ids
    sent[pl.ds(SCAN_ROW, chunks, stride=TILE), :] = scan_in[...].astype(f32)

    theta, phi = angle_in[0:1, :], angle_in[1:2, :]
    sin_theta = jnp.sin(theta)
    own_normal = [sin_theta * jnp.cos(phi), sin_theta * jnp.sin(phi), jnp.cos(theta)]
    n_mine = aligned(part * n_size, n_size)
    for c in range(3):
        for h in range(halves):
            k = part * n_size + c * halves + h
            pair_n[pl.ds(k, 1), :] = own_normal[c][:, h * LANES : (h + 1) * LANES]

    def raw_moments(r):
        at = aligned(r * LANES, LANES, LANES)
        xyz = [pts[i, at, :].T for i in range(3)]
        sums = [jnp.sum(x, axis=0, keepdims=True) for x in xyz]
        sums += [jnp.sum(xyz[i] * xyz[j], axis=0, keepdims=True) for i, j in PAIRS]
        for k, row in enumerate(sums):
            sent[pl.ds(r * TILE + k, 1), :] = row

    def load_step(r):
        points_copy(r).wait()
        for i in range(span // LANES):
            raw_moments(r * (span // LANES) + i)

    loop(loads, load_step)
    row_chunks = n_map // per

    def pack(peer_row):
        for g in range(per):
            peer = peer_row * per + g
            for u in range(parts):
                for half in range(2):
                    pieces = [
                        sent[
                            aligned(
                                ((u * per + a) * row_chunks + peer_row) * TILE + 8 * half, 8
                            ),
                            :,
                        ]
                        for a in range(per)
                    ]
                    at = aligned((peer * parts + u) * TILE + 8 * half, 8)
                    send1[at, :] = group_turn(pieces, g, group, slots)
            for q in range(3):
                send1[pl.ds(peer * parts * TILE + POSE_ROW + q, 1), :] = pose_lines[q]

    loop(row_chunks, pack)

    from_plane = n_map - 1 + n_tm - 1
    pl.semaphore_wait(barrier, jnp.where(reduces, from_plane, reducers))
    mine = aligned(mp * message, message)

    def message_of(other):
        return send1.at[aligned(other * message, message), :]

    @pl.when(jnp.logical_not(reduces))
    def _():
        send(pair_n.at[n_mine, :], pair_n.at[n_mine, :], near, 6)

    for other in others:
        send(message_of(other), recv1.at[mine, :], (tm, other * SHARE + SHARE - 1), 0)

    @pl.when(jnp.logical_not(reduces))
    def _():
        send(message_of(rd), recv1.at[mine, :], near, 0)

    eight = aligned(rd * 8, 8)

    def reduce_part():
        wait_rows(n_size, recvs.at[6])
        n_column = aligned(tm * SHARE * n_size, SHARE * n_size)
        for peer in column:
            send(pair_n, recv_n.at[n_column, :], peer, 1)
        recv1[mine, :] = send1[aligned(rd * message, message), :]
        recv_n[n_column, :] = pair_n[...]
        for t in range(n_tm):
            world[pl.ds(3 * n_tm + t, arrived, stride=4 * n_tm), :] = jnp.where(
                own_turn[t], 1.0, 0.0
            )
        quads[...] = jnp.zeros_like(quads)
        late[...] = jnp.zeros_like(late)
        wait_rows((n_map - 1) * message, recvs.at[0])

        def chunk(k, q, side):
            i, u = (q // parts, q % parts) if isinstance(q, int) else (q // parts, lax.rem(q, parts))
            return ((2 * i + side) * SHARE + k) * parts + u

        def couple_row(k, q, row):
            return jnp.concatenate(
                [recv1[pl.ds(chunk(k, q, side) * TILE + row, 1), :] for side in range(2)], axis=1
            )

        def couple_tile(ref, k, q, rows):
            return jnp.concatenate(
                [ref[aligned(chunk(k, q, side) * rows, rows), :] for side in range(2)], axis=1
            )

        def spread_out(ref, k, q, rows, value):
            for side in range(2):
                ref[aligned(chunk(k, q, side) * rows, rows), :] = value[
                    :, side * LANES : (side + 1) * LANES
                ]

        def each_couple(body):
            for k in range(SHARE):
                loop(couples, functools.partial(body, k))

        scan_iota = lax.broadcasted_iota(jnp.int32, (scans, 2 * LANES), 0).astype(f32)
        vox_iota = lax.broadcasted_iota(jnp.int32, (voxels, 2 * LANES), 0).astype(f32)

        def mark(k, q):
            scan_hot[k * couples + q] = jnp.where(
                couple_row(k, q, SCAN_ROW) == scan_iota, 1.0, 0.0
            ).astype(bf16)
            vox_hot[k * couples + q] = jnp.where(
                couple_row(k, q, VOX_ROW) == vox_iota, 1.0, 0.0
            ).astype(bf16)

        top = lax.broadcasted_iota(jnp.int32, (8, LANES), 0) < 4
        own_group = lane // own_scans
        columns = []
        for h in range(wide):
            at = [(h * spread + a) * message + 8 for a in range(spread)]
            tiles = [recv1[row : row + 8, :] for row in at]
            turned = [group_turn(tiles, g, own_group, own_scans) for g in range(4)]
            low = jnp.where(top, pltpu.roll(turned[1], 4, 0), turned[0])
            high = jnp.where(top, pltpu.roll(turned[3], 4, 0), turned[2])
            columns.append(jnp.concatenate([low, high], axis=0))
        pose_table = split(jnp.concatenate(columns, axis=1))
        table_row = {}
        for q in range(3):
            table_row[(1, q)], table_row[(0, q)] = q, 4 + q
            table_row[(3, q)], table_row[(2, q)] = 8 + q, 12 + q

        def look_up(k, q):
            mark(k, q)
            found = jnp.dot(pose_table, scan_hot[k * couples + q], preferred_element_type=f32)
            spread_out(table, k, q, TILE, joined(found))

        each_couple(look_up)
        rot = [[every(table, table_row[(i, j)], TILE) for j in range(3)] for i in range(3)]
        shift = [every(table, table_row[(3, j)], TILE) for j in range(3)]
        first = [every(recv1, k, TILE) for k in range(3)]
        turned_first = [sum(rot[i][j] * first[j] for j in range(3)) for i in range(3)]
        m1 = [turned_first[i] + npoints * shift[i] for i in range(3)]
        for c in range(3):
            for t in range(n_tm):
                world[pl.ds(c * n_tm + t, arrived, stride=4 * n_tm), :] = jnp.where(
                    own_turn[t], m1[c], 0.0
                )

        def voxel_sums(ref, rows, k):
            def add(q):
                return lax.dot_general(
                    split(couple_tile(ref, k, q, rows)),
                    vox_hot[k * couples + q],
                    CONTRACT_LAST,
                    preferred_element_type=f32,
                )

            return joined(summed(couples, add, 3 * rows, voxels))

        sums = [voxel_sums(world, 4 * n_tm, k) for k in range(SHARE)]
        wait_rows((n_tm - 1) * SHARE * n_size, recvs.at[1])
        normal = [
            [
                jnp.concatenate(
                    [
                        every(recv_n, k * n_size + c * halves + h, SHARE * n_size, n_tm)
                        for h in range(halves)
                    ],
                    axis=1,
                )
                for c in range(3)
            ]
            for k in range(SHARE)
        ]
        for k in range(SHARE):
            along = sum(normal[k][c] * sums[k][c * n_tm : (c + 1) * n_tm] for c in range(3))
            count = sums[k][3 * n_tm : 4 * n_tm]
            for h in range(halves):
                at = slice(h * LANES, (h + 1) * LANES)
                base = (k * halves + h) * a_rows
                send_a[base : base + n_tm, :] = along[:, at]
                send_a[base + n_tm : base + a_rows, :] = count[:, at]

        a_mine = aligned(tm * a_size, a_size)
        for peer in column:
            send(send_a, recv_a.at[a_mine, :], peer, 2)
        recv_a[a_mine, :] = send_a[...]

        normal_table = [
            split(jnp.concatenate(normal[k] + [jnp.zeros_like(normal[k][0])], axis=0))
            for k in range(SHARE)
        ]

        def find_normals(k, q):
            found = jnp.dot(normal_table[k], vox_hot[k * couples + q], preferred_element_type=f32)
            spread_out(normals, k, q, 4 * n_tm, joined(found))

        each_couple(find_normals)
        n = []
        for c in range(3):
            value = every(normals, c * n_tm, 4 * n_tm)
            for t in range(1, n_tm):
                value = jnp.where(own_turn[t], every(normals, c * n_tm + t, 4 * n_tm), value)
            n.append(value)
        second = [every(recv1, 3 + k, TILE) for k in range(6)]
        half_turned = [
            [sum(rot[i][k] * second[PAIR_ROW[(k, j)]] for k in range(3)) for j in range(3)]
            for i in range(3)
        ]
        m2 = [
            sum(half_turned[i][k] * rot[j][k] for k in range(3))
            + turned_first[i] * shift[j]
            + shift[i] * m1[j]
            for i, j in PAIRS
        ]
        quad = sum(n[i] ** 2 * m2[i] for i in range(3)) + 2.0 * sum(
            n[PAIRS[k][0]] * n[PAIRS[k][1]] * m2[k] for k in range(3, 6)
        )
        for t in range(n_tm):
            quads[pl.ds(t, arrived, stride=8), :] = jnp.where(own_turn[t], quad, 0.0)
        for k in range(SHARE):
            quad_sums = voxel_sums(quads, 8, k)
            for t in range(n_tm):
                for h in range(halves):
                    send_q[t, k * halves + h : k * halves + h + 1, :] = quad_sums[
                        t : t + 1, h * LANES : (h + 1) * LANES
                    ]
        for peer in column:
            send(send_q.at[peer[0]], recv_q.at[tm], peer, 3)
        recv_q[tm] = send_q[tm]

        def skew(v):
            return [
                n[2] * v[1] - n[1] * v[2],
                n[0] * v[2] - n[2] * v[0],
                n[1] * v[0] - n[0] * v[1],
            ]

        full = [[m2[PAIR_ROW[(i, j)]] for j in range(3)] for i in range(3)]
        skewed = [skew([full[k][j] for k in range(3)]) for j in range(3)]
        left = [[skewed[j][i] for j in range(3)] for i in range(3)]
        corner_block = [skew(left[i]) for i in range(3)]
        skew_first = skew(m1)
        found = {}
        for i in range(3):
            for j in range(3):
                if j >= i:
                    found[("h", i, j)] = corner_block[i][j]
                    found[("h", 3 + i, 3 + j)] = npoints * n[i] * n[j]
                found[("h", i, 3 + j)] = skew_first[i] * n[j]
        rest = n[0] * m1[0] + n[1] * m1[1] + n[2] * m1[2]
        for i in range(3):
            found[("g", i)] = sum(left[i][j] * n[j] for j in range(3))
            found[("g", 3 + i)] = n[i] * rest
            late[pl.ds(i, arrived, stride=8), :] = skew_first[i]
            late[pl.ds(3 + i, arrived, stride=8), :] = npoints * n[i]
        for name, value in found.items():
            terms[pl.ds(ROWS.index(name), arrived, stride=32), :] = value
        for k in range(len(found), 32):
            terms[pl.ds(k, arrived, stride=32), :] = jnp.zeros_like(rest)

        def scan_sums(k, tile, rows):
            def add(q):
                return lax.dot_general(
                    split(tile(k, q)),
                    scan_hot[k * couples + q],
                    CONTRACT_LAST,
                    preferred_element_type=f32,
                )

            return summed(couples, add, 3 * rows, scans)

        per_scan = scale * joined(
            sum(scan_sums(k, lambda k, q: couple_tile(terms, k, q, 32), 32) for k in range(SHARE))
        )
        for h in range(wide):
            pieces = [per_scan[8 * c : 8 * c + 8, h * LANES : (h + 1) * LANES] for c in range(4)]
            for b in range(spread):
                at = (h * spread + b) * 8
                send_h[at : at + 8, :] = group_turn(pieces, b, own_group, own_scans)
        for peer in plane:
            send(send_h.at[aligned(peer[1] * 8, 8), :], recv_h.at[eight, :], peer, 4)
        recv_h[eight, :] = send_h[aligned(mp * 8, 8), :]

        wait_rows((n_tm - 1) * a_size, recvs.at[2])
        offset_table = []
        for k in range(SHARE):
            offsets = []
            for h in range(halves):
                base = (k * halves + h) * a_rows
                total = recv_a[base : base + a_rows, :]
                for t in range(1, n_tm):
                    total = total + recv_a[t * a_size + base : t * a_size + base + a_rows, :]
                floor = jnp.maximum(total[n_tm:] * npoints, 1.0)
                offset = total[:n_tm] / floor
                total_a[base : base + n_tm, :] = offset
                total_a[base + n_tm : base + a_rows, :] = floor
                offsets.append(offset)
            offset = jnp.concatenate(offsets, axis=1)
            if n_tm % 8:
                offset = jnp.concatenate(
                    [offset, jnp.zeros((8 - n_tm % 8, voxels), f32)], axis=0
                )
            offset_table.append(split(offset))
        d_rows = offset.shape[0]
        turn_row = lax.broadcasted_iota(jnp.int32, (d_rows, 2 * LANES), 0)
        turn_lane = lax.rem(lax.broadcasted_iota(jnp.int32, turn_row.shape, 1), LANES) // slots

        def late_tile(k, q):
            value = joined(
                jnp.dot(offset_table[k], vox_hot[k * couples + q], preferred_element_type=f32)
            )
            turn = turn_lane
            if parts > 1:
                turn = turn + per * lax.rem(q, parts)
            d = jnp.sum(jnp.where(turn_row == turn, value, 0.0), axis=0, keepdims=True)
            return couple_tile(late, k, q, 8) * d

        moved = scale * joined(sum(scan_sums(k, late_tile, 8) for k in range(SHARE)))
        for h in range(wide):
            send_g[h * 8 : h * 8 + 8, :] = moved[:, h * LANES : (h + 1) * LANES]
        for peer in plane:
            source = send_g.at[aligned(peer[1] // spread * 8, 8), :]
            send(source, recv_g.at[eight, :], peer, 5)
        recv_g[eight, :] = send_g[aligned(mp // spread * 8, 8), :]

        pltpu.make_async_copy(
            recv_q.at[pl.ds(0, n_tm - 1)], recv_q.at[pl.ds(0, n_tm - 1)], recvs.at[3]
        ).wait()
        quad_total = recv_q[0]
        for t in range(1, n_tm):
            quad_total = quad_total + recv_q[t]
        own_offset = total_a[pl.ds(tm, SHARE * halves, stride=a_rows), :]
        own_floor = total_a[pl.ds(n_tm + tm, SHARE * halves, stride=a_rows), :]
        cost = quad_total / own_floor - own_offset**2
        send_c[...] = cost[0:halves]
        send(send_c, recv_c, first_of, 7)
        recv_c[...] = cost[halves:]

    pl.when(reduces)(reduce_part)


    def wait_plane(s):
        @pl.when(reduces)
        def _():
            wait_rows((reducers - 1) * 8, recvs.at[s])

        @pl.when(jnp.logical_not(reduces))
        def _():
            wait_rows(reducers * 8, recvs.at[s])

    lines[...] = jnp.zeros_like(lines)
    wait_plane(4)
    total = recv_h[0:8, :]
    for m in range(1, reducers):
        total = total + recv_h[m * 8 : m * 8 + 8, :]
    lined = [total] + [pltpu.roll(total, LANES - own_scans * c, 1) for c in range(1, 4)]

    def row_at(name):
        k = ROWS.index(name)
        return lined[k // 8][k % 8 : k % 8 + 1]

    for i in range(6):
        for j in range(6):
            lines[6 * i + j : 6 * i + j + 1, :] = row_at(("h", min(i, j), max(i, j)))
    hess_out[...] = lines[...].T[0:own_scans, 0:36]
    gradient = jnp.concatenate([row_at(("g", i)) for i in range(6)], axis=0)

    @pl.when(jnp.logical_not(reduces))
    def _():
        pltpu.make_async_copy(recv_c, recv_c, recvs.at[7]).wait()

    for h in range(halves):
        cost_out[:, h * LANES : (h + 1) * LANES] = recv_c[h : h + 1, :]

    wait_plane(5)
    change = recv_g[0:8, :]
    for m in range(1, reducers):
        change = change + recv_g[m * 8 : m * 8 + 8, :]
    change = pltpu.roll(change, LANES - own_scans * lax.rem(mp, spread), 1)
    grad_out[...] = (gradient - change[0:6])[:, 0:own_scans]

    @pl.when(reduces)
    def _():
        rows = (reducers - 1) * message + (n_map - 1) * 16 + halves
        rows += (n_tm - 1) * (SHARE * n_size + a_size + SHARE * halves)
        wait_rows(rows, sends.at[0])

    @pl.when(jnp.logical_not(reduces))
    def _():
        wait_rows(reducers * message + n_size, sends.at[0])


def finish(hess_in, grad_in, cost_in, hess_out, grad_out, cost_out, sems):
    copies = [
        pltpu.make_async_copy(src, dst, sems.at[i])
        for i, (src, dst) in enumerate(
            [(hess_in, hess_out), (grad_in, grad_out), (cost_in, cost_out)]
        )
    ]
    for copy in copies:
        copy.start()
    for copy in copies:
        copy.wait()


def local(points, poses, normal_angles, voxel_ids, scan_ids):
    blocks, npoints = points.shape[1:]
    n_tm, n_map = lax.axis_size("tm"), lax.axis_size("map")
    devices = n_tm * n_map
    slots = blocks // devices
    chunks = blocks // LANES
    vox_count = normal_angles.shape[1]
    own_scans = poses.shape[1]
    assert npoints == LANES and slots * 4 == LANES and own_scans * 4 == LANES
    assert n_map % 4 == 0 and n_map % SHARE == 0 and n_tm % 4 == 0 and vox_count % LANES == 0
    scale = own_scans * devices / (blocks * devices * npoints)
    f32, bf16 = jnp.float32, jnp.bfloat16
    scans = own_scans * n_map
    halves = vox_count // LANES
    sent_rows = n_map * n_tm // 4 * TILE
    arrived = SHARE * n_map * n_tm // 4
    n_rows = -(-3 * halves // 8) * 8
    a_rows = SHARE * 2 * n_tm * halves
    reducers = n_map // SHARE
    hbm = pl.BlockSpec(memory_space=pl.ANY)
    vmem = pl.BlockSpec(memory_space=pltpu.VMEM)
    shapes = [(own_scans, 36), (6, own_scans), (1, vox_count)]
    results = pl.pallas_call(
        functools.partial(kernel, (n_tm, n_map, slots, float(npoints), scale)),
        out_shape=tuple(pltpu.VMEM(shape, f32) for shape in shapes),
        in_specs=[hbm] * 5,
        out_specs=(vmem,) * 3,
        scratch_shapes=[
            pltpu.VMEM(points.shape, f32),
            pltpu.VMEM(poses.shape, f32),
            pltpu.VMEM(normal_angles.shape, f32),
            pltpu.VMEM((chunks, LANES), jnp.int32),
            pltpu.VMEM((chunks, LANES), jnp.int32),
            pltpu.VMEM((8, LANES), f32),
            pltpu.VMEM((chunks * TILE, LANES), f32),
            pltpu.VMEM((sent_rows, LANES), f32),
            pltpu.VMEM((arrived * TILE, LANES), f32),
            pltpu.VMEM((SHARE * n_rows, LANES), f32),
            pltpu.VMEM((n_tm * SHARE * n_rows, LANES), f32),
            pltpu.VMEM((arrived // 2, scans, 2 * LANES), bf16),
            pltpu.VMEM((arrived // 2, vox_count, 2 * LANES), bf16),
            pltpu.VMEM((arrived * TILE, LANES), f32),
            pltpu.VMEM((arrived * 4 * n_tm, LANES), f32),
            pltpu.VMEM((a_rows, LANES), f32),
            pltpu.VMEM((n_tm * a_rows, LANES), f32),
            pltpu.VMEM((a_rows, LANES), f32),
            pltpu.VMEM((arrived * 4 * n_tm, LANES), f32),
            pltpu.VMEM((arrived * 8, LANES), f32),
            pltpu.VMEM((n_tm, SHARE * halves, LANES), f32),
            pltpu.VMEM((n_tm, SHARE * halves, LANES), f32),
            pltpu.VMEM((halves, LANES), f32),
            pltpu.VMEM((halves, LANES), f32),
            pltpu.VMEM((arrived * 32, LANES), f32),
            pltpu.VMEM((arrived * 8, LANES), f32),
            pltpu.VMEM((n_map * 8, LANES), f32),
            pltpu.VMEM((reducers * 8, LANES), f32),
            pltpu.VMEM((scans // LANES * 8, LANES), f32),
            pltpu.VMEM((reducers * 8, LANES), f32),
            pltpu.VMEM((LANES, LANES), f32),
            pltpu.SemaphoreType.DMA((4,)),
            pltpu.SemaphoreType.DMA((4,)),
            pltpu.SemaphoreType.DMA((1,)),
            pltpu.SemaphoreType.DMA((8,)),
        ],
        compiler_params=pltpu.CompilerParams(collective_id=0, has_side_effects=True),
    )(
        points,
        poses,
        normal_angles,
        voxel_ids.reshape(chunks, LANES),
        scan_ids.reshape(chunks, LANES),
    )
    hess, grad, cost = pl.pallas_call(
        finish,
        out_shape=tuple(jax.ShapeDtypeStruct(shape, f32) for shape in shapes),
        in_specs=[vmem] * 3,
        out_specs=(hbm,) * 3,
        scratch_shapes=[pltpu.SemaphoreType.DMA((3,))],
    )(*[pltpu.with_memory_space_constraint(x, pltpu.VMEM) for x in results])
    return hess.T, grad, cost.reshape(vox_count)


def solution(mesh):
    return jax.shard_map(
        local,
        mesh=mesh,
        in_specs=(
            P(None, ("tm", "map"), None),
            P(None, ("tm", "map")),
            P(None, ("tm", "map")),
            P(("tm", "map")),
            P(("tm", "map")),
        ),
        out_specs=(P(None, ("tm", "map")), P(None, ("tm", "map")), P(("tm", "map"))),
        check_vma=False,
    )
```

```python
import functools

import jax
import jax.numpy as jnp
from jax import lax
from jax.experimental import pallas as pl
from jax.experimental.pallas import tpu as pltpu
from jax.sharding import PartitionSpec as P

LANES = 128
MESH = pl.DeviceIdType.MESH
PAIRS = [(0, 0), (1, 1), (2, 2), (0, 1), (0, 2), (1, 2)]
PAIR_ROW = {}
for _k, (_i, _j) in enumerate(PAIRS):
    PAIR_ROW[(_i, _j)] = _k
    PAIR_ROW[(_j, _i)] = _k

ROWS = [("h", i, j) for i in range(6) for j in range(i, 6)] + [("g", i) for i in range(6)]

TILE = 16
VOX_ROW, SCAN_ROW, POSE_ROW = 9, 10, 12
SHARE = 2
CONTRACT_LAST = (((1,), (1,)), ((), ()))


def split(x):
    high = x.astype(jnp.bfloat16).astype(jnp.float32)
    rest = x - high
    mid = rest.astype(jnp.bfloat16).astype(jnp.float32)
    return jnp.concatenate([high, mid, rest - mid], axis=0).astype(jnp.bfloat16)


def joined(y):
    rows = y.shape[0] // 3
    return y[:rows] + y[rows : 2 * rows] + y[2 * rows :]


def group_turn(pieces, out_group, group, lanes_per):
    total = None
    for a, piece in enumerate(pieces):
        shift = ((a - out_group) * lanes_per) % LANES
        moved = piece if shift == 0 else pltpu.roll(piece, shift, 1)
        total = moved if total is None else jnp.where(group == a, moved, total)
    return total


def loop(count, body):
    if count <= 8:
        for i in range(count):
            body(i)
    else:
        def step(i, carry):
            body(i)
            return carry

        lax.fori_loop(0, count, step, 0)


def summed(count, body, rows, columns):
    acc = jnp.zeros((rows, columns), jnp.float32)
    if count <= 8:
        for i in range(count):
            acc = acc + body(i)
        return acc
    return lax.fori_loop(0, count, lambda i, total: total + body(i), acc)


def aligned(start, size, unit=8):
    if not isinstance(start, int):
        start = pl.multiple_of(start, unit)
    return pl.ds(start, size)


def kernel(
    sizes,
    points,
    poses,
    angles,
    voxel_ids,
    scan_ids,
    hess_out,
    grad_out,
    cost_out,
    pts,
    pose_in,
    angle_in,
    vox_in,
    scan_in,
    pose_pad,
    sent,
    send1,
    recv1,
    pair_n,
    recv_n,
    scan_hot,
    vox_hot,
    world,
    send_a,
    recv_a,
    total_a,
    quads,
    send_q,
    recv_q,
    send_c,
    recv_c,
    terms,
    late,
    send_h,
    recv_h,
    send_g,
    recv_g,
    lines,
    pts_sem,
    in_sem,
    sends,
    recvs,
):
    n_tm, n_map, slots, npoints, scale = sizes
    reducers = n_map // SHARE
    blocks = pts.shape[1]
    chunks = blocks // LANES
    per = LANES // slots
    own_scans = pose_in.shape[1]
    spread = LANES // own_scans
    scans = own_scans * n_map
    wide = scans // LANES
    voxels = angle_in.shape[1]
    halves = voxels // LANES
    parts = n_tm // per
    step = SHARE * parts
    arrived = n_map * step
    couples = n_map // 2 * parts
    message = step * TILE
    n_size = pair_n.shape[0] // SHARE
    a_rows = 2 * n_tm
    a_size = SHARE * halves * a_rows
    tm = lax.axis_index("tm")
    mp = lax.axis_index("map")
    rd = mp // SHARE
    part = lax.rem(mp, SHARE)
    reduces = part == SHARE - 1
    f32, bf16 = jnp.float32, jnp.bfloat16

    small = [
        pltpu.make_async_copy(src, dst, in_sem.at[i])
        for i, (src, dst) in enumerate(
            [(poses, pose_in), (angles, angle_in), (voxel_ids, vox_in), (scan_ids, scan_in)]
        )
    ]
    loads = pts_sem.shape[0]
    span = blocks // loads

    def points_copy(r):
        rows = pl.ds(r * span, span)
        return pltpu.make_async_copy(points.at[:, rows, :], pts.at[:, rows, :], pts_sem.at[r])

    for copy in small:
        copy.start()
    loop(loads, lambda r: points_copy(r).start())
    barrier = pltpu.get_barrier_semaphore()
    near = (tm, rd * SHARE + SHARE - 1)
    first_of = (tm, rd * SHARE)
    plane = [(tm, lax.rem(mp + i, n_map)) for i in range(1, n_map)]
    column = [(lax.rem(tm + i, n_tm), mp) for i in range(1, n_tm)]
    others = [lax.rem(rd + i, reducers) for i in range(1, reducers)]

    def greet(peer):
        pl.semaphore_signal(barrier, inc=1, device_id=peer, device_id_type=MESH)

    @pl.when(reduces)
    def _():
        for peer in column + plane:
            greet(peer)
        for peer in column:

            @pl.when(peer[0] > tm)
            def _(peer=peer):
                greet((peer[0], rd * SHARE))

    @pl.when(jnp.logical_not(reduces))
    def _():
        for other in others:
            greet((tm, other * SHARE + SHARE - 1))
        greet(near)

    def send(source, dest, peer, s):
        pltpu.make_async_remote_copy(
            src_ref=source,
            dst_ref=dest,
            send_sem=sends.at[0],
            recv_sem=recvs.at[s],
            device_id=peer,
            device_id_type=MESH,
        ).start()

    def wait_rows(rows, sem):
        ref = pts.at[0, pl.ds(0, rows), :]
        pltpu.make_async_copy(ref, ref, sem).wait()

    def every(ref, k, stride, count=arrived):
        return ref[pl.ds(k, count, stride=stride), :]

    lane = lax.broadcasted_iota(jnp.int32, (8, LANES), 1)
    group = lane // slots
    chunk_of = lax.broadcasted_iota(jnp.int32, (arrived, LANES), 0)
    turn_of = (
        lax.broadcasted_iota(jnp.int32, (arrived, LANES), 1) // slots + per * lax.rem(chunk_of, parts)
    )
    own_turn = [turn_of == t for t in range(n_tm)]
    sent[...] = jnp.zeros_like(sent)

    for copy in small:
        copy.wait()
    pose_pad[...] = jnp.zeros_like(pose_pad)
    for g in range(spread):
        pose_pad[0:6, g * own_scans : (g + 1) * own_scans] = pose_in[...]
    pose = pose_pad[...]
    cos, sin = jnp.cos(pose), jnp.sin(pose)
    cx, cy, cz = cos[0:1], cos[1:2], cos[2:3]
    sx, sy, sz = sin[0:1], sin[1:2], sin[2:3]
    pose_rows = [
        [cz * cy, cz * sy * sx - sz * cx, cz * sy * cx + sz * sx],
        [sz * cy, sz * sy * sx + cz * cx, sz * sy * cx - cz * sx],
        [-sy, cy * sx, cy * cx],
        [pose[3:4], pose[4:5], pose[5:6]],
    ]
    scan_group = lane[0:1] // own_scans
    pose_lines = []
    for q in range(3):
        line = pose_rows[0][q]
        for g in range(1, 4):
            line = jnp.where(scan_group == g, pose_rows[g][q], line)
        pose_lines.append(line)

    ids = vox_in[...]
    row_of = lax.broadcasted_iota(jnp.int32, ids.shape, 0)
    lane_of = lax.broadcasted_iota(jnp.int32, ids.shape, 1)
    owner_of = row_of * per + lane_of // slots
    local_ids = jnp.where(ids >= 0, ids - owner_of * voxels, -1).astype(f32)
    sent[pl.ds(VOX_ROW, chunks, stride=TILE), :] = local_ids
    sent[pl.ds(SCAN_ROW, chunks, stride=TILE), :] = scan_in[...].astype(f32)

    theta, phi = angle_in[0:1, :], angle_in[1:2, :]
    sin_theta = jnp.sin(theta)
    own_normal = [sin_theta * jnp.cos(phi), sin_theta * jnp.sin(phi), jnp.cos(theta)]
    n_mine = aligned(part * n_size, n_size)
    for c in range(3):
        for h in range(halves):
            k = part * n_size + c * halves + h
            pair_n[pl.ds(k, 1), :] = own_normal[c][:, h * LANES : (h + 1) * LANES]

    def raw_moments(r):
        at = aligned(r * LANES, LANES, LANES)
        xyz = [pts[i, at, :].T for i in range(3)]
        sums = [jnp.sum(x, axis=0, keepdims=True) for x in xyz]
        sums += [jnp.sum(xyz[i] * xyz[j], axis=0, keepdims=True) for i, j in PAIRS]
        for k, row in enumerate(sums):
            sent[pl.ds(r * TILE + k, 1), :] = row

    def load_step(r):
        points_copy(r).wait()
        for i in range(span // LANES):
            raw_moments(r * (span // LANES) + i)

    loop(loads, load_step)
    row_chunks = n_map // per

    def pack(peer_row):
        for g in range(per):
            peer = peer_row * per + g
            for u in range(parts):
                for half in range(2):
                    pieces = [
                        sent[
                            aligned(
                                ((u * per + a) * row_chunks + peer_row) * TILE + 8 * half, 8
                            ),
                            :,
                        ]
                        for a in range(per)
                    ]
                    at = aligned((peer * parts + u) * TILE + 8 * half, 8)
                    send1[at, :] = group_turn(pieces, g, group, slots)
            for q in range(3):
                send1[pl.ds(peer * parts * TILE + POSE_ROW + q, 1), :] = pose_lines[q]

    loop(row_chunks, pack)

    from_plane = n_map - 1 + n_tm - 1
    pl.semaphore_wait(barrier, jnp.where(reduces, from_plane, reducers + tm))
    mine = aligned(mp * message, message)

    def message_of(other):
        return send1.at[aligned(other * message, message), :]

    def normals_to(t, k):
        return recv_n.at[aligned((t * SHARE + k) * n_size, n_size), :]

    @pl.when(jnp.logical_not(reduces))
    def _():
        for peer in column:

            @pl.when(peer[0] < tm)
            def _(peer=peer):
                send(pair_n.at[n_mine, :], normals_to(tm, 0), (peer[0], near[1]), 1)

        send(pair_n.at[n_mine, :], pair_n.at[n_mine, :], near, 6)

    for other in others:
        send(message_of(other), recv1.at[mine, :], (tm, other * SHARE + SHARE - 1), 0)

    @pl.when(jnp.logical_not(reduces))
    def _():
        send(message_of(rd), recv1.at[mine, :], near, 0)

    eight = aligned(rd * 8, 8)

    def reduce_part():
        for peer in column:
            send(pair_n.at[pl.ds(n_size, n_size), :], normals_to(tm, 1), peer, 1)
        wait_rows(n_size, recvs.at[6])
        for peer in column:

            @pl.when(peer[0] > tm)
            def _(peer=peer):
                send(pair_n.at[pl.ds(0, n_size), :], normals_to(tm, 0), peer, 1)

        n_column = aligned(tm * SHARE * n_size, SHARE * n_size)
        recv1[mine, :] = send1[aligned(rd * message, message), :]
        recv_n[n_column, :] = pair_n[...]
        for t in range(n_tm):
            world[pl.ds(3 * n_tm + t, arrived, stride=4 * n_tm), :] = jnp.where(
                own_turn[t], 1.0, 0.0
            )
        quads[...] = jnp.zeros_like(quads)
        late[...] = jnp.zeros_like(late)
        wait_rows((n_map - 1) * message, recvs.at[0])

        def chunk(k, q, side):
            i, u = (q // parts, q % parts) if isinstance(q, int) else (q // parts, lax.rem(q, parts))
            return ((2 * i + side) * SHARE + k) * parts + u

        def couple_row(k, q, row):
            return jnp.concatenate(
                [recv1[pl.ds(chunk(k, q, side) * TILE + row, 1), :] for side in range(2)], axis=1
            )

        def couple_tile(ref, k, q, rows):
            return jnp.concatenate(
                [ref[aligned(chunk(k, q, side) * rows, rows), :] for side in range(2)], axis=1
            )

        def each_couple(body):
            for k in range(SHARE):
                loop(couples, functools.partial(body, k))

        scan_iota = lax.broadcasted_iota(jnp.int32, (scans, 2 * LANES), 0).astype(f32)
        vox_iota = lax.broadcasted_iota(jnp.int32, (voxels, 2 * LANES), 0).astype(f32)

        def mark_scans(k, q):
            scan_hot[k * couples + q] = jnp.where(
                couple_row(k, q, SCAN_ROW) == scan_iota, 1.0, 0.0
            ).astype(bf16)

        def mark_voxels(k, q):
            vox_hot[k * couples + q] = jnp.where(
                couple_row(k, q, VOX_ROW) == vox_iota, 1.0, 0.0
            ).astype(bf16)

        top = lax.broadcasted_iota(jnp.int32, (8, LANES), 0) < 4
        own_group = lane // own_scans
        columns = []
        for h in range(wide):
            at = [(h * spread + a) * message + 8 for a in range(spread)]
            tiles = [recv1[row : row + 8, :] for row in at]
            turned = [group_turn(tiles, g, own_group, own_scans) for g in range(4)]
            low = jnp.where(top, pltpu.roll(turned[1], 4, 0), turned[0])
            high = jnp.where(top, pltpu.roll(turned[3], 4, 0), turned[2])
            columns.append(jnp.concatenate([low, high], axis=0))
        table_row = {}
        for q in range(3):
            table_row[(1, q)], table_row[(0, q)] = q, 4 + q
            table_row[(3, q)], table_row[(2, q)] = 8 + q, 12 + q

        def whole_row(row, count):
            return jnp.broadcast_to(row, (count, LANES))

        def gather(tables, high, low):
            value = jnp.take_along_axis(tables[0], low, axis=1, mode="promise_in_bounds")
            for h in range(1, len(tables)):
                other = jnp.take_along_axis(tables[h], low, axis=1, mode="promise_in_bounds")
                value = jnp.where(high == h, other, value)
            return value

        scan_of = every(recv1, SCAN_ROW, TILE).astype(jnp.int32)
        scan_low, scan_high = jnp.bitwise_and(scan_of, LANES - 1), scan_of // LANES

        def pose_of(i, j):
            row = table_row[(i, j)]
            rows = [whole_row(tile[row : row + 1], arrived) for tile in columns]
            return gather(rows, scan_high, scan_low)

        rot = [[pose_of(i, j) for j in range(3)] for i in range(3)]
        shift = [pose_of(3, j) for j in range(3)]
        first = [every(recv1, k, TILE) for k in range(3)]
        turned_first = [sum(rot[i][j] * first[j] for j in range(3)) for i in range(3)]
        m1 = [turned_first[i] + npoints * shift[i] for i in range(3)]
        for c in range(3):
            for t in range(n_tm):
                world[pl.ds(c * n_tm + t, arrived, stride=4 * n_tm), :] = jnp.where(
                    own_turn[t], m1[c], 0.0
                )

        each_couple(mark_voxels)

        def voxel_sums(ref, rows, k):
            def add(q):
                return lax.dot_general(
                    split(couple_tile(ref, k, q, rows)),
                    vox_hot[k * couples + q],
                    CONTRACT_LAST,
                    preferred_element_type=f32,
                )

            return joined(summed(couples, add, 3 * rows, voxels))

        sums = [voxel_sums(world, 4 * n_tm, k) for k in range(SHARE)]
        wait_rows((n_tm - 1) * SHARE * n_size, recvs.at[1])
        normal = [
            [
                jnp.concatenate(
                    [
                        every(recv_n, k * n_size + c * halves + h, SHARE * n_size, n_tm)
                        for h in range(halves)
                    ],
                    axis=1,
                )
                for c in range(3)
            ]
            for k in range(SHARE)
        ]
        for k in range(SHARE):
            along = sum(normal[k][c] * sums[k][c * n_tm : (c + 1) * n_tm] for c in range(3))
            count = sums[k][3 * n_tm : 4 * n_tm]
            for h in range(halves):
                at = slice(h * LANES, (h + 1) * LANES)
                base = (k * halves + h) * a_rows
                send_a[base : base + n_tm, :] = along[:, at]
                send_a[base + n_tm : base + a_rows, :] = count[:, at]

        a_mine = aligned(tm * a_size, a_size)
        for peer in column:
            send(send_a, recv_a.at[a_mine, :], peer, 2)
        recv_a[a_mine, :] = send_a[...]

        each_couple(mark_scans)
        vox_of = every(recv1, VOX_ROW, TILE).astype(jnp.int32)
        live = vox_of >= 0
        vox_low = jnp.bitwise_and(vox_of, LANES - 1)
        vox_high = jnp.where(live, vox_of, 0) // LANES
        part_of = lax.rem(lax.broadcasted_iota(jnp.int32, (step, LANES), 0) // parts, SHARE)

        def by_voxel(rows):
            value = None
            for t in range(n_tm):
                tables = []
                for h in range(halves):
                    tab = whole_row(rows(0, t, h), step)
                    for k in range(1, SHARE):
                        tab = jnp.where(part_of == k, whole_row(rows(k, t, h), step), tab)
                    tables.append(jnp.concatenate([tab] * n_map, axis=0))
                found = gather(tables, vox_high, vox_low)
                value = found if t == 0 else jnp.where(own_turn[t], found, value)
            return value

        n = []
        for c in range(3):
            value = by_voxel(
                lambda k, t, h: normal[k][c][t : t + 1, h * LANES : (h + 1) * LANES]
            )
            n.append(jnp.where(live, value, 0.0))
        second = [every(recv1, 3 + k, TILE) for k in range(6)]
        half_turned = [
            [sum(rot[i][k] * second[PAIR_ROW[(k, j)]] for k in range(3)) for j in range(3)]
            for i in range(3)
        ]
        m2 = [
            sum(half_turned[i][k] * rot[j][k] for k in range(3))
            + turned_first[i] * shift[j]
            + shift[i] * m1[j]
            for i, j in PAIRS
        ]
        quad = sum(n[i] ** 2 * m2[i] for i in range(3)) + 2.0 * sum(
            n[PAIRS[k][0]] * n[PAIRS[k][1]] * m2[k] for k in range(3, 6)
        )
        for t in range(n_tm):
            quads[pl.ds(t, arrived, stride=8), :] = jnp.where(own_turn[t], quad, 0.0)
        for k in range(SHARE):
            quad_sums = voxel_sums(quads, 8, k)
            for t in range(n_tm):
                for h in range(halves):
                    send_q[t, k * halves + h : k * halves + h + 1, :] = quad_sums[
                        t : t + 1, h * LANES : (h + 1) * LANES
                    ]
        for peer in column:
            send(send_q.at[peer[0]], recv_q.at[tm], peer, 3)
        recv_q[tm] = send_q[tm]

        def skew(v):
            return [
                n[2] * v[1] - n[1] * v[2],
                n[0] * v[2] - n[2] * v[0],
                n[1] * v[0] - n[0] * v[1],
            ]

        full = [[m2[PAIR_ROW[(i, j)]] for j in range(3)] for i in range(3)]
        skewed = [skew([full[k][j] for k in range(3)]) for j in range(3)]
        left = [[skewed[j][i] for j in range(3)] for i in range(3)]
        corner_block = [skew(left[i]) for i in range(3)]
        skew_first = skew(m1)
        found = {}
        for i in range(3):
            for j in range(3):
                if j >= i:
                    found[("h", i, j)] = corner_block[i][j]
                    found[("h", 3 + i, 3 + j)] = npoints * n[i] * n[j]
                found[("h", i, 3 + j)] = skew_first[i] * n[j]
        rest = n[0] * m1[0] + n[1] * m1[1] + n[2] * m1[2]
        for i in range(3):
            found[("g", i)] = sum(left[i][j] * n[j] for j in range(3))
            found[("g", 3 + i)] = n[i] * rest
        shares = skew_first + [npoints * n[i] for i in range(3)]
        for name, value in found.items():
            terms[pl.ds(ROWS.index(name), arrived, stride=32), :] = value
        for k in range(len(found), 32):
            terms[pl.ds(k, arrived, stride=32), :] = jnp.zeros_like(rest)

        def scan_sums(k, tile, rows):
            def add(q):
                return lax.dot_general(
                    split(tile(k, q)),
                    scan_hot[k * couples + q],
                    CONTRACT_LAST,
                    preferred_element_type=f32,
                )

            return summed(couples, add, 3 * rows, scans)

        per_scan = scale * joined(
            sum(scan_sums(k, lambda k, q: couple_tile(terms, k, q, 32), 32) for k in range(SHARE))
        )
        for h in range(wide):
            pieces = [per_scan[8 * c : 8 * c + 8, h * LANES : (h + 1) * LANES] for c in range(4)]
            for b in range(spread):
                at = (h * spread + b) * 8
                send_h[at : at + 8, :] = group_turn(pieces, b, own_group, own_scans)
        for peer in plane:
            send(send_h.at[aligned(peer[1] * 8, 8), :], recv_h.at[eight, :], peer, 4)
        recv_h[eight, :] = send_h[aligned(mp * 8, 8), :]

        wait_rows((n_tm - 1) * a_size, recvs.at[2])
        offset_rows = []
        for k in range(SHARE):
            offsets = []
            for h in range(halves):
                base = (k * halves + h) * a_rows
                total = recv_a[base : base + a_rows, :]
                for t in range(1, n_tm):
                    total = total + recv_a[t * a_size + base : t * a_size + base + a_rows, :]
                floor = jnp.maximum(total[n_tm:] * npoints, 1.0)
                offset = total[:n_tm] / floor
                total_a[base : base + n_tm, :] = offset
                total_a[base + n_tm : base + a_rows, :] = floor
                offsets.append(offset)
            offset_rows.append(offsets)
        offset_of = by_voxel(lambda k, t, h: offset_rows[k][h][t : t + 1])
        for i in range(6):
            late[pl.ds(i, arrived, stride=8), :] = shares[i] * offset_of
        moved = scale * joined(
            sum(scan_sums(k, lambda k, q: couple_tile(late, k, q, 8), 8) for k in range(SHARE))
        )
        for h in range(wide):
            send_g[h * 8 : h * 8 + 8, :] = moved[:, h * LANES : (h + 1) * LANES]
        for peer in plane:
            source = send_g.at[aligned(peer[1] // spread * 8, 8), :]
            send(source, recv_g.at[eight, :], peer, 5)
        recv_g[eight, :] = send_g[aligned(mp // spread * 8, 8), :]

        pltpu.make_async_copy(
            recv_q.at[pl.ds(0, n_tm - 1)], recv_q.at[pl.ds(0, n_tm - 1)], recvs.at[3]
        ).wait()
        quad_total = recv_q[0]
        for t in range(1, n_tm):
            quad_total = quad_total + recv_q[t]
        own_offset = total_a[pl.ds(tm, SHARE * halves, stride=a_rows), :]
        own_floor = total_a[pl.ds(n_tm + tm, SHARE * halves, stride=a_rows), :]
        cost = quad_total / own_floor - own_offset**2
        send_c[...] = cost[0:halves]
        send(send_c, recv_c, first_of, 7)
        recv_c[...] = cost[halves:]

    pl.when(reduces)(reduce_part)


    def wait_plane(s):
        @pl.when(reduces)
        def _():
            wait_rows((reducers - 1) * 8, recvs.at[s])

        @pl.when(jnp.logical_not(reduces))
        def _():
            wait_rows(reducers * 8, recvs.at[s])

    lines[...] = jnp.zeros_like(lines)
    wait_plane(4)
    total = recv_h[0:8, :]
    for m in range(1, reducers):
        total = total + recv_h[m * 8 : m * 8 + 8, :]
    lined = [total] + [pltpu.roll(total, LANES - own_scans * c, 1) for c in range(1, 4)]

    def row_at(name):
        k = ROWS.index(name)
        return lined[k // 8][k % 8 : k % 8 + 1]

    for i in range(6):
        for j in range(6):
            lines[6 * i + j : 6 * i + j + 1, :] = row_at(("h", min(i, j), max(i, j)))
    hess_out[...] = lines[...].T[0:own_scans, 0:36]
    gradient = jnp.concatenate([row_at(("g", i)) for i in range(6)], axis=0)

    @pl.when(jnp.logical_not(reduces))
    def _():
        pltpu.make_async_copy(recv_c, recv_c, recvs.at[7]).wait()

    for h in range(halves):
        cost_out[:, h * LANES : (h + 1) * LANES] = recv_c[h : h + 1, :]

    wait_plane(5)
    change = recv_g[0:8, :]
    for m in range(1, reducers):
        change = change + recv_g[m * 8 : m * 8 + 8, :]
    change = pltpu.roll(change, LANES - own_scans * lax.rem(mp, spread), 1)
    grad_out[...] = (gradient - change[0:6])[:, 0:own_scans]

    for t in range(n_tm):

        @pl.when(jnp.logical_and(reduces, tm == t))
        def _(t=t):
            rows = (reducers - 1) * message + (n_map - 1) * 16 + halves
            rows += (n_tm - 1) * (n_size + a_size + SHARE * halves) + (n_tm - 1 - t) * n_size
            wait_rows(rows, sends.at[0])

        @pl.when(jnp.logical_and(jnp.logical_not(reduces), tm == t))
        def _(t=t):
            wait_rows(reducers * message + (t + 1) * n_size, sends.at[0])


def finish(hess_in, grad_in, cost_in, hess_out, grad_out, cost_out, sems):
    copies = [
        pltpu.make_async_copy(src, dst, sems.at[i])
        for i, (src, dst) in enumerate(
            [(hess_in, hess_out), (grad_in, grad_out), (cost_in, cost_out)]
        )
    ]
    for copy in copies:
        copy.start()
    for copy in copies:
        copy.wait()


def local(points, poses, normal_angles, voxel_ids, scan_ids):
    blocks, npoints = points.shape[1:]
    n_tm, n_map = lax.axis_size("tm"), lax.axis_size("map")
    devices = n_tm * n_map
    slots = blocks // devices
    chunks = blocks // LANES
    vox_count = normal_angles.shape[1]
    own_scans = poses.shape[1]
    assert npoints == LANES and slots * 4 == LANES and own_scans * 4 == LANES
    assert n_map % 4 == 0 and n_map % SHARE == 0 and n_tm % 4 == 0 and vox_count % LANES == 0
    scale = own_scans * devices / (blocks * devices * npoints)
    f32, bf16 = jnp.float32, jnp.bfloat16
    scans = own_scans * n_map
    halves = vox_count // LANES
    sent_rows = n_map * n_tm // 4 * TILE
    arrived = SHARE * n_map * n_tm // 4
    n_rows = -(-3 * halves // 8) * 8
    a_rows = SHARE * 2 * n_tm * halves
    reducers = n_map // SHARE
    hbm = pl.BlockSpec(memory_space=pl.ANY)
    vmem = pl.BlockSpec(memory_space=pltpu.VMEM)
    shapes = [(own_scans, 36), (6, own_scans), (1, vox_count)]
    results = pl.pallas_call(
        functools.partial(kernel, (n_tm, n_map, slots, float(npoints), scale)),
        out_shape=tuple(pltpu.VMEM(shape, f32) for shape in shapes),
        in_specs=[hbm] * 5,
        out_specs=(vmem,) * 3,
        scratch_shapes=[
            pltpu.VMEM(points.shape, f32),
            pltpu.VMEM(poses.shape, f32),
            pltpu.VMEM(normal_angles.shape, f32),
            pltpu.VMEM((chunks, LANES), jnp.int32),
            pltpu.VMEM((chunks, LANES), jnp.int32),
            pltpu.VMEM((8, LANES), f32),
            pltpu.VMEM((chunks * TILE, LANES), f32),
            pltpu.VMEM((sent_rows, LANES), f32),
            pltpu.VMEM((arrived * TILE, LANES), f32),
            pltpu.VMEM((SHARE * n_rows, LANES), f32),
            pltpu.VMEM((n_tm * SHARE * n_rows, LANES), f32),
            pltpu.VMEM((arrived // 2, scans, 2 * LANES), bf16),
            pltpu.VMEM((arrived // 2, vox_count, 2 * LANES), bf16),
            pltpu.VMEM((arrived * 4 * n_tm, LANES), f32),
            pltpu.VMEM((a_rows, LANES), f32),
            pltpu.VMEM((n_tm * a_rows, LANES), f32),
            pltpu.VMEM((a_rows, LANES), f32),
            pltpu.VMEM((arrived * 8, LANES), f32),
            pltpu.VMEM((n_tm, SHARE * halves, LANES), f32),
            pltpu.VMEM((n_tm, SHARE * halves, LANES), f32),
            pltpu.VMEM((halves, LANES), f32),
            pltpu.VMEM((halves, LANES), f32),
            pltpu.VMEM((arrived * 32, LANES), f32),
            pltpu.VMEM((arrived * 8, LANES), f32),
            pltpu.VMEM((n_map * 8, LANES), f32),
            pltpu.VMEM((reducers * 8, LANES), f32),
            pltpu.VMEM((scans // LANES * 8, LANES), f32),
            pltpu.VMEM((reducers * 8, LANES), f32),
            pltpu.VMEM((LANES, LANES), f32),
            pltpu.SemaphoreType.DMA((4,)),
            pltpu.SemaphoreType.DMA((4,)),
            pltpu.SemaphoreType.DMA((1,)),
            pltpu.SemaphoreType.DMA((8,)),
        ],
        compiler_params=pltpu.CompilerParams(collective_id=0, has_side_effects=True),
    )(
        points,
        poses,
        normal_angles,
        voxel_ids.reshape(chunks, LANES),
        scan_ids.reshape(chunks, LANES),
    )
    hess, grad, cost = pl.pallas_call(
        finish,
        out_shape=tuple(jax.ShapeDtypeStruct(shape, f32) for shape in shapes),
        in_specs=[vmem] * 3,
        out_specs=(hbm,) * 3,
        scratch_shapes=[pltpu.SemaphoreType.DMA((3,))],
    )(*[pltpu.with_memory_space_constraint(x, pltpu.VMEM) for x in results])
    return hess.T, grad, cost.reshape(vox_count)


def solution(mesh):
    return jax.shard_map(
        local,
        mesh=mesh,
        in_specs=(
            P(None, ("tm", "map"), None),
            P(None, ("tm", "map")),
            P(None, ("tm", "map")),
            P(("tm", "map")),
            P(("tm", "map")),
        ),
        out_specs=(P(None, ("tm", "map")), P(None, ("tm", "map")), P(("tm", "map"))),
        check_vma=False,
    )
```

```python
import functools

import jax
import jax.numpy as jnp
from jax import lax
from jax.experimental import pallas as pl
from jax.experimental.pallas import tpu as pltpu
from jax.sharding import PartitionSpec as P

LANES = 128
MESH = pl.DeviceIdType.MESH
PAIRS = [(0, 0), (1, 1), (2, 2), (0, 1), (0, 2), (1, 2)]
PAIR_ROW = {}
for _k, (_i, _j) in enumerate(PAIRS):
    PAIR_ROW[(_i, _j)] = _k
    PAIR_ROW[(_j, _i)] = _k

ROWS = [("h", i, j) for i in range(6) for j in range(i, 6)] + [("g", i) for i in range(6)]

MARKS, FIRSTS = 0, 8
VOX_ROW, SCAN_ROW, LAST_ROW, POSE_ROW = 0, 1, 2, 3
SHARE = 2
CONTRACT_LAST = (((1,), (1,)), ((), ()))


def split(x):
    high = x.astype(jnp.bfloat16).astype(jnp.float32)
    rest = x - high
    mid = rest.astype(jnp.bfloat16).astype(jnp.float32)
    return jnp.concatenate([high, mid, rest - mid], axis=0).astype(jnp.bfloat16)


def joined(y):
    rows = y.shape[0] // 3
    return y[:rows] + y[rows : 2 * rows] + y[2 * rows :]


def group_turn(pieces, out_group, group, lanes_per):
    total = None
    for a, piece in enumerate(pieces):
        shift = ((a - out_group) * lanes_per) % LANES
        moved = piece if shift == 0 else pltpu.roll(piece, shift, 1)
        total = moved if total is None else jnp.where(group == a, moved, total)
    return total


def loop(count, body):
    if count <= 8:
        for i in range(count):
            body(i)
    else:
        def step(i, carry):
            body(i)
            return carry

        lax.fori_loop(0, count, step, 0)


def summed(count, body, rows, columns):
    acc = jnp.zeros((rows, columns), jnp.float32)
    if count <= 8:
        for i in range(count):
            acc = acc + body(i)
        return acc
    return lax.fori_loop(0, count, lambda i, total: total + body(i), acc)


def aligned(start, size, unit=8):
    if not isinstance(start, int):
        start = pl.multiple_of(start, unit)
    return pl.ds(start, size)


def kernel(
    sizes,
    points,
    poses,
    angles,
    voxel_ids,
    scan_ids,
    hess_out,
    grad_out,
    cost_out,
    pts,
    pose_in,
    angle_in,
    vox_in,
    scan_in,
    pose_pad,
    sent,
    send1,
    recv1,
    send2,
    recv2,
    pair_n,
    recv_n,
    world,
    send_a,
    recv_a,
    total_a,
    quads,
    send_q,
    recv_q,
    send_c,
    recv_c,
    terms,
    late,
    send_h,
    recv_h,
    send_g,
    recv_g,
    lines,
    pts_sem,
    in_sem,
    sends,
    recvs,
):
    n_tm, n_map, slots, npoints, scale = sizes
    reducers = n_map // SHARE
    blocks = pts.shape[1]
    chunks = blocks // LANES
    per = LANES // slots
    own_scans = pose_in.shape[1]
    spread = LANES // own_scans
    scans = own_scans * n_map
    wide = scans // LANES
    voxels = angle_in.shape[1]
    halves = voxels // LANES
    parts = n_tm // per
    step = SHARE * parts
    arrived = n_map * step
    couples = n_map // 2 * parts
    message = parts * 16
    rest_rows = parts * 8
    in_plane = n_map * parts
    n_size = pair_n.shape[0] // SHARE
    a_rows = 2 * n_tm
    a_size = SHARE * halves * a_rows
    tm = lax.axis_index("tm")
    mp = lax.axis_index("map")
    rd = mp // SHARE
    part = lax.rem(mp, SHARE)
    reduces = part == SHARE - 1
    f32, bf16 = jnp.float32, jnp.bfloat16

    small = [
        pltpu.make_async_copy(src, dst, in_sem.at[i])
        for i, (src, dst) in enumerate(
            [(poses, pose_in), (angles, angle_in), (voxel_ids, vox_in), (scan_ids, scan_in)]
        )
    ]
    loads = pts_sem.shape[0]
    span = blocks // loads

    def points_copy(r):
        rows = pl.ds(r * span, span)
        return pltpu.make_async_copy(points.at[:, rows, :], pts.at[:, rows, :], pts_sem.at[r])

    for copy in small:
        copy.start()
    loop(loads, lambda r: points_copy(r).start())
    barrier = pltpu.get_barrier_semaphore()
    near = (tm, rd * SHARE + SHARE - 1)
    first_of = (tm, rd * SHARE)
    plane = [(tm, lax.rem(mp + i, n_map)) for i in range(1, n_map)]
    column = [(lax.rem(tm + i, n_tm), mp) for i in range(1, n_tm)]
    others = [lax.rem(rd + i, reducers) for i in range(1, reducers)]

    def greet(peer):
        pl.semaphore_signal(barrier, inc=1, device_id=peer, device_id_type=MESH)

    @pl.when(reduces)
    def _():
        for peer in column + plane:
            greet(peer)
        for peer in column:

            @pl.when(peer[0] > tm)
            def _(peer=peer):
                greet((peer[0], rd * SHARE))

    @pl.when(jnp.logical_not(reduces))
    def _():
        for other in others:
            greet((tm, other * SHARE + SHARE - 1))
        greet(near)

    def send(source, dest, peer, s):
        pltpu.make_async_remote_copy(
            src_ref=source,
            dst_ref=dest,
            send_sem=sends.at[0],
            recv_sem=recvs.at[s],
            device_id=peer,
            device_id_type=MESH,
        ).start()

    def wait_rows(rows, sem):
        ref = pts.at[0, pl.ds(0, rows), :]
        pltpu.make_async_copy(ref, ref, sem).wait()

    def every(ref, k, stride, count=arrived):
        return ref[pl.ds(k, count, stride=stride), :]

    lane = lax.broadcasted_iota(jnp.int32, (8, LANES), 1)
    group = lane // slots
    chunk_of = lax.broadcasted_iota(jnp.int32, (arrived, LANES), 0)
    turn_of = (
        lax.broadcasted_iota(jnp.int32, (arrived, LANES), 1) // slots + per * lax.rem(chunk_of, parts)
    )
    top = lax.broadcasted_iota(jnp.int32, (8, LANES), 0) < 4
    own_turn = [turn_of == t for t in range(n_tm)]
    sent[...] = jnp.zeros_like(sent)

    for copy in small:
        copy.wait()
    pose_pad[...] = jnp.zeros_like(pose_pad)
    for g in range(spread):
        pose_pad[0:6, g * own_scans : (g + 1) * own_scans] = pose_in[...]
    pose = pose_pad[...]
    cos, sin = jnp.cos(0.5 * pose), jnp.sin(0.5 * pose)
    cx, cy, cz = cos[0:1], cos[1:2], cos[2:3]
    sx, sy, sz = sin[0:1], sin[1:2], sin[2:3]
    pose_rows = [
        [
            cx * cy * cz + sx * sy * sz,
            sx * cy * cz - cx * sy * sz,
            cx * sy * cz + sx * cy * sz,
            cx * cy * sz - sx * sy * cz,
        ],
        [pose[3:4], pose[4:5], pose[5:6], pose[6:7]],
    ]
    scan_group = lane[0:1] // own_scans
    pose_lines = []
    for line, *others_of in pose_rows:
        for g, row in enumerate(others_of):
            line = jnp.where(scan_group == g + 1, row, line)
        pose_lines.append(line)

    ids = vox_in[...]
    row_of = lax.broadcasted_iota(jnp.int32, ids.shape, 0)
    lane_of = lax.broadcasted_iota(jnp.int32, ids.shape, 1)
    owner_of = row_of * per + lane_of // slots
    local_ids = jnp.where(ids >= 0, ids - owner_of * voxels, -1).astype(f32)
    sent[pl.ds(8 + VOX_ROW, chunks, stride=16), :] = local_ids
    sent[pl.ds(8 + SCAN_ROW, chunks, stride=16), :] = scan_in[...].astype(f32)

    theta, phi = angle_in[0:1, :], angle_in[1:2, :]
    sin_theta = jnp.sin(theta)
    own_normal = [sin_theta * jnp.cos(phi), sin_theta * jnp.sin(phi), jnp.cos(theta)]
    n_mine = aligned(part * n_size, n_size)
    for c in range(3):
        for h in range(halves):
            k = part * n_size + c * halves + h
            pair_n[pl.ds(k, 1), :] = own_normal[c][:, h * LANES : (h + 1) * LANES]

    def raw_moments(r):
        at = aligned(r * LANES, LANES, LANES)
        xyz = [pts[i, at, :].T for i in range(3)]
        sums = [jnp.sum(x, axis=0, keepdims=True) for x in xyz]
        sums += [jnp.sum(xyz[i] * xyz[j], axis=0, keepdims=True) for i, j in PAIRS]
        for k, row in enumerate(sums):
            sent[pl.ds(r * 16 + (k if k < 8 else 8 + LAST_ROW), 1), :] = row

    def load_step(r):
        points_copy(r).wait()
        for i in range(span // LANES):
            raw_moments(r * (span // LANES) + i)

    loop(loads, load_step)
    row_chunks = n_map // per

    def pack(peer_row):
        for u in range(parts):
            turned = []
            for g in range(per):
                for half in range(2):
                    at = [((u * per + a) * row_chunks + peer_row) * 16 + 8 * half for a in range(per)]
                    pieces = [sent[aligned(row, 8), :] for row in at]
                    turned.append(group_turn(pieces, g, group, slots))
            for i in range(per // SHARE):
                moments, marks, moments_b, marks_b = turned[4 * i : 4 * i + 4]
                base = (peer_row * (per // SHARE) + i) * parts + u
                send1[aligned(base * 16 + MARKS, 8), :] = jnp.where(
                    top, marks, pltpu.roll(marks_b, 4, 0)
                )
                send1[aligned(base * 16 + FIRSTS, 8), :] = jnp.where(
                    top, moments, pltpu.roll(moments_b, 4, 0)
                )
                send2[aligned(base * 8, 8), :] = jnp.where(
                    top, pltpu.roll(moments, 4, 0), moments_b
                )
                for k in range(SHARE):
                    send1[pl.ds(base * 16 + MARKS + 4 * k + POSE_ROW, 1), :] = pose_lines[k]

    loop(row_chunks, pack)

    from_plane = n_map - 1 + n_tm - 1
    pl.semaphore_wait(barrier, jnp.where(reduces, from_plane, reducers + tm))
    mine = aligned(mp * message, message)

    rest_mine = aligned(mp * rest_rows, rest_rows)

    def send_moments(other, peer):
        send(send1.at[aligned(other * message, message), :], recv1.at[mine, :], peer, 0)

    def send_rest(other, peer):
        send(send2.at[aligned(other * rest_rows, rest_rows), :], recv2.at[rest_mine, :], peer, 8)

    def normals_to(t, k):
        return recv_n.at[aligned((t * SHARE + k) * n_size, n_size), :]

    @pl.when(jnp.logical_not(reduces))
    def _():
        for peer in column:

            @pl.when(peer[0] < tm)
            def _(peer=peer):
                send(pair_n.at[n_mine, :], normals_to(tm, 0), (peer[0], near[1]), 1)

        send(pair_n.at[n_mine, :], pair_n.at[n_mine, :], near, 6)

    for send_part in (send_moments, send_rest):
        for other in others:
            send_part(other, (tm, other * SHARE + SHARE - 1))

        @pl.when(jnp.logical_not(reduces))
        def _(send_part=send_part):
            send_part(rd, near)

    eight = aligned(rd * 8, 8)

    def reduce_part():
        for peer in column:
            send(pair_n.at[pl.ds(n_size, n_size), :], normals_to(tm, 1), peer, 1)
        wait_rows(n_size, recvs.at[6])
        for peer in column:

            @pl.when(peer[0] > tm)
            def _(peer=peer):
                send(pair_n.at[pl.ds(0, n_size), :], normals_to(tm, 0), peer, 1)

        n_column = aligned(tm * SHARE * n_size, SHARE * n_size)
        recv1[mine, :] = send1[aligned(rd * message, message), :]
        recv2[rest_mine, :] = send2[aligned(rd * rest_rows, rest_rows), :]
        recv_n[n_column, :] = pair_n[...]
        for t in range(n_tm):
            world[pl.ds(3 * n_tm + t, arrived, stride=4 * n_tm), :] = jnp.where(
                own_turn[t], 1.0, 0.0
            )
        quads[...] = jnp.zeros_like(quads)
        late[...] = jnp.zeros_like(late)
        wait_rows((n_map - 1) * message, recvs.at[0])

        def place(q, side):
            i, u = (q // parts, q % parts) if isinstance(q, int) else (q // parts, lax.rem(q, parts))
            return (2 * i + side) * parts + u

        def couple_row(k, q, row, turn):
            return jnp.concatenate(
                [
                    recv1[pl.ds(place(q, side) * 16 + 4 * k + row + turn, 1), :]
                    for side in range(2)
                ],
                axis=1,
            )

        def couple_tile(ref, k, q, rows):
            return jnp.concatenate(
                [ref[aligned((k * in_plane + place(q, side)) * rows, rows), :] for side in range(2)],
                axis=1,
            )

        def marked(row, count):
            kind = bf16 if count <= 256 else f32
            line = jnp.broadcast_to(row, (16, 2 * LANES)).astype(kind)
            number = lax.broadcasted_iota(jnp.int32, (count, 2 * LANES), 0).astype(f32).astype(kind)
            found = jnp.concatenate([line] * (count // 16), axis=0) == number
            return jnp.where(found, jnp.ones((), kind), jnp.zeros((), kind)).astype(bf16)

        again = jnp.minimum(tm, 0)

        def scan_hot(k, q, turn):
            return marked(couple_row(k, q, SCAN_ROW, turn), scans)

        def vox_hot(k, q, turn):
            return marked(couple_row(k, q, VOX_ROW, turn), voxels)

        own_group = lane // own_scans
        def each_part(ref, row, stride):
            return jnp.concatenate(
                [every(ref, row + 4 * k, stride, in_plane) for k in range(SHARE)], axis=0
            )

        def gather(tables, high, low):
            value = jnp.take_along_axis(tables[0], low, axis=1, mode="promise_in_bounds")
            for h in range(1, len(tables)):
                other = jnp.take_along_axis(tables[h], low, axis=1, mode="promise_in_bounds")
                value = jnp.where(high == h, other, value)
            return value

        columns = []
        for h in range(wide):
            at = [(h * spread + a) * message + MARKS for a in range(spread)]
            tiles = [recv1[row : row + 8, :] for row in at]
            columns.append([group_turn(tiles, g, own_group, own_scans) for g in range(4)])
        scan_of = each_part(recv1, MARKS + SCAN_ROW, 16).astype(jnp.int32)
        scan_low, scan_high = jnp.bitwise_and(scan_of, LANES - 1), scan_of // LANES

        def pose_of(k, g):
            row = 4 * k + POSE_ROW
            rows = [
                jnp.broadcast_to(turned[g][row : row + 1], (arrived, LANES)) for turned in columns
            ]
            return gather(rows, scan_high, scan_low)

        qw, qx, qy, qz = [pose_of(0, g) for g in range(4)]
        shift = [pose_of(1, g) for g in range(3)]
        rot = [
            [1 - 2 * (qy * qy + qz * qz), 2 * (qx * qy - qw * qz), 2 * (qx * qz + qw * qy)],
            [2 * (qx * qy + qw * qz), 1 - 2 * (qx * qx + qz * qz), 2 * (qy * qz - qw * qx)],
            [2 * (qx * qz - qw * qy), 2 * (qy * qz + qw * qx), 1 - 2 * (qx * qx + qy * qy)],
        ]
        first = [each_part(recv1, FIRSTS + k, 16) for k in range(3)]
        turned_first = [sum(rot[i][j] * first[j] for j in range(3)) for i in range(3)]
        m1 = [turned_first[i] + npoints * shift[i] for i in range(3)]
        for c in range(3):
            for t in range(n_tm):
                world[pl.ds(c * n_tm + t, arrived, stride=4 * n_tm), :] = jnp.where(
                    own_turn[t], m1[c], 0.0
                )

        def voxel_sums(ref, rows, k, turn):
            def add(q):
                return lax.dot_general(
                    split(couple_tile(ref, k, q, rows)),
                    vox_hot(k, q, turn),
                    CONTRACT_LAST,
                    preferred_element_type=f32,
                )

            return joined(summed(couples, add, 3 * rows, voxels))

        sums = [voxel_sums(world, 4 * n_tm, k, 0) for k in range(SHARE)]
        wait_rows((n_tm - 1) * SHARE * n_size, recvs.at[1])
        normal = [
            [
                jnp.concatenate(
                    [
                        every(recv_n, k * n_size + c * halves + h, SHARE * n_size, n_tm)
                        for h in range(halves)
                    ],
                    axis=1,
                )
                for c in range(3)
            ]
            for k in range(SHARE)
        ]
        for k in range(SHARE):
            along = sum(normal[k][c] * sums[k][c * n_tm : (c + 1) * n_tm] for c in range(3))
            count = sums[k][3 * n_tm : 4 * n_tm]
            for h in range(halves):
                at = slice(h * LANES, (h + 1) * LANES)
                base = (k * halves + h) * a_rows
                send_a[base : base + n_tm, :] = along[:, at]
                send_a[base + n_tm : base + a_rows, :] = count[:, at]

        a_mine = aligned(tm * a_size, a_size)
        for peer in column:
            send(send_a, recv_a.at[a_mine, :], peer, 2)
        recv_a[a_mine, :] = send_a[...]

        vox_of = each_part(recv1, MARKS + VOX_ROW, 16).astype(jnp.int32)
        live = vox_of >= 0
        vox_low = jnp.bitwise_and(vox_of, LANES - 1)
        vox_high = jnp.where(live, vox_of, 0) // LANES

        def by_voxel(rows):
            value = None
            for t in range(n_tm):
                tables = []
                for h in range(halves):
                    each = [jnp.broadcast_to(rows(k, t, h), (in_plane, LANES)) for k in range(SHARE)]
                    tables.append(jnp.concatenate(each, axis=0))
                found = gather(tables, vox_high, vox_low)
                value = found if t == 0 else jnp.where(own_turn[t], found, value)
            return value

        n = []
        for c in range(3):
            value = by_voxel(
                lambda k, t, h: normal[k][c][t : t + 1, h * LANES : (h + 1) * LANES]
            )
            n.append(jnp.where(live, value, 0.0))
        wait_rows((n_map - 1) * rest_rows, recvs.at[8])
        second = [each_part(recv1, FIRSTS + 3, 16)]
        second += [each_part(recv2, k, 8) for k in range(4)]
        second += [each_part(recv1, MARKS + LAST_ROW, 16)]
        half_turned = [
            [sum(rot[i][k] * second[PAIR_ROW[(k, j)]] for k in range(3)) for j in range(3)]
            for i in range(3)
        ]
        m2 = [
            sum(half_turned[i][k] * rot[j][k] for k in range(3))
            + turned_first[i] * shift[j]
            + shift[i] * m1[j]
            for i, j in PAIRS
        ]
        quad = sum(n[i] ** 2 * m2[i] for i in range(3)) + 2.0 * sum(
            n[PAIRS[k][0]] * n[PAIRS[k][1]] * m2[k] for k in range(3, 6)
        )
        for t in range(n_tm):
            quads[pl.ds(t, arrived, stride=8), :] = jnp.where(own_turn[t], quad, 0.0)
        for k in range(SHARE):
            quad_sums = voxel_sums(quads, 8, k, again)
            for t in range(n_tm):
                for h in range(halves):
                    send_q[t, k * halves + h : k * halves + h + 1, :] = quad_sums[
                        t : t + 1, h * LANES : (h + 1) * LANES
                    ]
        for peer in column:
            send(send_q.at[peer[0]], recv_q.at[tm], peer, 3)
        recv_q[tm] = send_q[tm]

        def skew(v):
            return [
                n[2] * v[1] - n[1] * v[2],
                n[0] * v[2] - n[2] * v[0],
                n[1] * v[0] - n[0] * v[1],
            ]

        full = [[m2[PAIR_ROW[(i, j)]] for j in range(3)] for i in range(3)]
        skewed = [skew([full[k][j] for k in range(3)]) for j in range(3)]
        left = [[skewed[j][i] for j in range(3)] for i in range(3)]
        corner_block = [skew(left[i]) for i in range(3)]
        skew_first = skew(m1)
        found = {}
        for i in range(3):
            for j in range(3):
                if j >= i:
                    found[("h", i, j)] = corner_block[i][j]
                    found[("h", 3 + i, 3 + j)] = npoints * n[i] * n[j]
                found[("h", i, 3 + j)] = skew_first[i] * n[j]
        rest = n[0] * m1[0] + n[1] * m1[1] + n[2] * m1[2]
        for i in range(3):
            found[("g", i)] = sum(left[i][j] * n[j] for j in range(3))
            found[("g", 3 + i)] = n[i] * rest
        shares = skew_first + [npoints * n[i] for i in range(3)]
        for name, value in found.items():
            terms[pl.ds(ROWS.index(name), arrived, stride=32), :] = value
        for k in range(len(found), 32):
            terms[pl.ds(k, arrived, stride=32), :] = jnp.zeros_like(rest)

        def scan_sums(k, tile, rows, turn):
            def add(q):
                return lax.dot_general(
                    split(tile(k, q)),
                    scan_hot(k, q, turn),
                    CONTRACT_LAST,
                    preferred_element_type=f32,
                )

            return summed(couples, add, 3 * rows, scans)

        per_scan = scale * joined(
            sum(
                scan_sums(k, lambda k, q: couple_tile(terms, k, q, 32), 32, 0) for k in range(SHARE)
            )
        )
        for h in range(wide):
            pieces = [per_scan[8 * c : 8 * c + 8, h * LANES : (h + 1) * LANES] for c in range(4)]
            for b in range(spread):
                at = (h * spread + b) * 8
                send_h[at : at + 8, :] = group_turn(pieces, b, own_group, own_scans)
        for peer in plane:
            send(send_h.at[aligned(peer[1] * 8, 8), :], recv_h.at[eight, :], peer, 4)
        recv_h[eight, :] = send_h[aligned(mp * 8, 8), :]

        wait_rows((n_tm - 1) * a_size, recvs.at[2])
        offset_rows = []
        for k in range(SHARE):
            offsets = []
            for h in range(halves):
                base = (k * halves + h) * a_rows
                total = recv_a[base : base + a_rows, :]
                for t in range(1, n_tm):
                    total = total + recv_a[t * a_size + base : t * a_size + base + a_rows, :]
                floor = jnp.maximum(total[n_tm:] * npoints, 1.0)
                offset = total[:n_tm] / floor
                total_a[base : base + n_tm, :] = offset
                total_a[base + n_tm : base + a_rows, :] = floor
                offsets.append(offset)
            offset_rows.append(offsets)
        offset_of = by_voxel(lambda k, t, h: offset_rows[k][h][t : t + 1])
        for i in range(6):
            late[pl.ds(i, arrived, stride=8), :] = shares[i] * offset_of
        moved = scale * joined(
            sum(
                scan_sums(k, lambda k, q: couple_tile(late, k, q, 8), 8, again)
                for k in range(SHARE)
            )
        )
        for h in range(wide):
            send_g[h * 8 : h * 8 + 8, :] = moved[:, h * LANES : (h + 1) * LANES]
        for peer in plane:
            source = send_g.at[aligned(peer[1] // spread * 8, 8), :]
            send(source, recv_g.at[eight, :], peer, 5)
        recv_g[eight, :] = send_g[aligned(mp // spread * 8, 8), :]

        pltpu.make_async_copy(
            recv_q.at[pl.ds(0, n_tm - 1)], recv_q.at[pl.ds(0, n_tm - 1)], recvs.at[3]
        ).wait()
        quad_total = recv_q[0]
        for t in range(1, n_tm):
            quad_total = quad_total + recv_q[t]
        own_offset = total_a[pl.ds(tm, SHARE * halves, stride=a_rows), :]
        own_floor = total_a[pl.ds(n_tm + tm, SHARE * halves, stride=a_rows), :]
        cost = quad_total / own_floor - own_offset**2
        send_c[...] = cost[0:halves]
        send(send_c, recv_c, first_of, 7)
        recv_c[...] = cost[halves:]

    pl.when(reduces)(reduce_part)


    def wait_plane(s):
        @pl.when(reduces)
        def _():
            wait_rows((reducers - 1) * 8, recvs.at[s])

        @pl.when(jnp.logical_not(reduces))
        def _():
            wait_rows(reducers * 8, recvs.at[s])

    lines[...] = jnp.zeros_like(lines)
    wait_plane(4)
    total = recv_h[0:8, :]
    for m in range(1, reducers):
        total = total + recv_h[m * 8 : m * 8 + 8, :]
    lined = [total] + [pltpu.roll(total, LANES - own_scans * c, 1) for c in range(1, 4)]

    def row_at(name):
        k = ROWS.index(name)
        return lined[k // 8][k % 8 : k % 8 + 1]

    for i in range(6):
        for j in range(6):
            lines[6 * i + j : 6 * i + j + 1, :] = row_at(("h", min(i, j), max(i, j)))
    hess_out[...] = lines[...].T[0:own_scans, 0:36]
    gradient = jnp.concatenate([row_at(("g", i)) for i in range(6)], axis=0)

    @pl.when(jnp.logical_not(reduces))
    def _():
        pltpu.make_async_copy(recv_c, recv_c, recvs.at[7]).wait()

    for h in range(halves):
        cost_out[:, h * LANES : (h + 1) * LANES] = recv_c[h : h + 1, :]

    wait_plane(5)
    change = recv_g[0:8, :]
    for m in range(1, reducers):
        change = change + recv_g[m * 8 : m * 8 + 8, :]
    change = pltpu.roll(change, LANES - own_scans * lax.rem(mp, spread), 1)
    grad_out[...] = (gradient - change[0:6])[:, 0:own_scans]

    for t in range(n_tm):

        @pl.when(jnp.logical_and(reduces, tm == t))
        def _(t=t):
            rows = (reducers - 1) * (message + rest_rows) + (n_map - 1) * 16 + halves
            rows += (n_tm - 1) * (n_size + a_size + SHARE * halves) + (n_tm - 1 - t) * n_size
            wait_rows(rows, sends.at[0])

        @pl.when(jnp.logical_and(jnp.logical_not(reduces), tm == t))
        def _(t=t):
            wait_rows(reducers * (message + rest_rows) + (t + 1) * n_size, sends.at[0])


def finish(hess_in, grad_in, cost_in, hess_out, grad_out, cost_out, sems):
    copies = [
        pltpu.make_async_copy(src, dst, sems.at[i])
        for i, (src, dst) in enumerate(
            [(hess_in, hess_out), (grad_in, grad_out), (cost_in, cost_out)]
        )
    ]
    for copy in copies:
        copy.start()
    for copy in copies:
        copy.wait()


def local(points, poses, normal_angles, voxel_ids, scan_ids):
    blocks, npoints = points.shape[1:]
    n_tm, n_map = lax.axis_size("tm"), lax.axis_size("map")
    devices = n_tm * n_map
    slots = blocks // devices
    chunks = blocks // LANES
    vox_count = normal_angles.shape[1]
    own_scans = poses.shape[1]
    assert npoints == LANES and slots * 4 == LANES and own_scans * 4 == LANES
    assert n_map % 4 == 0 and n_map % SHARE == 0 and n_tm % 4 == 0 and vox_count % LANES == 0
    scale = own_scans * devices / (blocks * devices * npoints)
    f32 = jnp.float32
    scans = own_scans * n_map
    halves = vox_count // LANES
    in_plane = n_map * n_tm // 4
    reducers = n_map // SHARE
    packed = reducers * n_tm // 4
    arrived = SHARE * n_map * n_tm // 4
    n_rows = -(-3 * halves // 8) * 8
    a_rows = SHARE * 2 * n_tm * halves
    hbm = pl.BlockSpec(memory_space=pl.ANY)
    vmem = pl.BlockSpec(memory_space=pltpu.VMEM)
    shapes = [(own_scans, 36), (6, own_scans), (1, vox_count)]
    results = pl.pallas_call(
        functools.partial(kernel, (n_tm, n_map, slots, float(npoints), scale)),
        out_shape=tuple(pltpu.VMEM(shape, f32) for shape in shapes),
        in_specs=[hbm] * 5,
        out_specs=(vmem,) * 3,
        scratch_shapes=[
            pltpu.VMEM(points.shape, f32),
            pltpu.VMEM(poses.shape, f32),
            pltpu.VMEM(normal_angles.shape, f32),
            pltpu.VMEM((chunks, LANES), jnp.int32),
            pltpu.VMEM((chunks, LANES), jnp.int32),
            pltpu.VMEM((8, LANES), f32),
            pltpu.VMEM((chunks * 16, LANES), f32),
            pltpu.VMEM((packed * 16, LANES), f32),
            pltpu.VMEM((in_plane * 16, LANES), f32),
            pltpu.VMEM((packed * 8, LANES), f32),
            pltpu.VMEM((in_plane * 8, LANES), f32),
            pltpu.VMEM((SHARE * n_rows, LANES), f32),
            pltpu.VMEM((n_tm * SHARE * n_rows, LANES), f32),
            pltpu.VMEM((arrived * 4 * n_tm, LANES), f32),
            pltpu.VMEM((a_rows, LANES), f32),
            pltpu.VMEM((n_tm * a_rows, LANES), f32),
            pltpu.VMEM((a_rows, LANES), f32),
            pltpu.VMEM((arrived * 8, LANES), f32),
            pltpu.VMEM((n_tm, SHARE * halves, LANES), f32),
            pltpu.VMEM((n_tm, SHARE * halves, LANES), f32),
            pltpu.VMEM((halves, LANES), f32),
            pltpu.VMEM((halves, LANES), f32),
            pltpu.VMEM((arrived * 32, LANES), f32),
            pltpu.VMEM((arrived * 8, LANES), f32),
            pltpu.VMEM((n_map * 8, LANES), f32),
            pltpu.VMEM((reducers * 8, LANES), f32),
            pltpu.VMEM((scans // LANES * 8, LANES), f32),
            pltpu.VMEM((reducers * 8, LANES), f32),
            pltpu.VMEM((LANES, LANES), f32),
            pltpu.SemaphoreType.DMA((2,)),
            pltpu.SemaphoreType.DMA((4,)),
            pltpu.SemaphoreType.DMA((1,)),
            pltpu.SemaphoreType.DMA((9,)),
        ],
        compiler_params=pltpu.CompilerParams(collective_id=0, has_side_effects=True),
    )(
        points,
        poses,
        normal_angles,
        voxel_ids.reshape(chunks, LANES),
        scan_ids.reshape(chunks, LANES),
    )
    hess, grad, cost = pl.pallas_call(
        finish,
        out_shape=tuple(jax.ShapeDtypeStruct(shape, f32) for shape in shapes),
        in_specs=[vmem] * 3,
        out_specs=(hbm,) * 3,
        scratch_shapes=[pltpu.SemaphoreType.DMA((3,))],
    )(*[pltpu.with_memory_space_constraint(x, pltpu.VMEM) for x in results])
    return hess.T, grad, cost.reshape(vox_count)


def solution(mesh):
    return jax.shard_map(
        local,
        mesh=mesh,
        in_specs=(
            P(None, ("tm", "map"), None),
            P(None, ("tm", "map")),
            P(None, ("tm", "map")),
            P(("tm", "map")),
            P(("tm", "map")),
        ),
        out_specs=(P(None, ("tm", "map")), P(None, ("tm", "map")), P(("tm", "map"))),
        check_vma=False,
    )
```

```python
import functools

import jax
import jax.numpy as jnp
from jax import lax
from jax.experimental import pallas as pl
from jax.experimental.pallas import tpu as pltpu
from jax.sharding import PartitionSpec as P

LANES = 128
MESH = pl.DeviceIdType.MESH
PAIRS = [(0, 0), (1, 1), (2, 2), (0, 1), (0, 2), (1, 2)]
PAIR_ROW = {}
for _k, (_i, _j) in enumerate(PAIRS):
    PAIR_ROW[(_i, _j)] = _k
    PAIR_ROW[(_j, _i)] = _k

ROWS = [("h", i, j) for i in range(6) for j in range(i, 6)] + [("g", i) for i in range(6)]

MARKS, FIRSTS = 0, 8
VOX_ROW, SCAN_ROW, LAST_ROW, POSE_ROW = 0, 1, 2, 3
SHARE = 2
LEVELS = 4
CONTRACT_LAST = (((1,), (1,)), ((), ()))


def split(x):
    high = x.astype(jnp.bfloat16).astype(jnp.float32)
    rest = x - high
    mid = rest.astype(jnp.bfloat16).astype(jnp.float32)
    return jnp.concatenate([high, mid, rest - mid], axis=0).astype(jnp.bfloat16)


def joined(y):
    rows = y.shape[0] // 3
    return y[:rows] + y[rows : 2 * rows] + y[2 * rows :]


def group_turn(pieces, out_group, group, lanes_per):
    total = None
    for a, piece in enumerate(pieces):
        shift = ((a - out_group) * lanes_per) % LANES
        moved = piece if shift == 0 else pltpu.roll(piece, shift, 1)
        total = moved if total is None else jnp.where(group == a, moved, total)
    return total


def loop(count, body):
    if count <= 8:
        for i in range(count):
            body(i)
    else:
        def step(i, carry):
            body(i)
            return carry

        lax.fori_loop(0, count, step, 0)


def summed(count, body, rows, columns):
    acc = jnp.zeros((rows, columns), jnp.float32)
    if count <= 8:
        for i in range(count):
            acc = acc + body(i)
        return acc
    return lax.fori_loop(0, count, lambda i, total: total + body(i), acc)


def aligned(start, size, unit=8):
    if not isinstance(start, int):
        start = pl.multiple_of(start, unit)
    return pl.ds(start, size)


def kernel(
    sizes,
    points,
    poses,
    angles,
    voxel_ids,
    scan_ids,
    hess_out,
    grad_out,
    cost_out,
    pts,
    pose_in,
    angle_in,
    vox_in,
    scan_in,
    pose_pad,
    sent,
    send1,
    recv1,
    send2,
    recv2,
    pair_n,
    recv_n,
    world,
    send_a,
    recv_a,
    total_a,
    quads,
    send_q,
    recv_q,
    send_c,
    recv_c,
    terms,
    late,
    send_h,
    recv_h,
    send_g,
    recv_g,
    lines,
    pts_sem,
    in_sem,
    sends,
    recvs,
):
    n_tm, n_map, slots, npoints, scale = sizes
    reducers = n_map // SHARE
    blocks = pts.shape[1]
    chunks = blocks // LANES
    per = LANES // slots
    own_scans = pose_in.shape[1]
    spread = LANES // own_scans
    scans = own_scans * n_map
    wide = scans // LANES
    voxels = angle_in.shape[1]
    halves = voxels // LANES
    parts = n_tm // per
    step = SHARE * parts
    arrived = n_map * step
    couples = n_map // 2 * parts
    message = parts * 16
    rest_rows = parts * 8
    in_plane = n_map * parts
    n_size = pair_n.shape[0] // SHARE
    in_level = n_map // LEVELS
    a_rows = 2 * n_tm
    a_size = SHARE * halves * a_rows
    tm = lax.axis_index("tm")
    mp = lax.axis_index("map")
    rd = mp // SHARE
    part = lax.rem(mp, SHARE)
    reduces = part == SHARE - 1
    f32, bf16 = jnp.float32, jnp.bfloat16

    small = [
        pltpu.make_async_copy(src, dst, in_sem.at[i])
        for i, (src, dst) in enumerate(
            [(poses, pose_in), (angles, angle_in), (voxel_ids, vox_in), (scan_ids, scan_in)]
        )
    ]
    loads = pts_sem.shape[0]
    span = blocks // loads

    def points_copy(r):
        rows = pl.ds(r * span, span)
        return pltpu.make_async_copy(points.at[:, rows, :], pts.at[:, rows, :], pts_sem.at[r])

    for copy in small:
        copy.start()
    loop(loads, lambda r: points_copy(r).start())
    barrier = pltpu.get_barrier_semaphore()
    near = (tm, rd * SHARE + SHARE - 1)
    first_of = (tm, rd * SHARE)
    plane = [(tm, lax.rem(mp + i, n_map)) for i in range(1, n_map)]
    column = [(lax.rem(tm + i, n_tm), mp) for i in range(1, n_tm)]
    others = [lax.rem(rd + i, reducers) for i in range(1, reducers)]

    def greet(peer):
        pl.semaphore_signal(barrier, inc=1, device_id=peer, device_id_type=MESH)

    @pl.when(reduces)
    def _():
        for peer in column + plane:
            greet(peer)
        for peer in column:

            @pl.when(peer[0] > tm)
            def _(peer=peer):
                greet((peer[0], rd * SHARE))

    @pl.when(jnp.logical_not(reduces))
    def _():
        for other in others:
            greet((tm, other * SHARE + SHARE - 1))
        greet(near)

    def send(source, dest, peer, s):
        pltpu.make_async_remote_copy(
            src_ref=source,
            dst_ref=dest,
            send_sem=sends.at[0],
            recv_sem=recvs.at[s],
            device_id=peer,
            device_id_type=MESH,
        ).start()

    def wait_rows(rows, sem):
        ref = pts.at[0, pl.ds(0, rows), :]
        pltpu.make_async_copy(ref, ref, sem).wait()

    def every(ref, k, stride, count=arrived):
        return ref[pl.ds(k, count, stride=stride), :]

    lane = lax.broadcasted_iota(jnp.int32, (8, LANES), 1)
    group = lane // slots
    chunk_of = lax.broadcasted_iota(jnp.int32, (arrived, LANES), 0)
    turn_of = (
        lax.broadcasted_iota(jnp.int32, (arrived, LANES), 1) // slots + per * lax.rem(chunk_of, parts)
    )
    top = lax.broadcasted_iota(jnp.int32, (8, LANES), 0) < 4
    own_turn = [turn_of == t for t in range(n_tm)]
    sent[...] = jnp.zeros_like(sent)

    for copy in small:
        copy.wait()
    pose_pad[...] = jnp.zeros_like(pose_pad)
    for g in range(spread):
        pose_pad[0:6, g * own_scans : (g + 1) * own_scans] = pose_in[...]
    pose = pose_pad[...]
    cos, sin = jnp.cos(0.5 * pose), jnp.sin(0.5 * pose)
    cx, cy, cz = cos[0:1], cos[1:2], cos[2:3]
    sx, sy, sz = sin[0:1], sin[1:2], sin[2:3]
    pose_rows = [
        [
            cx * cy * cz + sx * sy * sz,
            sx * cy * cz - cx * sy * sz,
            cx * sy * cz + sx * cy * sz,
            cx * cy * sz - sx * sy * cz,
        ],
        [pose[3:4], pose[4:5], pose[5:6], pose[6:7]],
    ]
    scan_group = lane[0:1] // own_scans
    pose_lines = []
    for line, *others_of in pose_rows:
        for g, row in enumerate(others_of):
            line = jnp.where(scan_group == g + 1, row, line)
        pose_lines.append(line)

    ids = vox_in[...]
    row_of = lax.broadcasted_iota(jnp.int32, ids.shape, 0)
    lane_of = lax.broadcasted_iota(jnp.int32, ids.shape, 1)
    owner_of = row_of * per + lane_of // slots
    local_ids = jnp.where(ids >= 0, ids - owner_of * voxels, -1).astype(f32)
    sent[pl.ds(8 + VOX_ROW, chunks, stride=16), :] = local_ids
    sent[pl.ds(8 + SCAN_ROW, chunks, stride=16), :] = scan_in[...].astype(f32)

    theta, phi = angle_in[0:1, :], angle_in[1:2, :]
    sin_theta = jnp.sin(theta)
    own_normal = [sin_theta * jnp.cos(phi), sin_theta * jnp.sin(phi), jnp.cos(theta)]
    n_mine = aligned(part * n_size, n_size)
    for c in range(3):
        for h in range(halves):
            k = part * n_size + c * halves + h
            pair_n[pl.ds(k, 1), :] = own_normal[c][:, h * LANES : (h + 1) * LANES]

    def raw_moments(r):
        at = aligned(r * LANES, LANES, LANES)
        xyz = [pts[i, at, :].T for i in range(3)]
        sums = [jnp.sum(x, axis=0, keepdims=True) for x in xyz]
        sums += [jnp.sum(xyz[i] * xyz[j], axis=0, keepdims=True) for i, j in PAIRS]
        for k, row in enumerate(sums):
            sent[pl.ds(r * 16 + (k if k < 8 else 8 + LAST_ROW), 1), :] = row

    def load_step(r):
        points_copy(r).wait()
        for i in range(span // LANES):
            raw_moments(r * (span // LANES) + i)

    loop(loads, load_step)
    row_chunks = n_map // per

    def pack(peer_row):
        for u in range(parts):
            turned = []
            for g in range(per):
                for half in range(2):
                    at = [((u * per + a) * row_chunks + peer_row) * 16 + 8 * half for a in range(per)]
                    pieces = [sent[aligned(row, 8), :] for row in at]
                    turned.append(group_turn(pieces, g, group, slots))
            for i in range(per // SHARE):
                moments, marks, moments_b, marks_b = turned[4 * i : 4 * i + 4]
                base = (peer_row * (per // SHARE) + i) * parts + u
                send1[aligned(base * 16 + MARKS, 8), :] = jnp.where(
                    top, marks, pltpu.roll(marks_b, 4, 0)
                )
                send1[aligned(base * 16 + FIRSTS, 8), :] = jnp.where(
                    top, moments, pltpu.roll(moments_b, 4, 0)
                )
                send2[aligned(base * 8, 8), :] = jnp.where(
                    top, pltpu.roll(moments, 4, 0), moments_b
                )
                for k in range(SHARE):
                    send1[pl.ds(base * 16 + MARKS + 4 * k + POSE_ROW, 1), :] = pose_lines[k]

    loop(row_chunks, pack)

    from_plane = n_map - 1 + n_tm - 1
    pl.semaphore_wait(barrier, jnp.where(reduces, from_plane, reducers + tm))
    mine = aligned(mp * message, message)

    rest_mine = aligned(mp * rest_rows, rest_rows)

    def send_moments(other, peer):
        send(send1.at[aligned(other * message, message), :], recv1.at[mine, :], peer, 0)

    def send_rest(other, peer):
        send(send2.at[aligned(other * rest_rows, rest_rows), :], recv2.at[rest_mine, :], peer, 8)

    def normals_to(t, k):
        return recv_n.at[aligned((t * SHARE + k) * n_size, n_size), :]

    @pl.when(jnp.logical_not(reduces))
    def _():
        for peer in column:

            @pl.when(peer[0] < tm)
            def _(peer=peer):
                send(pair_n.at[n_mine, :], normals_to(tm, 0), (peer[0], near[1]), 1)

        send(pair_n.at[n_mine, :], pair_n.at[n_mine, :], near, 6)

    for send_part in (send_moments, send_rest):
        for other in others:
            send_part(other, (tm, other * SHARE + SHARE - 1))

        @pl.when(jnp.logical_not(reduces))
        def _(send_part=send_part):
            send_part(rd, near)

    eight = aligned(rd * 8, 8)

    def reduce_part():
        for peer in column:
            send(pair_n.at[pl.ds(n_size, n_size), :], normals_to(tm, 1), peer, 1)
        wait_rows(n_size, recvs.at[6])
        for peer in column:

            @pl.when(peer[0] > tm)
            def _(peer=peer):
                send(pair_n.at[pl.ds(0, n_size), :], normals_to(tm, 0), peer, 1)

        n_column = aligned(tm * SHARE * n_size, SHARE * n_size)
        recv1[mine, :] = send1[aligned(rd * message, message), :]
        recv2[rest_mine, :] = send2[aligned(rd * rest_rows, rest_rows), :]
        recv_n[n_column, :] = pair_n[...]
        for t in range(n_tm):
            world[pl.ds(3 * n_tm + t, arrived, stride=4 * n_tm), :] = jnp.where(
                own_turn[t], 1.0, 0.0
            )
        quads[...] = jnp.zeros_like(quads)
        send_g[...] = jnp.zeros_like(send_g)
        late[...] = jnp.zeros_like(late)
        wait_rows((n_map - 1) * message, recvs.at[0])

        def place(q, side):
            i, u = (q // parts, q % parts) if isinstance(q, int) else (q // parts, lax.rem(q, parts))
            return (2 * i + side) * parts + u

        def couple_row(k, q, row, turn):
            return jnp.concatenate(
                [
                    recv1[pl.ds(place(q, side) * 16 + 4 * k + row + turn, 1), :]
                    for side in range(2)
                ],
                axis=1,
            )

        def couple_tile(ref, k, q, rows):
            return jnp.concatenate(
                [ref[aligned((k * in_plane + place(q, side)) * rows, rows), :] for side in range(2)],
                axis=1,
            )

        def marked(row, count):
            kind = bf16 if count <= 256 else f32
            line = jnp.broadcast_to(row, (16, 2 * LANES)).astype(kind)
            number = lax.broadcasted_iota(jnp.int32, (count, 2 * LANES), 0).astype(f32).astype(kind)
            found = jnp.concatenate([line] * (count // 16), axis=0) == number
            return jnp.where(found, jnp.ones((), kind), jnp.zeros((), kind)).astype(bf16)

        def two_level(values, row, levels, count):
            low = count // levels
            number = row.astype(jnp.int32)
            high_line = jnp.broadcast_to(number // low, (16, 2 * LANES)).astype(f32).astype(bf16)
            low_row = jnp.bitwise_and(number, low - 1).astype(f32)
            three = split(values)
            rows = three.shape[0]
            high = jnp.concatenate([high_line] * (-(-rows // 16)), axis=0)[:rows]
            picked = [
                jnp.where(high == jnp.full((), h, bf16), three, jnp.zeros((), bf16))
                for h in range(levels)
            ]
            return jnp.concatenate(picked, axis=0), marked(low_row, low)

        def product(left, right):
            return lax.dot_general(left, right, CONTRACT_LAST, preferred_element_type=f32)

        def products(each_side, kinds, rows, columns):
            if couples > 8:
                return sum(
                    summed(couples, lambda q, k=k: product(*each_side(k, q)), rows, columns)
                    for k in kinds
                )
            sides = [each_side(k, q) for k in kinds for q in range(couples)]
            return product(*[jnp.concatenate(side, axis=1) for side in zip(*sides)])

        again = jnp.minimum(tm, 0)

        def scan_hot(k, q, turn):
            return marked(couple_row(k, q, SCAN_ROW, turn), scans)

        def vox_hot(k, q, turn):
            return marked(couple_row(k, q, VOX_ROW, turn), voxels)

        own_group = lane // own_scans
        def each_part(ref, row, stride):
            return jnp.concatenate(
                [every(ref, row + 4 * k, stride, in_plane) for k in range(SHARE)], axis=0
            )

        def gather(tables, high, low):
            value = jnp.take_along_axis(tables[0], low, axis=1, mode="promise_in_bounds")
            for h in range(1, len(tables)):
                other = jnp.take_along_axis(tables[h], low, axis=1, mode="promise_in_bounds")
                value = jnp.where(high == h, other, value)
            return value

        columns = []
        for h in range(wide):
            at = [(h * spread + a) * message + MARKS for a in range(spread)]
            tiles = [recv1[row : row + 8, :] for row in at]
            columns.append([group_turn(tiles, g, own_group, own_scans) for g in range(4)])
        scan_of = each_part(recv1, MARKS + SCAN_ROW, 16).astype(jnp.int32)
        scan_low, scan_high = jnp.bitwise_and(scan_of, LANES - 1), scan_of // LANES

        def pose_of(k, g):
            row = 4 * k + POSE_ROW
            rows = [
                jnp.broadcast_to(turned[g][row : row + 1], (arrived, LANES)) for turned in columns
            ]
            return gather(rows, scan_high, scan_low)

        qw, qx, qy, qz = [pose_of(0, g) for g in range(4)]
        shift = [pose_of(1, g) for g in range(3)]
        rot = [
            [1 - 2 * (qy * qy + qz * qz), 2 * (qx * qy - qw * qz), 2 * (qx * qz + qw * qy)],
            [2 * (qx * qy + qw * qz), 1 - 2 * (qx * qx + qz * qz), 2 * (qy * qz - qw * qx)],
            [2 * (qx * qz - qw * qy), 2 * (qy * qz + qw * qx), 1 - 2 * (qx * qx + qy * qy)],
        ]
        first = [each_part(recv1, FIRSTS + k, 16) for k in range(3)]
        turned_first = [sum(rot[i][j] * first[j] for j in range(3)) for i in range(3)]
        m1 = [turned_first[i] + npoints * shift[i] for i in range(3)]
        for c in range(3):
            for t in range(n_tm):
                world[pl.ds(c * n_tm + t, arrived, stride=4 * n_tm), :] = jnp.where(
                    own_turn[t], m1[c], 0.0
                )

        def voxel_sums(ref, rows, k, turn):
            def add(q):
                return lax.dot_general(
                    split(couple_tile(ref, k, q, rows)),
                    vox_hot(k, q, turn),
                    CONTRACT_LAST,
                    preferred_element_type=f32,
                )

            return joined(summed(couples, add, 3 * rows, voxels))

        def first_sums(k):
            rows = 12 * n_tm

            def sides(k, q):
                values = couple_tile(world, k, q, 4 * n_tm)
                return two_level(values, couple_row(k, q, VOX_ROW, 0), halves, voxels)

            found = products(sides, [k], halves * rows, LANES)
            return jnp.concatenate(
                [joined(found[h * rows : (h + 1) * rows]) for h in range(halves)], axis=1
            )

        sums = [first_sums(k) for k in range(SHARE)]
        wait_rows((n_tm - 1) * SHARE * n_size, recvs.at[1])
        normal = [
            [
                jnp.concatenate(
                    [
                        every(recv_n, k * n_size + c * halves + h, SHARE * n_size, n_tm)
                        for h in range(halves)
                    ],
                    axis=1,
                )
                for c in range(3)
            ]
            for k in range(SHARE)
        ]
        for k in range(SHARE):
            along = sum(normal[k][c] * sums[k][c * n_tm : (c + 1) * n_tm] for c in range(3))
            count = sums[k][3 * n_tm : 4 * n_tm]
            for h in range(halves):
                at = slice(h * LANES, (h + 1) * LANES)
                base = (k * halves + h) * a_rows
                send_a[base : base + n_tm, :] = along[:, at]
                send_a[base + n_tm : base + a_rows, :] = count[:, at]

        a_mine = aligned(tm * a_size, a_size)
        for peer in column:
            send(send_a, recv_a.at[a_mine, :], peer, 2)
        recv_a[a_mine, :] = send_a[...]

        vox_of = each_part(recv1, MARKS + VOX_ROW, 16).astype(jnp.int32)
        live = vox_of >= 0
        vox_low = jnp.bitwise_and(vox_of, LANES - 1)
        vox_high = jnp.where(live, vox_of, 0) // LANES

        def by_voxel(rows):
            value = None
            for t in range(n_tm):
                tables = []
                for h in range(halves):
                    each = [jnp.broadcast_to(rows(k, t, h), (in_plane, LANES)) for k in range(SHARE)]
                    tables.append(jnp.concatenate(each, axis=0))
                found = gather(tables, vox_high, vox_low)
                value = found if t == 0 else jnp.where(own_turn[t], found, value)
            return value

        n = []
        for c in range(3):
            value = by_voxel(
                lambda k, t, h: normal[k][c][t : t + 1, h * LANES : (h + 1) * LANES]
            )
            n.append(jnp.where(live, value, 0.0))
        wait_rows((n_map - 1) * rest_rows, recvs.at[8])
        second = [each_part(recv1, FIRSTS + 3, 16)]
        second += [each_part(recv2, k, 8) for k in range(4)]
        second += [each_part(recv1, MARKS + LAST_ROW, 16)]
        half_turned = [
            [sum(rot[i][k] * second[PAIR_ROW[(k, j)]] for k in range(3)) for j in range(3)]
            for i in range(3)
        ]
        m2 = [
            sum(half_turned[i][k] * rot[j][k] for k in range(3))
            + turned_first[i] * shift[j]
            + shift[i] * m1[j]
            for i, j in PAIRS
        ]
        quad = sum(n[i] ** 2 * m2[i] for i in range(3)) + 2.0 * sum(
            n[PAIRS[k][0]] * n[PAIRS[k][1]] * m2[k] for k in range(3, 6)
        )
        for t in range(n_tm):
            quads[pl.ds(t, arrived, stride=8), :] = jnp.where(own_turn[t], quad, 0.0)
        for k in range(SHARE):
            quad_sums = voxel_sums(quads, 8, k, again)
            for t in range(n_tm):
                for h in range(halves):
                    send_q[t, k * halves + h : k * halves + h + 1, :] = quad_sums[
                        t : t + 1, h * LANES : (h + 1) * LANES
                    ]
        for peer in column:
            send(send_q.at[peer[0]], recv_q.at[tm], peer, 3)
        recv_q[tm] = send_q[tm]

        def skew(v):
            return [
                n[2] * v[1] - n[1] * v[2],
                n[0] * v[2] - n[2] * v[0],
                n[1] * v[0] - n[0] * v[1],
            ]

        full = [[m2[PAIR_ROW[(i, j)]] for j in range(3)] for i in range(3)]
        skewed = [skew([full[k][j] for k in range(3)]) for j in range(3)]
        left = [[skewed[j][i] for j in range(3)] for i in range(3)]
        corner_block = [skew(left[i]) for i in range(3)]
        skew_first = skew(m1)
        found = {}
        for i in range(3):
            for j in range(3):
                if j >= i:
                    found[("h", i, j)] = corner_block[i][j]
                    found[("h", 3 + i, 3 + j)] = npoints * n[i] * n[j]
                found[("h", i, 3 + j)] = skew_first[i] * n[j]
        rest = n[0] * m1[0] + n[1] * m1[1] + n[2] * m1[2]
        for i in range(3):
            found[("g", i)] = sum(left[i][j] * n[j] for j in range(3))
            found[("g", 3 + i)] = n[i] * rest
        shares = skew_first + [npoints * n[i] for i in range(3)]
        for name, value in found.items():
            terms[pl.ds(ROWS.index(name), arrived, stride=32), :] = value
        for k in range(len(found), 32):
            terms[pl.ds(k, arrived, stride=32), :] = jnp.zeros_like(rest)

        def scan_sums(k, tile, rows, turn):
            def add(q):
                return lax.dot_general(
                    split(tile(k, q)),
                    scan_hot(k, q, turn),
                    CONTRACT_LAST,
                    preferred_element_type=f32,
                )

            return summed(couples, add, 3 * rows, scans)

        per_scan = scale * joined(
            sum(
                scan_sums(k, lambda k, q: couple_tile(terms, k, q, 32), 32, 0) for k in range(SHARE)
            )
        )
        for h in range(wide):
            pieces = [per_scan[8 * c : 8 * c + 8, h * LANES : (h + 1) * LANES] for c in range(4)]
            for b in range(spread):
                at = (h * spread + b) * 8
                send_h[at : at + 8, :] = group_turn(pieces, b, own_group, own_scans)
        for peer in plane:
            send(send_h.at[aligned(peer[1] * 8, 8), :], recv_h.at[eight, :], peer, 4)
        recv_h[eight, :] = send_h[aligned(mp * 8, 8), :]

        wait_rows((n_tm - 1) * a_size, recvs.at[2])
        offset_rows = []
        for k in range(SHARE):
            offsets = []
            for h in range(halves):
                base = (k * halves + h) * a_rows
                total = recv_a[base : base + a_rows, :]
                for t in range(1, n_tm):
                    total = total + recv_a[t * a_size + base : t * a_size + base + a_rows, :]
                floor = jnp.maximum(total[n_tm:] * npoints, 1.0)
                offset = total[:n_tm] / floor
                total_a[base : base + n_tm, :] = offset
                total_a[base + n_tm : base + a_rows, :] = floor
                offsets.append(offset)
            offset_rows.append(offsets)
        offset_of = by_voxel(lambda k, t, h: offset_rows[k][h][t : t + 1])
        for i in range(6):
            late[pl.ds(i, arrived, stride=8), :] = shares[i] * offset_of

        def late_sides(k, q):
            values = couple_tile(late, k, q, 8)
            return two_level(values, couple_row(k, q, SCAN_ROW, again), LEVELS, scans)

        moved = products(late_sides, range(SHARE), LEVELS * 24, scans // LEVELS)
        for h in range(LEVELS):
            send_g[h * 8 : h * 8 + 8, 0 : scans // LEVELS] = scale * joined(
                moved[h * 24 : h * 24 + 24]
            )
        for peer in plane:
            source = send_g.at[aligned(peer[1] // in_level * 8, 8), :]
            send(source, recv_g.at[eight, :], peer, 5)
        recv_g[eight, :] = send_g[aligned(mp // in_level * 8, 8), :]

        pltpu.make_async_copy(
            recv_q.at[pl.ds(0, n_tm - 1)], recv_q.at[pl.ds(0, n_tm - 1)], recvs.at[3]
        ).wait()
        quad_total = recv_q[0]
        for t in range(1, n_tm):
            quad_total = quad_total + recv_q[t]
        own_offset = total_a[pl.ds(tm, SHARE * halves, stride=a_rows), :]
        own_floor = total_a[pl.ds(n_tm + tm, SHARE * halves, stride=a_rows), :]
        cost = quad_total / own_floor - own_offset**2
        send_c[...] = cost[0:halves]
        send(send_c, recv_c, first_of, 7)
        recv_c[...] = cost[halves:]

    pl.when(reduces)(reduce_part)


    def wait_plane(s):
        @pl.when(reduces)
        def _():
            wait_rows((reducers - 1) * 8, recvs.at[s])

        @pl.when(jnp.logical_not(reduces))
        def _():
            wait_rows(reducers * 8, recvs.at[s])

    lines[...] = jnp.zeros_like(lines)
    wait_plane(4)
    total = recv_h[0:8, :]
    for m in range(1, reducers):
        total = total + recv_h[m * 8 : m * 8 + 8, :]
    lined = [total] + [pltpu.roll(total, LANES - own_scans * c, 1) for c in range(1, 4)]

    def row_at(name):
        k = ROWS.index(name)
        return lined[k // 8][k % 8 : k % 8 + 1]

    for i in range(6):
        for j in range(6):
            lines[6 * i + j : 6 * i + j + 1, :] = row_at(("h", min(i, j), max(i, j)))
    hess_out[...] = lines[...].T[0:own_scans, 0:36]
    gradient = jnp.concatenate([row_at(("g", i)) for i in range(6)], axis=0)

    @pl.when(jnp.logical_not(reduces))
    def _():
        pltpu.make_async_copy(recv_c, recv_c, recvs.at[7]).wait()

    for h in range(halves):
        cost_out[:, h * LANES : (h + 1) * LANES] = recv_c[h : h + 1, :]

    wait_plane(5)
    change = recv_g[0:8, :]
    for m in range(1, reducers):
        change = change + recv_g[m * 8 : m * 8 + 8, :]
    change = pltpu.roll(change, LANES - own_scans * lax.rem(mp, in_level), 1)
    grad_out[...] = (gradient - change[0:6])[:, 0:own_scans]

    for t in range(n_tm):

        @pl.when(jnp.logical_and(reduces, tm == t))
        def _(t=t):
            rows = (reducers - 1) * (message + rest_rows) + (n_map - 1) * 16 + halves
            rows += (n_tm - 1) * (n_size + a_size + SHARE * halves) + (n_tm - 1 - t) * n_size
            wait_rows(rows, sends.at[0])

        @pl.when(jnp.logical_and(jnp.logical_not(reduces), tm == t))
        def _(t=t):
            wait_rows(reducers * (message + rest_rows) + (t + 1) * n_size, sends.at[0])


def finish(hess_in, grad_in, cost_in, hess_out, grad_out, cost_out, sems):
    copies = [
        pltpu.make_async_copy(src, dst, sems.at[i])
        for i, (src, dst) in enumerate(
            [(hess_in, hess_out), (grad_in, grad_out), (cost_in, cost_out)]
        )
    ]
    for copy in copies:
        copy.start()
    for copy in copies:
        copy.wait()


def local(points, poses, normal_angles, voxel_ids, scan_ids):
    blocks, npoints = points.shape[1:]
    n_tm, n_map = lax.axis_size("tm"), lax.axis_size("map")
    devices = n_tm * n_map
    slots = blocks // devices
    chunks = blocks // LANES
    vox_count = normal_angles.shape[1]
    own_scans = poses.shape[1]
    assert npoints == LANES and slots * 4 == LANES and own_scans * 4 == LANES
    assert n_map % LEVELS == 0 and n_map <= 4 * LEVELS and n_map % 4 == 0 and n_map % SHARE == 0 and n_tm % 4 == 0 and vox_count % LANES == 0
    scale = own_scans * devices / (blocks * devices * npoints)
    f32 = jnp.float32
    scans = own_scans * n_map
    halves = vox_count // LANES
    in_plane = n_map * n_tm // 4
    reducers = n_map // SHARE
    packed = reducers * n_tm // 4
    arrived = SHARE * n_map * n_tm // 4
    n_rows = -(-3 * halves // 8) * 8
    a_rows = SHARE * 2 * n_tm * halves
    hbm = pl.BlockSpec(memory_space=pl.ANY)
    vmem = pl.BlockSpec(memory_space=pltpu.VMEM)
    shapes = [(own_scans, 36), (6, own_scans), (1, vox_count)]
    results = pl.pallas_call(
        functools.partial(kernel, (n_tm, n_map, slots, float(npoints), scale)),
        out_shape=tuple(pltpu.VMEM(shape, f32) for shape in shapes),
        in_specs=[hbm] * 5,
        out_specs=(vmem,) * 3,
        scratch_shapes=[
            pltpu.VMEM(points.shape, f32),
            pltpu.VMEM(poses.shape, f32),
            pltpu.VMEM(normal_angles.shape, f32),
            pltpu.VMEM((chunks, LANES), jnp.int32),
            pltpu.VMEM((chunks, LANES), jnp.int32),
            pltpu.VMEM((8, LANES), f32),
            pltpu.VMEM((chunks * 16, LANES), f32),
            pltpu.VMEM((packed * 16, LANES), f32),
            pltpu.VMEM((in_plane * 16, LANES), f32),
            pltpu.VMEM((packed * 8, LANES), f32),
            pltpu.VMEM((in_plane * 8, LANES), f32),
            pltpu.VMEM((SHARE * n_rows, LANES), f32),
            pltpu.VMEM((n_tm * SHARE * n_rows, LANES), f32),
            pltpu.VMEM((arrived * 4 * n_tm, LANES), f32),
            pltpu.VMEM((a_rows, LANES), f32),
            pltpu.VMEM((n_tm * a_rows, LANES), f32),
            pltpu.VMEM((a_rows, LANES), f32),
            pltpu.VMEM((arrived * 8, LANES), f32),
            pltpu.VMEM((n_tm, SHARE * halves, LANES), f32),
            pltpu.VMEM((n_tm, SHARE * halves, LANES), f32),
            pltpu.VMEM((halves, LANES), f32),
            pltpu.VMEM((halves, LANES), f32),
            pltpu.VMEM((arrived * 32, LANES), f32),
            pltpu.VMEM((arrived * 8, LANES), f32),
            pltpu.VMEM((n_map * 8, LANES), f32),
            pltpu.VMEM((reducers * 8, LANES), f32),
            pltpu.VMEM((LEVELS * 8, LANES), f32),
            pltpu.VMEM((reducers * 8, LANES), f32),
            pltpu.VMEM((LANES, LANES), f32),
            pltpu.SemaphoreType.DMA((2,)),
            pltpu.SemaphoreType.DMA((4,)),
            pltpu.SemaphoreType.DMA((1,)),
            pltpu.SemaphoreType.DMA((9,)),
        ],
        compiler_params=pltpu.CompilerParams(collective_id=0, has_side_effects=True),
    )(
        points,
        poses,
        normal_angles,
        voxel_ids.reshape(chunks, LANES),
        scan_ids.reshape(chunks, LANES),
    )
    hess, grad, cost = pl.pallas_call(
        finish,
        out_shape=tuple(jax.ShapeDtypeStruct(shape, f32) for shape in shapes),
        in_specs=[vmem] * 3,
        out_specs=(hbm,) * 3,
        scratch_shapes=[pltpu.SemaphoreType.DMA((3,))],
    )(*[pltpu.with_memory_space_constraint(x, pltpu.VMEM) for x in results])
    return hess.T, grad, cost.reshape(vox_count)


def solution(mesh):
    return jax.shard_map(
        local,
        mesh=mesh,
        in_specs=(
            P(None, ("tm", "map"), None),
            P(None, ("tm", "map")),
            P(None, ("tm", "map")),
            P(("tm", "map")),
            P(("tm", "map")),
        ),
        out_specs=(P(None, ("tm", "map")), P(None, ("tm", "map")), P(("tm", "map"))),
        check_vma=False,
    )
```

```python
import functools

import jax
import jax.numpy as jnp
from jax import lax
from jax.experimental import pallas as pl
from jax.experimental.pallas import tpu as pltpu
from jax.sharding import PartitionSpec as P

LANES = 128
MESH = pl.DeviceIdType.MESH
PAIRS = [(0, 0), (1, 1), (2, 2), (0, 1), (0, 2), (1, 2)]
PAIR_ROW = {}
for _k, (_i, _j) in enumerate(PAIRS):
    PAIR_ROW[(_i, _j)] = _k
    PAIR_ROW[(_j, _i)] = _k

ROWS = [("h", i, j) for i in range(6) for j in range(i, 6)] + [("g", i) for i in range(6)]

MARKS, FIRSTS = 0, 8
VOX_ROW, SCAN_ROW, LAST_ROW, POSE_ROW = 0, 1, 2, 3
SHARE = 2
LEVELS = 4
CONTRACT_LAST = (((1,), (1,)), ((), ()))


def split(x):
    high = x.astype(jnp.bfloat16).astype(jnp.float32)
    rest = x - high
    mid = rest.astype(jnp.bfloat16).astype(jnp.float32)
    return jnp.concatenate([high, mid, rest - mid], axis=0).astype(jnp.bfloat16)


def joined(y):
    rows = y.shape[0] // 3
    return y[:rows] + y[rows : 2 * rows] + y[2 * rows :]


def group_turn(pieces, out_group, group, lanes_per):
    total = None
    for a, piece in enumerate(pieces):
        shift = ((a - out_group) * lanes_per) % LANES
        moved = piece if shift == 0 else pltpu.roll(piece, shift, 1)
        total = moved if total is None else jnp.where(group == a, moved, total)
    return total


def loop(count, body):
    if count <= 8:
        for i in range(count):
            body(i)
    else:
        def step(i, carry):
            body(i)
            return carry

        lax.fori_loop(0, count, step, 0)


def summed(count, body, rows, columns):
    acc = jnp.zeros((rows, columns), jnp.float32)
    if count <= 8:
        for i in range(count):
            acc = acc + body(i)
        return acc
    return lax.fori_loop(0, count, lambda i, total: total + body(i), acc)


def flipped(place, bits):
    for b in range(bits.bit_length()):
        if bits >> b & 1:
            place = place + (1 - 2 * lax.rem(place // 2**b, 2)) * 2**b
    return place


def aligned(start, size, unit=8):
    if not isinstance(start, int):
        start = pl.multiple_of(start, unit)
    return pl.ds(start, size)


def kernel(
    sizes,
    points,
    poses,
    angles,
    voxel_ids,
    scan_ids,
    hess_out,
    grad_out,
    cost_out,
    pts,
    pose_in,
    angle_in,
    vox_in,
    scan_in,
    pose_pad,
    sent,
    send1,
    recv1,
    send2,
    recv2,
    pair_n,
    recv_n,
    world,
    send_a,
    recv_a,
    total_a,
    quads,
    send_q,
    recv_q,
    send_c,
    recv_c,
    terms,
    late,
    late_high,
    late_low,
    send_h,
    recv_h,
    send_g,
    recv_g,
    lines,
    pts_sem,
    in_sem,
    sends,
    recvs,
):
    n_tm, n_map, slots, npoints, scale = sizes
    reducers = n_map // SHARE
    blocks = pts.shape[1]
    chunks = blocks // LANES
    per = LANES // slots
    own_scans = pose_in.shape[1]
    spread = LANES // own_scans
    scans = own_scans * n_map
    wide = scans // LANES
    voxels = angle_in.shape[1]
    halves = voxels // LANES
    parts = n_tm // per
    step = SHARE * parts
    arrived = n_map * step
    couples = n_map // 2 * parts
    message = parts * 16
    rest_rows = parts * 8
    in_plane = n_map * parts
    n_size = pair_n.shape[0] // SHARE
    in_level = n_map // LEVELS
    a_rows = 2 * n_tm
    a_size = SHARE * halves * a_rows
    tm = lax.axis_index("tm")
    mp = lax.axis_index("map")
    rd = mp // SHARE
    part = lax.rem(mp, SHARE)
    reduces = part == SHARE - 1
    f32, bf16 = jnp.float32, jnp.bfloat16

    small = [
        pltpu.make_async_copy(src, dst, in_sem.at[i])
        for i, (src, dst) in enumerate(
            [(poses, pose_in), (angles, angle_in), (voxel_ids, vox_in), (scan_ids, scan_in)]
        )
    ]
    loads = pts_sem.shape[0]
    span = blocks // loads

    def points_copy(r):
        rows = pl.ds(r * span, span)
        return pltpu.make_async_copy(points.at[:, rows, :], pts.at[:, rows, :], pts_sem.at[r])

    for copy in small:
        copy.start()
    loop(loads, lambda r: points_copy(r).start())
    barrier = pltpu.get_barrier_semaphore()
    near = (tm, rd * SHARE + SHARE - 1)
    first_of = (tm, rd * SHARE)
    plane = [(tm, flipped(mp, i)) for i in range(n_map - 1, 0, -1)]
    column = [(lax.rem(tm + i, n_tm), mp) for i in range(1, n_tm)]
    others = [flipped(rd, i) for i in range(reducers - 1, 0, -1)]

    def greet(peer):
        pl.semaphore_signal(barrier, inc=1, device_id=peer, device_id_type=MESH)

    @pl.when(reduces)
    def _():
        for peer in column + plane:
            greet(peer)
        for peer in column:

            @pl.when(peer[0] > tm)
            def _(peer=peer):
                greet((peer[0], rd * SHARE))

    @pl.when(jnp.logical_not(reduces))
    def _():
        for other in others:
            greet((tm, other * SHARE + SHARE - 1))
        greet(near)

    def send(source, dest, peer, s):
        pltpu.make_async_remote_copy(
            src_ref=source,
            dst_ref=dest,
            send_sem=sends.at[0],
            recv_sem=recvs.at[s],
            device_id=peer,
            device_id_type=MESH,
        ).start()

    def wait_rows(rows, sem):
        ref = pts.at[0, pl.ds(0, rows), :]
        pltpu.make_async_copy(ref, ref, sem).wait()

    def every(ref, k, stride, count=arrived):
        return ref[pl.ds(k, count, stride=stride), :]

    lane = lax.broadcasted_iota(jnp.int32, (8, LANES), 1)
    group = lane // slots
    chunk_of = lax.broadcasted_iota(jnp.int32, (arrived, LANES), 0)
    turn_of = (
        lax.broadcasted_iota(jnp.int32, (arrived, LANES), 1) // slots + per * lax.rem(chunk_of, parts)
    )
    top = lax.broadcasted_iota(jnp.int32, (8, LANES), 0) < 4
    own_turn = [turn_of == t for t in range(n_tm)]
    sent[...] = jnp.zeros_like(sent)

    for copy in small:
        copy.wait()
    pose_pad[...] = jnp.zeros_like(pose_pad)
    for g in range(spread):
        pose_pad[0:6, g * own_scans : (g + 1) * own_scans] = pose_in[...]
    pose = pose_pad[...]
    cos, sin = jnp.cos(0.5 * pose), jnp.sin(0.5 * pose)
    cx, cy, cz = cos[0:1], cos[1:2], cos[2:3]
    sx, sy, sz = sin[0:1], sin[1:2], sin[2:3]
    pose_rows = [
        [
            cx * cy * cz + sx * sy * sz,
            sx * cy * cz - cx * sy * sz,
            cx * sy * cz + sx * cy * sz,
            cx * cy * sz - sx * sy * cz,
        ],
        [pose[3:4], pose[4:5], pose[5:6], pose[6:7]],
    ]
    scan_group = lane[0:1] // own_scans
    pose_lines = []
    for line, *others_of in pose_rows:
        for g, row in enumerate(others_of):
            line = jnp.where(scan_group == g + 1, row, line)
        pose_lines.append(line)

    ids = vox_in[...]
    row_of = lax.broadcasted_iota(jnp.int32, ids.shape, 0)
    lane_of = lax.broadcasted_iota(jnp.int32, ids.shape, 1)
    owner_of = row_of * per + lane_of // slots
    local_ids = jnp.where(ids >= 0, ids - owner_of * voxels, -1).astype(f32)
    sent[pl.ds(8 + VOX_ROW, chunks, stride=16), :] = local_ids
    sent[pl.ds(8 + SCAN_ROW, chunks, stride=16), :] = scan_in[...].astype(f32)

    theta, phi = angle_in[0:1, :], angle_in[1:2, :]
    sin_theta = jnp.sin(theta)
    own_normal = [sin_theta * jnp.cos(phi), sin_theta * jnp.sin(phi), jnp.cos(theta)]
    n_mine = aligned(part * n_size, n_size)
    for c in range(3):
        for h in range(halves):
            k = part * n_size + c * halves + h
            pair_n[pl.ds(k, 1), :] = own_normal[c][:, h * LANES : (h + 1) * LANES]

    def raw_moments(r):
        at = aligned(r * LANES, LANES, LANES)
        xyz = [pts[i, at, :].T for i in range(3)]
        sums = [jnp.sum(x, axis=0, keepdims=True) for x in xyz]
        sums += [jnp.sum(xyz[i] * xyz[j], axis=0, keepdims=True) for i, j in PAIRS]
        for k, row in enumerate(sums):
            sent[pl.ds(r * 16 + (k if k < 8 else 8 + LAST_ROW), 1), :] = row

    def load_step(r):
        points_copy(r).wait()
        for i in range(span // LANES):
            raw_moments(r * (span // LANES) + i)

    loop(loads, load_step)
    row_chunks = n_map // per

    def pack(peer_row):
        for u in range(parts):
            turned = []
            for g in range(per):
                for half in range(2):
                    at = [((u * per + a) * row_chunks + peer_row) * 16 + 8 * half for a in range(per)]
                    pieces = [sent[aligned(row, 8), :] for row in at]
                    turned.append(group_turn(pieces, g, group, slots))
            for i in range(per // SHARE):
                moments, marks, moments_b, marks_b = turned[4 * i : 4 * i + 4]
                base = (peer_row * (per // SHARE) + i) * parts + u
                send1[aligned(base * 16 + MARKS, 8), :] = jnp.where(
                    top, marks, pltpu.roll(marks_b, 4, 0)
                )
                send1[aligned(base * 16 + FIRSTS, 8), :] = jnp.where(
                    top, moments, pltpu.roll(moments_b, 4, 0)
                )
                send2[aligned(base * 8, 8), :] = jnp.where(
                    top, pltpu.roll(moments, 4, 0), moments_b
                )
                for k in range(SHARE):
                    send1[pl.ds(base * 16 + MARKS + 4 * k + POSE_ROW, 1), :] = pose_lines[k]

    loop(row_chunks, pack)

    from_plane = n_map - 1 + n_tm - 1
    pl.semaphore_wait(barrier, jnp.where(reduces, from_plane, reducers + tm))
    mine = aligned(mp * message, message)

    rest_mine = aligned(mp * rest_rows, rest_rows)

    def send_moments(other, peer):
        send(send1.at[aligned(other * message, message), :], recv1.at[mine, :], peer, 0)

    def send_rest(other, peer):
        send(send2.at[aligned(other * rest_rows, rest_rows), :], recv2.at[rest_mine, :], peer, 7)

    def normals_to(t, k):
        return recv_n.at[aligned((t * SHARE + k) * n_size, n_size), :]

    @pl.when(jnp.logical_not(reduces))
    def _():
        for peer in column:

            @pl.when(peer[0] < tm)
            def _(peer=peer):
                send(pair_n.at[n_mine, :], normals_to(tm, 0), (peer[0], near[1]), 1)

        send(pair_n.at[n_mine, :], pair_n.at[n_mine, :], near, 6)

    for send_part in (send_moments, send_rest):
        for other in others:
            send_part(other, (tm, other * SHARE + SHARE - 1))

        @pl.when(jnp.logical_not(reduces))
        def _(send_part=send_part):
            send_part(rd, near)

    eight = aligned(rd * 8, 8)

    def reduce_part():
        for peer in column:
            send(pair_n.at[pl.ds(n_size, n_size), :], normals_to(tm, 1), peer, 1)
        wait_rows(n_size, recvs.at[6])
        for peer in column:

            @pl.when(peer[0] > tm)
            def _(peer=peer):
                send(pair_n.at[pl.ds(0, n_size), :], normals_to(tm, 0), peer, 1)

        n_column = aligned(tm * SHARE * n_size, SHARE * n_size)
        recv1[mine, :] = send1[aligned(rd * message, message), :]
        recv2[rest_mine, :] = send2[aligned(rd * rest_rows, rest_rows), :]
        recv_n[n_column, :] = pair_n[...]
        for t in range(n_tm):
            world[pl.ds(3 * n_tm + t, arrived, stride=4 * n_tm), :] = jnp.where(
                own_turn[t], 1.0, 0.0
            )
        quads[...] = jnp.zeros_like(quads)
        send_g[...] = jnp.zeros_like(send_g)
        late[...] = jnp.zeros_like(late)
        wait_rows((n_map - 1) * message, recvs.at[0])

        def place(q, side):
            i, u = (q // parts, q % parts) if isinstance(q, int) else (q // parts, lax.rem(q, parts))
            return (2 * i + side) * parts + u

        def couple_row(k, q, row, turn):
            return jnp.concatenate(
                [
                    recv1[pl.ds(place(q, side) * 16 + 4 * k + row + turn, 1), :]
                    for side in range(2)
                ],
                axis=1,
            )

        def couple_tile(ref, k, q, rows):
            return jnp.concatenate(
                [ref[aligned((k * in_plane + place(q, side)) * rows, rows), :] for side in range(2)],
                axis=1,
            )

        def marked(row, count):
            kind = bf16 if count <= 256 else f32
            line = jnp.broadcast_to(row, (16, 2 * LANES)).astype(kind)
            number = lax.broadcasted_iota(jnp.int32, (count, 2 * LANES), 0).astype(f32).astype(kind)
            found = jnp.concatenate([line] * (count // 16), axis=0) == number
            return jnp.where(found, jnp.ones((), kind), jnp.zeros((), kind)).astype(bf16)

        def two_levels_of(row, levels, count):
            low = count // levels
            number = row.astype(jnp.int32)
            high = jnp.broadcast_to(number // low, (16, 2 * LANES)).astype(f32).astype(bf16)
            return high, marked(jnp.bitwise_and(number, low - 1).astype(f32), low)

        def picked(values, high_line, levels):
            three = split(values)
            rows = three.shape[0]
            high = jnp.concatenate([high_line] * (-(-rows // 16)), axis=0)[:rows]
            return jnp.concatenate(
                [
                    jnp.where(high == jnp.full((), h, bf16), three, jnp.zeros((), bf16))
                    for h in range(levels)
                ],
                axis=0,
            )

        def two_level(values, row, levels, count):
            high, low_marks = two_levels_of(row, levels, count)
            return picked(values, high, levels), low_marks

        def product(left, right):
            return lax.dot_general(left, right, CONTRACT_LAST, preferred_element_type=f32)

        def products(each_side, kinds, rows, columns):
            if couples > 8:
                return sum(
                    summed(couples, lambda q, k=k: product(*each_side(k, q)), rows, columns)
                    for k in kinds
                )
            sides = [each_side(k, q) for k in kinds for q in range(couples)]
            return product(*[jnp.concatenate(side, axis=1) for side in zip(*sides)])

        again = jnp.minimum(tm, 0)

        def scan_hot(k, q, turn):
            return marked(couple_row(k, q, SCAN_ROW, turn), scans)

        def vox_hot(k, q, turn):
            return marked(couple_row(k, q, VOX_ROW, turn), voxels)

        own_group = lane // own_scans
        def each_part(ref, row, stride):
            return jnp.concatenate(
                [every(ref, row + 4 * k, stride, in_plane) for k in range(SHARE)], axis=0
            )

        def gather(tables, high, low):
            value = jnp.take_along_axis(tables[0], low, axis=1, mode="promise_in_bounds")
            for h in range(1, len(tables)):
                other = jnp.take_along_axis(tables[h], low, axis=1, mode="promise_in_bounds")
                value = jnp.where(high == h, other, value)
            return value

        columns = []
        for h in range(wide):
            at = [(h * spread + a) * message + MARKS for a in range(spread)]
            tiles = [recv1[row : row + 8, :] for row in at]
            columns.append([group_turn(tiles, g, own_group, own_scans) for g in range(4)])
        scan_of = each_part(recv1, MARKS + SCAN_ROW, 16).astype(jnp.int32)
        scan_low, scan_high = jnp.bitwise_and(scan_of, LANES - 1), scan_of // LANES

        def pose_of(k, g):
            row = 4 * k + POSE_ROW
            rows = [
                jnp.broadcast_to(turned[g][row : row + 1], (arrived, LANES)) for turned in columns
            ]
            return gather(rows, scan_high, scan_low)

        qw, qx, qy, qz = [pose_of(0, g) for g in range(4)]
        shift = [pose_of(1, g) for g in range(3)]
        rot = [
            [1 - 2 * (qy * qy + qz * qz), 2 * (qx * qy - qw * qz), 2 * (qx * qz + qw * qy)],
            [2 * (qx * qy + qw * qz), 1 - 2 * (qx * qx + qz * qz), 2 * (qy * qz - qw * qx)],
            [2 * (qx * qz - qw * qy), 2 * (qy * qz + qw * qx), 1 - 2 * (qx * qx + qy * qy)],
        ]
        first = [each_part(recv1, FIRSTS + k, 16) for k in range(3)]
        turned_first = [sum(rot[i][j] * first[j] for j in range(3)) for i in range(3)]
        m1 = [turned_first[i] + npoints * shift[i] for i in range(3)]
        for c in range(3):
            for t in range(n_tm):
                world[pl.ds(c * n_tm + t, arrived, stride=4 * n_tm), :] = jnp.where(
                    own_turn[t], m1[c], 0.0
                )

        def voxel_sums(ref, rows, k, turn):
            def add(q):
                return lax.dot_general(
                    split(couple_tile(ref, k, q, rows)),
                    vox_hot(k, q, turn),
                    CONTRACT_LAST,
                    preferred_element_type=f32,
                )

            return joined(summed(couples, add, 3 * rows, voxels))

        def first_sums(k):
            rows = 12 * n_tm

            def sides(k, q):
                values = couple_tile(world, k, q, 4 * n_tm)
                return two_level(values, couple_row(k, q, VOX_ROW, 0), halves, voxels)

            found = products(sides, [k], halves * rows, LANES)
            return jnp.concatenate(
                [joined(found[h * rows : (h + 1) * rows]) for h in range(halves)], axis=1
            )

        sums = [first_sums(k) for k in range(SHARE)]
        wait_rows((n_tm - 1) * SHARE * n_size, recvs.at[1])
        normal = [
            [
                jnp.concatenate(
                    [
                        every(recv_n, k * n_size + c * halves + h, SHARE * n_size, n_tm)
                        for h in range(halves)
                    ],
                    axis=1,
                )
                for c in range(3)
            ]
            for k in range(SHARE)
        ]
        for k in range(SHARE):
            along = sum(normal[k][c] * sums[k][c * n_tm : (c + 1) * n_tm] for c in range(3))
            count = sums[k][3 * n_tm : 4 * n_tm]
            for h in range(halves):
                at = slice(h * LANES, (h + 1) * LANES)
                base = (k * halves + h) * a_rows
                send_a[base : base + n_tm, :] = along[:, at]
                send_a[base + n_tm : base + a_rows, :] = count[:, at]

        a_mine = aligned(tm * a_size, a_size)
        for peer in column:
            send(send_a, recv_a.at[a_mine, :], peer, 2)
        recv_a[a_mine, :] = send_a[...]

        vox_of = each_part(recv1, MARKS + VOX_ROW, 16).astype(jnp.int32)
        live = vox_of >= 0
        vox_low = jnp.bitwise_and(vox_of, LANES - 1)
        vox_high = jnp.where(live, vox_of, 0) // LANES

        def by_voxel(rows):
            value = None
            for t in range(n_tm):
                tables = []
                for h in range(halves):
                    each = [jnp.broadcast_to(rows(k, t, h), (in_plane, LANES)) for k in range(SHARE)]
                    tables.append(jnp.concatenate(each, axis=0))
                found = gather(tables, vox_high, vox_low)
                value = found if t == 0 else jnp.where(own_turn[t], found, value)
            return value

        n = []
        for c in range(3):
            value = by_voxel(
                lambda k, t, h: normal[k][c][t : t + 1, h * LANES : (h + 1) * LANES]
            )
            n.append(jnp.where(live, value, 0.0))
        wait_rows((n_map - 1) * rest_rows, recvs.at[7])
        second = [each_part(recv1, FIRSTS + 3, 16)]
        second += [each_part(recv2, k, 8) for k in range(4)]
        second += [each_part(recv1, MARKS + LAST_ROW, 16)]
        half_turned = [
            [sum(rot[i][k] * second[PAIR_ROW[(k, j)]] for k in range(3)) for j in range(3)]
            for i in range(3)
        ]
        m2 = [
            sum(half_turned[i][k] * rot[j][k] for k in range(3))
            + turned_first[i] * shift[j]
            + shift[i] * m1[j]
            for i, j in PAIRS
        ]
        quad = sum(n[i] ** 2 * m2[i] for i in range(3)) + 2.0 * sum(
            n[PAIRS[k][0]] * n[PAIRS[k][1]] * m2[k] for k in range(3, 6)
        )
        for t in range(n_tm):
            quads[pl.ds(t, arrived, stride=8), :] = jnp.where(own_turn[t], quad, 0.0)
        for k in range(SHARE):
            quad_sums = voxel_sums(quads, 8, k, again)
            for t in range(n_tm):
                for h in range(halves):
                    send_q[t, k * halves + h : k * halves + h + 1, :] = quad_sums[
                        t : t + 1, h * LANES : (h + 1) * LANES
                    ]
        for peer in column:
            send(send_q.at[peer[0]], recv_q.at[tm], peer, 3)
        recv_q[tm] = send_q[tm]

        def skew(v):
            return [
                n[2] * v[1] - n[1] * v[2],
                n[0] * v[2] - n[2] * v[0],
                n[1] * v[0] - n[0] * v[1],
            ]

        full = [[m2[PAIR_ROW[(i, j)]] for j in range(3)] for i in range(3)]
        skewed = [skew([full[k][j] for k in range(3)]) for j in range(3)]
        left = [[skewed[j][i] for j in range(3)] for i in range(3)]
        corner_block = [skew(left[i]) for i in range(3)]
        skew_first = skew(m1)
        found = {}
        for i in range(3):
            for j in range(3):
                if j >= i:
                    found[("h", i, j)] = corner_block[i][j]
                    found[("h", 3 + i, 3 + j)] = npoints * n[i] * n[j]
                found[("h", i, 3 + j)] = skew_first[i] * n[j]
        rest = n[0] * m1[0] + n[1] * m1[1] + n[2] * m1[2]
        for i in range(3):
            found[("g", i)] = sum(left[i][j] * n[j] for j in range(3))
            found[("g", 3 + i)] = n[i] * rest
        shares = skew_first + [npoints * n[i] for i in range(3)]
        for name, value in found.items():
            terms[pl.ds(ROWS.index(name), arrived, stride=32), :] = value
        for k in range(len(found), 32):
            terms[pl.ds(k, arrived, stride=32), :] = jnp.zeros_like(rest)

        def scan_sums(k, tile, rows, turn):
            def add(q):
                return lax.dot_general(
                    split(tile(k, q)),
                    scan_hot(k, q, turn),
                    CONTRACT_LAST,
                    preferred_element_type=f32,
                )

            return summed(couples, add, 3 * rows, scans)

        per_scan = scale * joined(
            sum(
                scan_sums(k, lambda k, q: couple_tile(terms, k, q, 32), 32, 0) for k in range(SHARE)
            )
        )
        for h in range(wide):
            pieces = [per_scan[8 * c : 8 * c + 8, h * LANES : (h + 1) * LANES] for c in range(4)]
            for b in range(spread):
                at = (h * spread + b) * 8
                send_h[at : at + 8, :] = group_turn(pieces, b, own_group, own_scans)
        for peer in plane:
            send(send_h.at[aligned(peer[1] * 8, 8), :], recv_h.at[eight, :], peer, 4)
        recv_h[eight, :] = send_h[aligned(mp * 8, 8), :]

        for k in range(SHARE):

            def keep_marks(q, k=k):
                at = k * couples + q
                late_high[at], late_low[at] = two_levels_of(
                    couple_row(k, q, SCAN_ROW, again), LEVELS, scans
                )

            loop(couples, keep_marks)

        wait_rows((n_tm - 1) * a_size, recvs.at[2])
        offset_rows = []
        for k in range(SHARE):
            offsets = []
            for h in range(halves):
                base = (k * halves + h) * a_rows
                total = recv_a[base : base + a_rows, :]
                for t in range(1, n_tm):
                    total = total + recv_a[t * a_size + base : t * a_size + base + a_rows, :]
                floor = jnp.maximum(total[n_tm:] * npoints, 1.0)
                offset = total[:n_tm] / floor
                total_a[base : base + n_tm, :] = offset
                total_a[base + n_tm : base + a_rows, :] = floor
                offsets.append(offset)
            offset_rows.append(offsets)
        offset_of = by_voxel(lambda k, t, h: offset_rows[k][h][t : t + 1])
        for i in range(6):
            late[pl.ds(i, arrived, stride=8), :] = shares[i] * offset_of

        def late_sides(k, q):
            at = k * couples + q + again
            return picked(couple_tile(late, k, q, 8), late_high[at], LEVELS), late_low[at]

        moved = products(late_sides, range(SHARE), LEVELS * 24, scans // LEVELS)
        for h in range(LEVELS):
            send_g[h * 8 : h * 8 + 8, 0 : scans // LEVELS] = scale * joined(
                moved[h * 24 : h * 24 + 24]
            )
        for peer in plane:
            source = send_g.at[aligned(peer[1] // in_level * 8, 8), :]
            send(source, recv_g.at[eight, :], peer, 5)
        recv_g[eight, :] = send_g[aligned(mp // in_level * 8, 8), :]

        pltpu.make_async_copy(
            recv_q.at[pl.ds(0, n_tm - 1)], recv_q.at[pl.ds(0, n_tm - 1)], recvs.at[3]
        ).wait()
        quad_total = recv_q[0]
        for t in range(1, n_tm):
            quad_total = quad_total + recv_q[t]
        own_offset = total_a[pl.ds(tm, SHARE * halves, stride=a_rows), :]
        own_floor = total_a[pl.ds(n_tm + tm, SHARE * halves, stride=a_rows), :]
        cost = quad_total / own_floor - own_offset**2
        send_c[...] = cost[0:halves]
        send(send_c, recv_c, first_of, 6)
        recv_c[...] = cost[halves:]

    pl.when(reduces)(reduce_part)


    def wait_plane(s):
        @pl.when(reduces)
        def _():
            wait_rows((reducers - 1) * 8, recvs.at[s])

        @pl.when(jnp.logical_not(reduces))
        def _():
            wait_rows(reducers * 8, recvs.at[s])

    lines[...] = jnp.zeros_like(lines)
    wait_plane(4)
    total = recv_h[0:8, :]
    for m in range(1, reducers):
        total = total + recv_h[m * 8 : m * 8 + 8, :]
    lined = [total] + [pltpu.roll(total, LANES - own_scans * c, 1) for c in range(1, 4)]

    def row_at(name):
        k = ROWS.index(name)
        return lined[k // 8][k % 8 : k % 8 + 1]

    for i in range(6):
        for j in range(6):
            lines[6 * i + j : 6 * i + j + 1, :] = row_at(("h", min(i, j), max(i, j)))
    hess_out[...] = lines[...].T[0:own_scans, 0:36]
    gradient = jnp.concatenate([row_at(("g", i)) for i in range(6)], axis=0)

    @pl.when(jnp.logical_not(reduces))
    def _():
        pltpu.make_async_copy(recv_c, recv_c, recvs.at[6]).wait()

    for h in range(halves):
        cost_out[:, h * LANES : (h + 1) * LANES] = recv_c[h : h + 1, :]

    wait_plane(5)
    change = recv_g[0:8, :]
    for m in range(1, reducers):
        change = change + recv_g[m * 8 : m * 8 + 8, :]
    change = pltpu.roll(change, LANES - own_scans * lax.rem(mp, in_level), 1)
    grad_out[...] = (gradient - change[0:6])[:, 0:own_scans]

    for t in range(n_tm):

        @pl.when(jnp.logical_and(reduces, tm == t))
        def _(t=t):
            rows = (reducers - 1) * (message + rest_rows) + (n_map - 1) * 16 + halves
            rows += (n_tm - 1) * (n_size + a_size + SHARE * halves) + (n_tm - 1 - t) * n_size
            wait_rows(rows, sends.at[0])

        @pl.when(jnp.logical_and(jnp.logical_not(reduces), tm == t))
        def _(t=t):
            wait_rows(reducers * (message + rest_rows) + (t + 1) * n_size, sends.at[0])


def finish(hess_in, grad_in, cost_in, hess_out, grad_out, cost_out, sems):
    copies = [
        pltpu.make_async_copy(src, dst, sems.at[i])
        for i, (src, dst) in enumerate(
            [(hess_in, hess_out), (grad_in, grad_out), (cost_in, cost_out)]
        )
    ]
    for copy in copies:
        copy.start()
    for copy in copies:
        copy.wait()


def local(points, poses, normal_angles, voxel_ids, scan_ids):
    blocks, npoints = points.shape[1:]
    n_tm, n_map = lax.axis_size("tm"), lax.axis_size("map")
    devices = n_tm * n_map
    slots = blocks // devices
    chunks = blocks // LANES
    vox_count = normal_angles.shape[1]
    own_scans = poses.shape[1]
    assert npoints == LANES and slots * 4 == LANES and own_scans * 4 == LANES
    assert n_map & (n_map - 1) == 0 and n_map % LEVELS == 0 and n_map <= 4 * LEVELS and n_map % 4 == 0 and n_map % SHARE == 0 and n_tm % 4 == 0 and vox_count % LANES == 0
    scale = own_scans * devices / (blocks * devices * npoints)
    f32, bf16 = jnp.float32, jnp.bfloat16
    scans = own_scans * n_map
    halves = vox_count // LANES
    in_plane = n_map * n_tm // 4
    reducers = n_map // SHARE
    packed = reducers * n_tm // 4
    arrived = SHARE * n_map * n_tm // 4
    n_rows = -(-3 * halves // 8) * 8
    a_rows = SHARE * 2 * n_tm * halves
    hbm = pl.BlockSpec(memory_space=pl.ANY)
    vmem = pl.BlockSpec(memory_space=pltpu.VMEM)
    shapes = [(own_scans, 36), (6, own_scans), (1, vox_count)]
    results = pl.pallas_call(
        functools.partial(kernel, (n_tm, n_map, slots, float(npoints), scale)),
        out_shape=tuple(pltpu.VMEM(shape, f32) for shape in shapes),
        in_specs=[hbm] * 5,
        out_specs=(vmem,) * 3,
        scratch_shapes=[
            pltpu.VMEM(points.shape, f32),
            pltpu.VMEM(poses.shape, f32),
            pltpu.VMEM(normal_angles.shape, f32),
            pltpu.VMEM((chunks, LANES), jnp.int32),
            pltpu.VMEM((chunks, LANES), jnp.int32),
            pltpu.VMEM((8, LANES), f32),
            pltpu.VMEM((chunks * 16, LANES), f32),
            pltpu.VMEM((packed * 16, LANES), f32),
            pltpu.VMEM((in_plane * 16, LANES), f32),
            pltpu.VMEM((packed * 8, LANES), f32),
            pltpu.VMEM((in_plane * 8, LANES), f32),
            pltpu.VMEM((SHARE * n_rows, LANES), f32),
            pltpu.VMEM((n_tm * SHARE * n_rows, LANES), f32),
            pltpu.VMEM((arrived * 4 * n_tm, LANES), f32),
            pltpu.VMEM((a_rows, LANES), f32),
            pltpu.VMEM((n_tm * a_rows, LANES), f32),
            pltpu.VMEM((a_rows, LANES), f32),
            pltpu.VMEM((arrived * 8, LANES), f32),
            pltpu.VMEM((n_tm, SHARE * halves, LANES), f32),
            pltpu.VMEM((n_tm, SHARE * halves, LANES), f32),
            pltpu.VMEM((halves, LANES), f32),
            pltpu.VMEM((halves, LANES), f32),
            pltpu.VMEM((arrived * 32, LANES), f32),
            pltpu.VMEM((arrived * 8, LANES), f32),
            pltpu.VMEM((arrived // 2, 16, 2 * LANES), bf16),
            pltpu.VMEM((arrived // 2, scans // LEVELS, 2 * LANES), bf16),
            pltpu.VMEM((n_map * 8, LANES), f32),
            pltpu.VMEM((reducers * 8, LANES), f32),
            pltpu.VMEM((LEVELS * 8, LANES), f32),
            pltpu.VMEM((reducers * 8, LANES), f32),
            pltpu.VMEM((LANES, LANES), f32),
            pltpu.SemaphoreType.DMA((2,)),
            pltpu.SemaphoreType.DMA((4,)),
            pltpu.SemaphoreType.DMA((1,)),
            pltpu.SemaphoreType.DMA((8,)),
        ],
        compiler_params=pltpu.CompilerParams(collective_id=0, has_side_effects=True),
    )(
        points,
        poses,
        normal_angles,
        voxel_ids.reshape(chunks, LANES),
        scan_ids.reshape(chunks, LANES),
    )
    hess, grad, cost = pl.pallas_call(
        finish,
        out_shape=tuple(jax.ShapeDtypeStruct(shape, f32) for shape in shapes),
        in_specs=[vmem] * 3,
        out_specs=(hbm,) * 3,
        scratch_shapes=[pltpu.SemaphoreType.DMA((3,))],
    )(*[pltpu.with_memory_space_constraint(x, pltpu.VMEM) for x in results])
    return hess.T, grad, cost.reshape(vox_count)


def solution(mesh):
    return jax.shard_map(
        local,
        mesh=mesh,
        in_specs=(
            P(None, ("tm", "map"), None),
            P(None, ("tm", "map")),
            P(None, ("tm", "map")),
            P(("tm", "map")),
            P(("tm", "map")),
        ),
        out_specs=(P(None, ("tm", "map")), P(None, ("tm", "map")), P(("tm", "map"))),
        check_vma=False,
    )
```

```python
import functools

import jax
import jax.numpy as jnp
from jax import lax
from jax.experimental import pallas as pl
from jax.experimental.pallas import tpu as pltpu
from jax.sharding import PartitionSpec as P

LANES = 128
MESH = pl.DeviceIdType.MESH
PAIRS = [(0, 0), (1, 1), (2, 2), (0, 1), (0, 2), (1, 2)]
PAIR_ROW = {}
for _k, (_i, _j) in enumerate(PAIRS):
    PAIR_ROW[(_i, _j)] = _k
    PAIR_ROW[(_j, _i)] = _k

ROWS = [("h", i, j) for i in range(6) for j in range(i, 6)] + [("g", i) for i in range(6)]

MARKS, FIRSTS = 0, 8
VOX_ROW, SCAN_ROW, POSE_ROW = 0, 1, 3
SHARE = 2
LEVELS = 4
CONTRACT_LAST = (((1,), (1,)), ((), ()))


def split(x):
    high = x.astype(jnp.bfloat16).astype(jnp.float32)
    rest = x - high
    mid = rest.astype(jnp.bfloat16).astype(jnp.float32)
    return jnp.concatenate([high, mid, rest - mid], axis=0).astype(jnp.bfloat16)


def joined(y):
    rows = y.shape[0] // 3
    return y[:rows] + y[rows : 2 * rows] + y[2 * rows :]


def group_turn(pieces, out_group, group, lanes_per):
    total = None
    for a, piece in enumerate(pieces):
        shift = ((a - out_group) * lanes_per) % LANES
        moved = piece if shift == 0 else pltpu.roll(piece, shift, 1)
        total = moved if total is None else jnp.where(group == a, moved, total)
    return total


def loop(count, body):
    if count <= 8:
        for i in range(count):
            body(i)
    else:
        def step(i, carry):
            body(i)
            return carry

        lax.fori_loop(0, count, step, 0)


def summed(count, body, rows, columns):
    acc = jnp.zeros((rows, columns), jnp.float32)
    if count <= 8:
        for i in range(count):
            acc = acc + body(i)
        return acc
    return lax.fori_loop(0, count, lambda i, total: total + body(i), acc)


def flipped(place, bits):
    for b in range(bits.bit_length()):
        if bits >> b & 1:
            place = place + (1 - 2 * lax.rem(place // 2**b, 2)) * 2**b
    return place


def aligned(start, size, unit=8):
    if not isinstance(start, int):
        start = pl.multiple_of(start, unit)
    return pl.ds(start, size)


def kernel(
    sizes,
    points,
    poses,
    angles,
    voxel_ids,
    scan_ids,
    hess_out,
    grad_out,
    cost_out,
    pts,
    pose_in,
    angle_in,
    vox_in,
    scan_in,
    pose_pad,
    sent,
    sent2,
    send1,
    recv1,
    send2,
    recv2,
    pair_n,
    recv_n,
    world,
    send_a,
    recv_a,
    total_a,
    quads,
    send_q,
    recv_q,
    send_c,
    recv_c,
    terms,
    late,
    late_high,
    late_low,
    send_h,
    recv_h,
    send_g,
    recv_g,
    lines,
    pts_sem,
    in_sem,
    sends,
    recvs,
):
    n_tm, n_map, slots, npoints, scale = sizes
    reducers = n_map // SHARE
    blocks = pts.shape[1]
    chunks = blocks // LANES
    per = LANES // slots
    own_scans = pose_in.shape[1]
    spread = LANES // own_scans
    scans = own_scans * n_map
    wide = scans // LANES
    voxels = angle_in.shape[1]
    halves = voxels // LANES
    parts = n_tm // per
    step = SHARE * parts
    arrived = n_map * step
    couples = n_map // 2 * parts
    message = parts * 16
    rest_rows = step * 8
    in_plane = n_map * parts
    n_size = pair_n.shape[0] // SHARE
    in_level = n_map // LEVELS
    a_rows = 2 * n_tm
    a_size = SHARE * halves * a_rows
    tm = lax.axis_index("tm")
    mp = lax.axis_index("map")
    rd = mp // SHARE
    part = lax.rem(mp, SHARE)
    reduces = part == SHARE - 1
    f32, bf16 = jnp.float32, jnp.bfloat16

    small = [
        pltpu.make_async_copy(src, dst, in_sem.at[i])
        for i, (src, dst) in enumerate(
            [(poses, pose_in), (angles, angle_in), (voxel_ids, vox_in), (scan_ids, scan_in)]
        )
    ]
    loads = pts_sem.shape[0]
    span = blocks // loads

    def points_copy(r):
        rows = pl.ds(r * span, span)
        return pltpu.make_async_copy(points.at[:, rows, :], pts.at[:, rows, :], pts_sem.at[r])

    for copy in small:
        copy.start()
    loop(loads, lambda r: points_copy(r).start())
    barrier = pltpu.get_barrier_semaphore()
    near = (tm, rd * SHARE + SHARE - 1)
    first_of = (tm, rd * SHARE)
    plane = [(tm, flipped(mp, i)) for i in range(n_map - 1, 0, -1)]
    column = [(lax.rem(tm + i, n_tm), mp) for i in range(1, n_tm)]
    others = [flipped(rd, i) for i in range(reducers - 1, 0, -1)]

    def greet(peer):
        pl.semaphore_signal(barrier, inc=1, device_id=peer, device_id_type=MESH)

    @pl.when(reduces)
    def _():
        for peer in column + plane:
            greet(peer)
        for peer in column:

            @pl.when(peer[0] > tm)
            def _(peer=peer):
                greet((peer[0], rd * SHARE))

    @pl.when(jnp.logical_not(reduces))
    def _():
        for other in others:
            greet((tm, other * SHARE + SHARE - 1))
        greet(near)

    def send(source, dest, peer, s):
        pltpu.make_async_remote_copy(
            src_ref=source,
            dst_ref=dest,
            send_sem=sends.at[0],
            recv_sem=recvs.at[s],
            device_id=peer,
            device_id_type=MESH,
        ).start()

    def wait_rows(rows, sem):
        ref = pts.at[0, pl.ds(0, rows), :]
        pltpu.make_async_copy(ref, ref, sem).wait()

    def every(ref, k, stride, count=arrived):
        return ref[pl.ds(k, count, stride=stride), :]

    lane = lax.broadcasted_iota(jnp.int32, (8, LANES), 1)
    group = lane // slots
    chunk_of = lax.broadcasted_iota(jnp.int32, (arrived, LANES), 0)
    turn_of = (
        lax.broadcasted_iota(jnp.int32, (arrived, LANES), 1) // slots + per * lax.rem(chunk_of, parts)
    )
    top = lax.broadcasted_iota(jnp.int32, (8, LANES), 0) < 4
    own_turn = [turn_of == t for t in range(n_tm)]
    sent[...] = jnp.zeros_like(sent)
    sent2[...] = jnp.zeros_like(sent2)

    for copy in small:
        copy.wait()
    pose_pad[...] = jnp.zeros_like(pose_pad)
    for g in range(spread):
        pose_pad[0:6, g * own_scans : (g + 1) * own_scans] = pose_in[...]
    pose = pose_pad[...]
    cos, sin = jnp.cos(0.5 * pose), jnp.sin(0.5 * pose)
    cx, cy, cz = cos[0:1], cos[1:2], cos[2:3]
    sx, sy, sz = sin[0:1], sin[1:2], sin[2:3]
    pose_rows = [
        [
            cx * cy * cz + sx * sy * sz,
            sx * cy * cz - cx * sy * sz,
            cx * sy * cz + sx * cy * sz,
            cx * cy * sz - sx * sy * cz,
        ],
        [pose[3:4], pose[4:5], pose[5:6], pose[6:7]],
    ]
    scan_group = lane[0:1] // own_scans
    pose_lines = []
    for line, *others_of in pose_rows:
        for g, row in enumerate(others_of):
            line = jnp.where(scan_group == g + 1, row, line)
        pose_lines.append(line)

    ids = vox_in[...]
    row_of = lax.broadcasted_iota(jnp.int32, ids.shape, 0)
    lane_of = lax.broadcasted_iota(jnp.int32, ids.shape, 1)
    owner_of = row_of * per + lane_of // slots
    local_ids = jnp.where(ids >= 0, ids - owner_of * voxels, -1).astype(f32)
    sent[pl.ds(4 + VOX_ROW, chunks, stride=8), :] = local_ids
    sent[pl.ds(4 + SCAN_ROW, chunks, stride=8), :] = scan_in[...].astype(f32)

    theta, phi = angle_in[0:1, :], angle_in[1:2, :]
    sin_theta = jnp.sin(theta)
    own_normal = [sin_theta * jnp.cos(phi), sin_theta * jnp.sin(phi), jnp.cos(theta)]
    n_mine = aligned(part * n_size, n_size)
    for c in range(3):
        for h in range(halves):
            k = part * n_size + c * halves + h
            pair_n[pl.ds(k, 1), :] = own_normal[c][:, h * LANES : (h + 1) * LANES]

    def first_moments(r):
        at = aligned(r * LANES, LANES, LANES)
        for i in range(3):
            turned = pts[i, at, :].T
            pts[i, at, :] = turned
            sent[pl.ds(r * 8 + i, 1), :] = jnp.sum(turned, axis=0, keepdims=True)

    def second_moments(r):
        at = aligned(r * LANES, LANES, LANES)
        xyz = [pts[i, at, :] for i in range(3)]
        for k, (i, j) in enumerate(PAIRS):
            sent2[pl.ds(r * 8 + k, 1), :] = jnp.sum(xyz[i] * xyz[j], axis=0, keepdims=True)

    def load_step(r):
        points_copy(r).wait()
        for i in range(span // LANES):
            first_moments(r * (span // LANES) + i)

    loop(loads, load_step)
    row_chunks = n_map // per

    def turned_tiles(ref, peer_row, u):
        at = [((u * per + a) * row_chunks + peer_row) * 8 for a in range(per)]
        pieces = [ref[aligned(row, 8), :] for row in at]
        return [group_turn(pieces, g, group, slots) for g in range(per)]

    def pack(peer_row):
        for u in range(parts):
            tiles = turned_tiles(sent, peer_row, u)
            for i in range(per // SHARE):
                low, high = tiles[SHARE * i : SHARE * (i + 1)]
                base = ((peer_row * (per // SHARE) + i) * parts + u) * 16
                send1[aligned(base + FIRSTS, 8), :] = jnp.where(top, low, pltpu.roll(high, 4, 0))
                send1[aligned(base + MARKS, 8), :] = jnp.where(top, pltpu.roll(low, 4, 0), high)
                for k in range(SHARE):
                    send1[pl.ds(base + MARKS + 4 * k + POSE_ROW, 1), :] = pose_lines[k]

    def pack_rest(peer_row):
        for u in range(parts):
            for g, tile in enumerate(turned_tiles(sent2, peer_row, u)):
                base = (peer_row * (per // SHARE) + g // SHARE) * parts + u
                send2[aligned((base * SHARE + g % SHARE) * 8, 8), :] = tile

    loop(row_chunks, pack)

    from_plane = n_map - 1 + n_tm - 1
    pl.semaphore_wait(barrier, jnp.where(reduces, from_plane, reducers + tm))
    mine = aligned(mp * message, message)

    rest_mine = aligned(mp * rest_rows, rest_rows)

    def send_moments(other, peer):
        send(send1.at[aligned(other * message, message), :], recv1.at[mine, :], peer, 0)

    def send_rest(other, peer):
        send(send2.at[aligned(other * rest_rows, rest_rows), :], recv2.at[rest_mine, :], peer, 7)

    def normals_to(t, k):
        return recv_n.at[aligned((t * SHARE + k) * n_size, n_size), :]

    @pl.when(jnp.logical_not(reduces))
    def _():
        for peer in column:

            @pl.when(peer[0] < tm)
            def _(peer=peer):
                send(pair_n.at[n_mine, :], normals_to(tm, 0), (peer[0], near[1]), 1)

        send(pair_n.at[n_mine, :], pair_n.at[n_mine, :], near, 6)

    def to_reducers(send_part):
        for other in others:
            send_part(other, (tm, other * SHARE + SHARE - 1))

        @pl.when(jnp.logical_not(reduces))
        def _():
            send_part(rd, near)

    to_reducers(send_moments)

    @pl.when(reduces)
    def _():
        for peer in column:
            send(pair_n.at[pl.ds(n_size, n_size), :], normals_to(tm, 1), peer, 1)

    loop(chunks, second_moments)
    loop(row_chunks, pack_rest)
    to_reducers(send_rest)
    eight = aligned(rd * 8, 8)

    def reduce_part():
        wait_rows(n_size, recvs.at[6])
        for peer in column:

            @pl.when(peer[0] > tm)
            def _(peer=peer):
                send(pair_n.at[pl.ds(0, n_size), :], normals_to(tm, 0), peer, 1)

        n_column = aligned(tm * SHARE * n_size, SHARE * n_size)
        recv1[mine, :] = send1[aligned(rd * message, message), :]
        recv2[rest_mine, :] = send2[aligned(rd * rest_rows, rest_rows), :]
        recv_n[n_column, :] = pair_n[...]
        for t in range(n_tm):
            world[pl.ds(3 * n_tm + t, arrived, stride=4 * n_tm), :] = jnp.where(
                own_turn[t], 1.0, 0.0
            )
        quads[...] = jnp.zeros_like(quads)
        send_g[...] = jnp.zeros_like(send_g)
        late[...] = jnp.zeros_like(late)
        wait_rows((n_map - 1) * message, recvs.at[0])

        def place(q, side):
            i, u = (q // parts, q % parts) if isinstance(q, int) else (q // parts, lax.rem(q, parts))
            return (2 * i + side) * parts + u

        def couple_row(k, q, row, turn):
            return jnp.concatenate(
                [
                    recv1[pl.ds(place(q, side) * 16 + 4 * k + row + turn, 1), :]
                    for side in range(2)
                ],
                axis=1,
            )

        def couple_tile(ref, k, q, rows):
            return jnp.concatenate(
                [ref[aligned((k * in_plane + place(q, side)) * rows, rows), :] for side in range(2)],
                axis=1,
            )

        def marked(row, count):
            kind = bf16 if count <= 256 else f32
            line = jnp.broadcast_to(row, (16, 2 * LANES)).astype(kind)
            number = lax.broadcasted_iota(jnp.int32, (count, 2 * LANES), 0).astype(f32).astype(kind)
            found = jnp.concatenate([line] * (count // 16), axis=0) == number
            return jnp.where(found, jnp.ones((), kind), jnp.zeros((), kind)).astype(bf16)

        def two_levels_of(row, levels, count):
            low = count // levels
            number = row.astype(jnp.int32)
            high = jnp.broadcast_to(number // low, (16, 2 * LANES)).astype(f32).astype(bf16)
            return high, marked(jnp.bitwise_and(number, low - 1).astype(f32), low)

        def picked(values, high_line, levels):
            three = split(values)
            rows = three.shape[0]
            high = jnp.concatenate([high_line] * (-(-rows // 16)), axis=0)[:rows]
            return jnp.concatenate(
                [
                    jnp.where(high == jnp.full((), h, bf16), three, jnp.zeros((), bf16))
                    for h in range(levels)
                ],
                axis=0,
            )

        def two_level(values, row, levels, count):
            high, low_marks = two_levels_of(row, levels, count)
            return picked(values, high, levels), low_marks

        def product(left, right):
            return lax.dot_general(left, right, CONTRACT_LAST, preferred_element_type=f32)

        def products(each_side, kinds, rows, columns):
            if couples > 8:
                return sum(
                    summed(couples, lambda q, k=k: product(*each_side(k, q)), rows, columns)
                    for k in kinds
                )
            sides = [each_side(k, q) for k in kinds for q in range(couples)]
            return product(*[jnp.concatenate(side, axis=1) for side in zip(*sides)])

        again = jnp.minimum(tm, 0)

        def scan_hot(k, q, turn):
            return marked(couple_row(k, q, SCAN_ROW, turn), scans)

        def vox_hot(k, q, turn):
            return marked(couple_row(k, q, VOX_ROW, turn), voxels)

        own_group = lane // own_scans
        def each_part(ref, row, gap):
            return jnp.concatenate(
                [every(ref, row + gap * k, 16, in_plane) for k in range(SHARE)], axis=0
            )

        def gather(tables, high, low):
            value = jnp.take_along_axis(tables[0], low, axis=1, mode="promise_in_bounds")
            for h in range(1, len(tables)):
                other = jnp.take_along_axis(tables[h], low, axis=1, mode="promise_in_bounds")
                value = jnp.where(high == h, other, value)
            return value

        columns = []
        for h in range(wide):
            at = [(h * spread + a) * message + MARKS for a in range(spread)]
            tiles = [recv1[row : row + 8, :] for row in at]
            columns.append([group_turn(tiles, g, own_group, own_scans) for g in range(4)])
        scan_of = each_part(recv1, MARKS + SCAN_ROW, 4).astype(jnp.int32)
        scan_low, scan_high = jnp.bitwise_and(scan_of, LANES - 1), scan_of // LANES

        def pose_of(k, g):
            row = 4 * k + POSE_ROW
            rows = [
                jnp.broadcast_to(turned[g][row : row + 1], (arrived, LANES)) for turned in columns
            ]
            return gather(rows, scan_high, scan_low)

        qw, qx, qy, qz = [pose_of(0, g) for g in range(4)]
        shift = [pose_of(1, g) for g in range(3)]
        rot = [
            [1 - 2 * (qy * qy + qz * qz), 2 * (qx * qy - qw * qz), 2 * (qx * qz + qw * qy)],
            [2 * (qx * qy + qw * qz), 1 - 2 * (qx * qx + qz * qz), 2 * (qy * qz - qw * qx)],
            [2 * (qx * qz - qw * qy), 2 * (qy * qz + qw * qx), 1 - 2 * (qx * qx + qy * qy)],
        ]
        first = [each_part(recv1, FIRSTS + k, 4) for k in range(3)]
        turned_first = [sum(rot[i][j] * first[j] for j in range(3)) for i in range(3)]
        m1 = [turned_first[i] + npoints * shift[i] for i in range(3)]
        for c in range(3):
            for t in range(n_tm):
                world[pl.ds(c * n_tm + t, arrived, stride=4 * n_tm), :] = jnp.where(
                    own_turn[t], m1[c], 0.0
                )

        def voxel_sums(ref, rows, k, turn):
            def add(q):
                return lax.dot_general(
                    split(couple_tile(ref, k, q, rows)),
                    vox_hot(k, q, turn),
                    CONTRACT_LAST,
                    preferred_element_type=f32,
                )

            return joined(summed(couples, add, 3 * rows, voxels))

        def first_sums(k):
            rows = 12 * n_tm

            def sides(k, q):
                values = couple_tile(world, k, q, 4 * n_tm)
                return two_level(values, couple_row(k, q, VOX_ROW, 0), halves, voxels)

            found = products(sides, [k], halves * rows, LANES)
            return jnp.concatenate(
                [joined(found[h * rows : (h + 1) * rows]) for h in range(halves)], axis=1
            )

        sums = [first_sums(k) for k in range(SHARE)]
        wait_rows((n_tm - 1) * SHARE * n_size, recvs.at[1])
        normal = [
            [
                jnp.concatenate(
                    [
                        every(recv_n, k * n_size + c * halves + h, SHARE * n_size, n_tm)
                        for h in range(halves)
                    ],
                    axis=1,
                )
                for c in range(3)
            ]
            for k in range(SHARE)
        ]
        for k in range(SHARE):
            along = sum(normal[k][c] * sums[k][c * n_tm : (c + 1) * n_tm] for c in range(3))
            count = sums[k][3 * n_tm : 4 * n_tm]
            for h in range(halves):
                at = slice(h * LANES, (h + 1) * LANES)
                base = (k * halves + h) * a_rows
                send_a[base : base + n_tm, :] = along[:, at]
                send_a[base + n_tm : base + a_rows, :] = count[:, at]

        a_mine = aligned(tm * a_size, a_size)
        for peer in column:
            send(send_a, recv_a.at[a_mine, :], peer, 2)
        recv_a[a_mine, :] = send_a[...]

        vox_of = each_part(recv1, MARKS + VOX_ROW, 4).astype(jnp.int32)
        live = vox_of >= 0
        vox_low = jnp.bitwise_and(vox_of, LANES - 1)
        vox_high = jnp.where(live, vox_of, 0) // LANES

        def by_voxel(rows):
            value = None
            for t in range(n_tm):
                tables = []
                for h in range(halves):
                    each = [jnp.broadcast_to(rows(k, t, h), (in_plane, LANES)) for k in range(SHARE)]
                    tables.append(jnp.concatenate(each, axis=0))
                found = gather(tables, vox_high, vox_low)
                value = found if t == 0 else jnp.where(own_turn[t], found, value)
            return value

        n = []
        for c in range(3):
            value = by_voxel(
                lambda k, t, h: normal[k][c][t : t + 1, h * LANES : (h + 1) * LANES]
            )
            n.append(jnp.where(live, value, 0.0))
        wait_rows((n_map - 1) * rest_rows, recvs.at[7])
        second = [each_part(recv2, k, 8) for k in range(6)]
        half_turned = [
            [sum(rot[i][k] * second[PAIR_ROW[(k, j)]] for k in range(3)) for j in range(3)]
            for i in range(3)
        ]
        m2 = [
            sum(half_turned[i][k] * rot[j][k] for k in range(3))
            + turned_first[i] * shift[j]
            + shift[i] * m1[j]
            for i, j in PAIRS
        ]
        quad = sum(n[i] ** 2 * m2[i] for i in range(3)) + 2.0 * sum(
            n[PAIRS[k][0]] * n[PAIRS[k][1]] * m2[k] for k in range(3, 6)
        )
        for t in range(n_tm):
            quads[pl.ds(t, arrived, stride=8), :] = jnp.where(own_turn[t], quad, 0.0)
        for k in range(SHARE):
            quad_sums = voxel_sums(quads, 8, k, again)
            for t in range(n_tm):
                for h in range(halves):
                    send_q[t, k * halves + h : k * halves + h + 1, :] = quad_sums[
                        t : t + 1, h * LANES : (h + 1) * LANES
                    ]
        for peer in column:
            send(send_q.at[peer[0]], recv_q.at[tm], peer, 3)
        recv_q[tm] = send_q[tm]

        def skew(v):
            return [
                n[2] * v[1] - n[1] * v[2],
                n[0] * v[2] - n[2] * v[0],
                n[1] * v[0] - n[0] * v[1],
            ]

        full = [[m2[PAIR_ROW[(i, j)]] for j in range(3)] for i in range(3)]
        skewed = [skew([full[k][j] for k in range(3)]) for j in range(3)]
        left = [[skewed[j][i] for j in range(3)] for i in range(3)]
        corner_block = [skew(left[i]) for i in range(3)]
        skew_first = skew(m1)
        found = {}
        for i in range(3):
            for j in range(3):
                if j >= i:
                    found[("h", i, j)] = corner_block[i][j]
                    found[("h", 3 + i, 3 + j)] = npoints * n[i] * n[j]
                found[("h", i, 3 + j)] = skew_first[i] * n[j]
        rest = n[0] * m1[0] + n[1] * m1[1] + n[2] * m1[2]
        for i in range(3):
            found[("g", i)] = sum(left[i][j] * n[j] for j in range(3))
            found[("g", 3 + i)] = n[i] * rest
        shares = skew_first + [npoints * n[i] for i in range(3)]
        for name, value in found.items():
            terms[pl.ds(ROWS.index(name), arrived, stride=32), :] = value
        for k in range(len(found), 32):
            terms[pl.ds(k, arrived, stride=32), :] = jnp.zeros_like(rest)

        def scan_sums(k, tile, rows, turn):
            def add(q):
                return lax.dot_general(
                    split(tile(k, q)),
                    scan_hot(k, q, turn),
                    CONTRACT_LAST,
                    preferred_element_type=f32,
                )

            return summed(couples, add, 3 * rows, scans)

        per_scan = scale * joined(
            sum(
                scan_sums(k, lambda k, q: couple_tile(terms, k, q, 32), 32, 0) for k in range(SHARE)
            )
        )
        for h in range(wide):
            pieces = [per_scan[8 * c : 8 * c + 8, h * LANES : (h + 1) * LANES] for c in range(4)]
            for b in range(spread):
                at = (h * spread + b) * 8
                send_h[at : at + 8, :] = group_turn(pieces, b, own_group, own_scans)
        for peer in plane:
            send(send_h.at[aligned(peer[1] * 8, 8), :], recv_h.at[eight, :], peer, 4)
        recv_h[eight, :] = send_h[aligned(mp * 8, 8), :]

        for k in range(SHARE):

            def keep_marks(q, k=k):
                at = k * couples + q
                late_high[at], late_low[at] = two_levels_of(
                    couple_row(k, q, SCAN_ROW, again), LEVELS, scans
                )

            loop(couples, keep_marks)

        wait_rows((n_tm - 1) * a_size, recvs.at[2])
        offset_rows = []
        for k in range(SHARE):
            offsets = []
            for h in range(halves):
                base = (k * halves + h) * a_rows
                total = recv_a[base : base + a_rows, :]
                for t in range(1, n_tm):
                    total = total + recv_a[t * a_size + base : t * a_size + base + a_rows, :]
                floor = jnp.maximum(total[n_tm:] * npoints, 1.0)
                offset = total[:n_tm] / floor
                total_a[base : base + n_tm, :] = offset
                total_a[base + n_tm : base + a_rows, :] = floor
                offsets.append(offset)
            offset_rows.append(offsets)
        offset_of = by_voxel(lambda k, t, h: offset_rows[k][h][t : t + 1])
        for i in range(6):
            late[pl.ds(i, arrived, stride=8), :] = shares[i] * offset_of

        def late_sides(k, q):
            at = k * couples + q + again
            return picked(couple_tile(late, k, q, 8), late_high[at], LEVELS), late_low[at]

        moved = products(late_sides, range(SHARE), LEVELS * 24, scans // LEVELS)
        for h in range(LEVELS):
            send_g[h * 8 : h * 8 + 8, 0 : scans // LEVELS] = scale * joined(
                moved[h * 24 : h * 24 + 24]
            )
        for peer in plane:
            source = send_g.at[aligned(peer[1] // in_level * 8, 8), :]
            send(source, recv_g.at[eight, :], peer, 5)
        recv_g[eight, :] = send_g[aligned(mp // in_level * 8, 8), :]

        pltpu.make_async_copy(
            recv_q.at[pl.ds(0, n_tm - 1)], recv_q.at[pl.ds(0, n_tm - 1)], recvs.at[3]
        ).wait()
        quad_total = recv_q[0]
        for t in range(1, n_tm):
            quad_total = quad_total + recv_q[t]
        own_offset = total_a[pl.ds(tm, SHARE * halves, stride=a_rows), :]
        own_floor = total_a[pl.ds(n_tm + tm, SHARE * halves, stride=a_rows), :]
        cost = quad_total / own_floor - own_offset**2
        send_c[...] = cost[0:halves]
        send(send_c, recv_c, first_of, 6)
        recv_c[...] = cost[halves:]

    pl.when(reduces)(reduce_part)


    def wait_plane(s):
        @pl.when(reduces)
        def _():
            wait_rows((reducers - 1) * 8, recvs.at[s])

        @pl.when(jnp.logical_not(reduces))
        def _():
            wait_rows(reducers * 8, recvs.at[s])

    lines[...] = jnp.zeros_like(lines)
    wait_plane(4)
    total = recv_h[0:8, :]
    for m in range(1, reducers):
        total = total + recv_h[m * 8 : m * 8 + 8, :]
    lined = [total] + [pltpu.roll(total, LANES - own_scans * c, 1) for c in range(1, 4)]

    def row_at(name):
        k = ROWS.index(name)
        return lined[k // 8][k % 8 : k % 8 + 1]

    for i in range(6):
        for j in range(6):
            lines[6 * i + j : 6 * i + j + 1, :] = row_at(("h", min(i, j), max(i, j)))
    hess_out[...] = lines[...].T[0:own_scans, 0:36]
    gradient = jnp.concatenate([row_at(("g", i)) for i in range(6)], axis=0)

    @pl.when(jnp.logical_not(reduces))
    def _():
        pltpu.make_async_copy(recv_c, recv_c, recvs.at[6]).wait()

    for h in range(halves):
        cost_out[:, h * LANES : (h + 1) * LANES] = recv_c[h : h + 1, :]

    wait_plane(5)
    change = recv_g[0:8, :]
    for m in range(1, reducers):
        change = change + recv_g[m * 8 : m * 8 + 8, :]
    change = pltpu.roll(change, LANES - own_scans * lax.rem(mp, in_level), 1)
    grad_out[...] = (gradient - change[0:6])[:, 0:own_scans]

    for t in range(n_tm):

        @pl.when(jnp.logical_and(reduces, tm == t))
        def _(t=t):
            rows = (reducers - 1) * (message + rest_rows) + (n_map - 1) * 16 + halves
            rows += (n_tm - 1) * (n_size + a_size + SHARE * halves) + (n_tm - 1 - t) * n_size
            wait_rows(rows, sends.at[0])

        @pl.when(jnp.logical_and(jnp.logical_not(reduces), tm == t))
        def _(t=t):
            wait_rows(reducers * (message + rest_rows) + (t + 1) * n_size, sends.at[0])


def finish(hess_in, grad_in, cost_in, hess_out, grad_out, cost_out, sems):
    copies = [
        pltpu.make_async_copy(src, dst, sems.at[i])
        for i, (src, dst) in enumerate(
            [(hess_in, hess_out), (grad_in, grad_out), (cost_in, cost_out)]
        )
    ]
    for copy in copies:
        copy.start()
    for copy in copies:
        copy.wait()


def local(points, poses, normal_angles, voxel_ids, scan_ids):
    blocks, npoints = points.shape[1:]
    n_tm, n_map = lax.axis_size("tm"), lax.axis_size("map")
    devices = n_tm * n_map
    slots = blocks // devices
    chunks = blocks // LANES
    vox_count = normal_angles.shape[1]
    own_scans = poses.shape[1]
    assert npoints == LANES and slots * 4 == LANES and own_scans * 4 == LANES
    assert n_map & (n_map - 1) == 0 and n_map % LEVELS == 0 and n_map <= 4 * LEVELS and n_map % 4 == 0 and n_map % SHARE == 0 and n_tm % 4 == 0 and vox_count % LANES == 0
    scale = own_scans * devices / (blocks * devices * npoints)
    f32, bf16 = jnp.float32, jnp.bfloat16
    scans = own_scans * n_map
    halves = vox_count // LANES
    in_plane = n_map * n_tm // 4
    reducers = n_map // SHARE
    packed = reducers * n_tm // 4
    arrived = SHARE * n_map * n_tm // 4
    n_rows = -(-3 * halves // 8) * 8
    a_rows = SHARE * 2 * n_tm * halves
    hbm = pl.BlockSpec(memory_space=pl.ANY)
    vmem = pl.BlockSpec(memory_space=pltpu.VMEM)
    shapes = [(own_scans, 36), (6, own_scans), (1, vox_count)]
    results = pl.pallas_call(
        functools.partial(kernel, (n_tm, n_map, slots, float(npoints), scale)),
        out_shape=tuple(pltpu.VMEM(shape, f32) for shape in shapes),
        in_specs=[hbm] * 5,
        out_specs=(vmem,) * 3,
        scratch_shapes=[
            pltpu.VMEM(points.shape, f32),
            pltpu.VMEM(poses.shape, f32),
            pltpu.VMEM(normal_angles.shape, f32),
            pltpu.VMEM((chunks, LANES), jnp.int32),
            pltpu.VMEM((chunks, LANES), jnp.int32),
            pltpu.VMEM((8, LANES), f32),
            pltpu.VMEM((chunks * 8, LANES), f32),
            pltpu.VMEM((chunks * 8, LANES), f32),
            pltpu.VMEM((packed * 16, LANES), f32),
            pltpu.VMEM((in_plane * 16, LANES), f32),
            pltpu.VMEM((packed * 16, LANES), f32),
            pltpu.VMEM((in_plane * 16, LANES), f32),
            pltpu.VMEM((SHARE * n_rows, LANES), f32),
            pltpu.VMEM((n_tm * SHARE * n_rows, LANES), f32),
            pltpu.VMEM((arrived * 4 * n_tm, LANES), f32),
            pltpu.VMEM((a_rows, LANES), f32),
            pltpu.VMEM((n_tm * a_rows, LANES), f32),
            pltpu.VMEM((a_rows, LANES), f32),
            pltpu.VMEM((arrived * 8, LANES), f32),
            pltpu.VMEM((n_tm, SHARE * halves, LANES), f32),
            pltpu.VMEM((n_tm, SHARE * halves, LANES), f32),
            pltpu.VMEM((halves, LANES), f32),
            pltpu.VMEM((halves, LANES), f32),
            pltpu.VMEM((arrived * 32, LANES), f32),
            pltpu.VMEM((arrived * 8, LANES), f32),
            pltpu.VMEM((arrived // 2, 16, 2 * LANES), bf16),
            pltpu.VMEM((arrived // 2, scans // LEVELS, 2 * LANES), bf16),
            pltpu.VMEM((n_map * 8, LANES), f32),
            pltpu.VMEM((reducers * 8, LANES), f32),
            pltpu.VMEM((LEVELS * 8, LANES), f32),
            pltpu.VMEM((reducers * 8, LANES), f32),
            pltpu.VMEM((LANES, LANES), f32),
            pltpu.SemaphoreType.DMA((2,)),
            pltpu.SemaphoreType.DMA((4,)),
            pltpu.SemaphoreType.DMA((1,)),
            pltpu.SemaphoreType.DMA((8,)),
        ],
        compiler_params=pltpu.CompilerParams(collective_id=0, has_side_effects=True),
    )(
        points,
        poses,
        normal_angles,
        voxel_ids.reshape(chunks, LANES),
        scan_ids.reshape(chunks, LANES),
    )
    hess, grad, cost = pl.pallas_call(
        finish,
        out_shape=tuple(jax.ShapeDtypeStruct(shape, f32) for shape in shapes),
        in_specs=[vmem] * 3,
        out_specs=(hbm,) * 3,
        scratch_shapes=[pltpu.SemaphoreType.DMA((3,))],
    )(*[pltpu.with_memory_space_constraint(x, pltpu.VMEM) for x in results])
    return hess.T, grad, cost.reshape(vox_count)


def solution(mesh):
    return jax.shard_map(
        local,
        mesh=mesh,
        in_specs=(
            P(None, ("tm", "map"), None),
            P(None, ("tm", "map")),
            P(None, ("tm", "map")),
            P(("tm", "map")),
            P(("tm", "map")),
        ),
        out_specs=(P(None, ("tm", "map")), P(None, ("tm", "map")), P(("tm", "map"))),
        check_vma=False,
    )
```
